16 devices in a mesh: dp: 4 (over z, y), cp: 4 (over x, core).
Axes of the slice: x: 2, y: 2, z: 2, core: 2. Of those that a mesh axis runs over, the one named last changes fastest.
Arguments:
- hidden: bfloat16 [128, 8, 1024], P('dp'), parts along dimension 0
- memory: bfloat16 [128, 1024, 1024], P('dp', 'cp'), parts along dimension 0
- ln_gain: bfloat16 [1024], replicated
- ln_bias: bfloat16 [1024], replicated
- w_q: bfloat16 [1024, 1024], replicated
- b_q: bfloat16 [1024], replicated
- w_k: bfloat16 [1024, 1024], replicated
- w_v: bfloat16 [1024, 1024], replicated
- b_v: bfloat16 [1024], replicated
- w_o: bfloat16 [1024, 1024], replicated
- b_o: bfloat16 [1024], replicated
- grad_y: bfloat16 [128, 8, 1024], P('dp'), parts along dimension 0
Outputs:
- output 1: bfloat16 [128, 8, 1024], P('dp'), parts along dimension 0
- output 2: bfloat16 [128, 8, 1024], P('dp'), parts along dimension 0
- output 3: bfloat16 [128, 1024, 1024], P('dp', 'cp'), parts along dimension 0
- output 4: float32 [4096], P('dp'), parts along dimension 0
- output 5: float32 [4096], P('dp'), parts along dimension 0
- output 6: float32 [4096, 1024], P('dp'), parts along dimension 0
- output 7: float32 [4096], P('dp'), parts along dimension 0
- output 8: float32 [4096, 1024], P('dp'), parts along dimension 0
- output 9: float32 [4096, 1024], P('dp'), parts along dimension 0
- output 10: float32 [4096], P('dp'), parts along dimension 0
- output 11: float32 [4096, 1024], P('dp'), parts along dimension 0
- output 12: float32 [4096], P('dp'), parts along dimension 0
There are 4 independent parts. The reference program is written for one: setup_inputs(seed, part) draws one part's arguments, and reference() takes and returns one part's arrays. A program takes and returns all parts, laid end to end along the dimension named above; an argument that names none is the same for every part.
All inputs are finite; a program needn't handle non-finite values.
Results may differ from the reference program's by a relative error of at most 0.00976275.
Values are sent between devices in bfloat16 or wider.
A program may use at most 1 GiB of HBM per device.

```python
import math
import jax
import jax.numpy as jnp
from jax import lax

BATCH = 32
TOKENS = 8
FRAMES = 1024
D = 1024
HEADS = 16
HEAD = 64
EPS = 1e-5


def setup_inputs(seed: int = 0, part: int = 0) -> dict:
    root_key = jax.random.key(seed)
    shared_key, group_key = jax.random.split(root_key)
    group_key = jax.random.fold_in(group_key, part)
    act_keys = jax.random.split(group_key, 3)
    weight_keys = jax.random.split(shared_key, 9)
    inv_root = D ** -0.5
    sharpness = math.sqrt(math.log(FRAMES / 16.0))
    qk_std = math.sqrt(sharpness) * inv_root

    def draw(draw_key, dims, spread):
        return (jax.random.normal(draw_key, dims, jnp.float32) * spread).astype(jnp.bfloat16)

    return {
        "hidden": draw(act_keys[0], (BATCH, TOKENS, D), 1.0),
        "memory": draw(act_keys[1], (BATCH, FRAMES, D), 1.0),
        "ln_gain": (1.0 + 0.2 * jax.random.normal(weight_keys[0], (D,), jnp.float32)).astype(jnp.bfloat16),
        "ln_bias": draw(weight_keys[1], (D,), 0.2),
        "w_q": draw(weight_keys[2], (D, D), qk_std),
        "b_q": draw(weight_keys[3], (D,), 0.3),
        "w_k": draw(weight_keys[4], (D, D), qk_std),
        "w_v": draw(weight_keys[5], (D, D), inv_root),
        "b_v": draw(weight_keys[6], (D,), 0.3),
        "w_o": draw(weight_keys[7], (D, D), 2.0 * inv_root),
        "b_o": draw(weight_keys[8], (D,), 0.3),
        "grad_y": draw(act_keys[2], (BATCH, TOKENS, D), 1.0),
    }


def widen(array_in):
    return array_in.astype(jnp.float32)


def reference(hidden, memory, ln_gain, ln_bias, w_q, b_q, w_k, w_v, b_v, w_o, b_o, grad_y):
    logit_scale = HEAD ** -0.5
    hidden_f32 = widen(hidden)
    memory_f32 = widen(memory)
    centered = hidden_f32 - jnp.mean(hidden_f32, axis=-1, keepdims=True)
    inv_std = lax.rsqrt(jnp.mean(centered * centered, axis=-1, keepdims=True) + EPS)
    x_hat = centered * inv_std
    x_norm = (x_hat * widen(ln_gain) + widen(ln_bias)).astype(jnp.bfloat16)
    q_proj = (jnp.einsum("btd,de->bte", widen(x_norm), widen(w_q)) + widen(b_q)).astype(jnp.bfloat16)
    k_proj = jnp.einsum("bfd,de->bfe", memory_f32, widen(w_k)).astype(jnp.bfloat16)
    v_proj = (jnp.einsum("bfd,de->bfe", memory_f32, widen(w_v)) + widen(b_v)).astype(jnp.bfloat16)
    q_heads = widen(q_proj).reshape(BATCH, TOKENS, HEADS, HEAD)
    k_heads = widen(k_proj).reshape(BATCH, FRAMES, HEADS, HEAD)
    v_heads = widen(v_proj).reshape(BATCH, FRAMES, HEADS, HEAD)
    logits = jnp.einsum("bthe,bfhe->bhtf", q_heads, k_heads) * logit_scale
    attn_probs = jax.nn.softmax(logits, axis=-1)
    probs_low = widen(attn_probs.astype(jnp.bfloat16))
    attn_out = jnp.einsum("bhtf,bfhe->bthe", probs_low, v_heads).reshape(BATCH, TOKENS, D).astype(jnp.bfloat16)
    out_y = (hidden_f32 + jnp.einsum("btd,de->bte", widen(attn_out), widen(w_o)) + widen(b_o)).astype(jnp.bfloat16)

    dy_f32 = widen(grad_y)
    grad_wo = jnp.einsum("btd,bte->de", widen(attn_out), dy_f32)
    grad_bo = jnp.sum(dy_f32, axis=(0, 1))
    d_attn = jnp.einsum("bte,de->btd", dy_f32, widen(w_o)).astype(jnp.bfloat16)
    d_heads = widen(d_attn).reshape(BATCH, TOKENS, HEADS, HEAD)
    d_probs = jnp.einsum("bthe,bfhe->bhtf", d_heads, v_heads)
    row_dot = jnp.sum(attn_probs * d_probs, axis=-1, keepdims=True)
    d_logits = widen((attn_probs * (d_probs - row_dot) * logit_scale).astype(jnp.bfloat16))
    grad_q = jnp.einsum("bhtf,bfhe->bthe", d_logits, k_heads).reshape(BATCH, TOKENS, D)
    grad_k = jnp.einsum("bhtf,bthe->bfhe", d_logits, q_heads).reshape(BATCH, FRAMES, D).astype(jnp.bfloat16)
    grad_v = jnp.einsum("bhtf,bthe->bfhe", probs_low, d_heads).reshape(BATCH, FRAMES, D)
    grad_bq = jnp.sum(grad_q, axis=(0, 1))
    grad_bv = jnp.sum(grad_v, axis=(0, 1))
    dq_low = widen(grad_q.astype(jnp.bfloat16))
    dk_low = widen(grad_k)
    dv_low = widen(grad_v.astype(jnp.bfloat16))
    grad_wq = jnp.einsum("btd,bte->de", widen(x_norm), dq_low)
    d_xnorm = jnp.einsum("bte,de->btd", dq_low, widen(w_q))
    grad_wk = jnp.einsum("bfd,bfe->de", memory_f32, dk_low)
    grad_wv = jnp.einsum("bfd,bfe->de", memory_f32, dv_low)
    grad_mem = (jnp.einsum("bfe,de->bfd", dk_low, widen(w_k)) + jnp.einsum("bfe,de->bfd", dv_low, widen(w_v))).astype(jnp.bfloat16)
    grad_ln_gain = jnp.sum(d_xnorm * x_hat, axis=(0, 1))
    grad_ln_bias = jnp.sum(d_xnorm, axis=(0, 1))
    d_hat = d_xnorm * widen(ln_gain)
    d_hidden = inv_std * (d_hat - jnp.mean(d_hat, axis=-1, keepdims=True) - x_hat * jnp.mean(d_hat * x_hat, axis=-1, keepdims=True))
    grad_h = (dy_f32 + d_hidden).astype(jnp.bfloat16)
    return (out_y, grad_h, grad_mem, grad_ln_gain, grad_ln_bias, grad_wq, grad_bq, grad_wk, grad_wv, grad_bv, grad_wo, grad_bo)
```

```python
import functools

import jax
import jax.numpy as jnp
from jax import lax
from jax.experimental import pallas as pl
from jax.experimental.pallas import tpu as pltpu
from jax.sharding import PartitionSpec as P

EPS = 1e-5
HEAD = 64
PAIR = 2 * HEAD
F32 = jnp.float32
BF16 = jnp.bfloat16
NT = (((1,), (1,)), ((), ()))
TN = (((0,), (0,)), ((), ()))
NN = (((1,), (0,)), ((), ()))
VMEM_LIMIT = 60 * 1024 * 1024


def dot(a, b, dims):
    return lax.dot_general(a, b, dims, preferred_element_type=F32)


def split_heads(x):
    low = lax.broadcasted_iota(jnp.int32, x.shape, 1) < HEAD
    zero = jnp.zeros_like(x)
    return jnp.concatenate([jnp.where(low, x, zero), jnp.where(low, zero, x)], axis=0)


def join_heads(x):
    rows = x.shape[0] // 2
    low = lax.broadcasted_iota(jnp.int32, (rows, x.shape[1]), 1) < HEAD
    return jnp.where(low, x[:rows], x[rows:])


def front_kernel(h_ref, gy_ref, g_ref, b_ref, wq_ref, bq_ref, wk_ref, wv_ref, bv_ref, wo_ref,
                 q_ref, do_ref, z_ref, r_ref, x_scr):
    n_seq, n_tok = z_ref.shape[0], h_ref.shape[0] // z_ref.shape[0]

    @pl.when(pl.program_id(0) == 0)
    def _():
        h = h_ref[...].astype(F32)
        c = h - jnp.mean(h, axis=-1, keepdims=True)
        inv = lax.rsqrt(jnp.mean(c * c, axis=-1, keepdims=True) + EPS)
        x_scr[...] = (c * inv * g_ref[...].astype(F32) + b_ref[...].astype(F32)).astype(BF16)

    q = (dot(x_scr[...], wq_ref[...], NN) + bq_ref[...].astype(F32)).astype(BF16)
    d = dot(gy_ref[...], wo_ref[...], NT).astype(BF16)
    q_ref[...] = q
    do_ref[...] = d
    q2, d2 = split_heads(q), split_heads(d)
    half = q.shape[0]
    step = 256

    def place(part, x, w_ref):
        for j in range(0, w_ref.shape[0], step):
            t = dot(x, w_ref[j:j + step, :], NT)
            t = jnp.concatenate([t[:half].reshape(n_seq, n_tok, step), t[half:].reshape(n_seq, n_tok, step)], axis=1)
            z_ref[:, part, :, j:j + step] = t.astype(BF16)

    place(0, q2, wk_ref)
    place(1, d2, wv_ref)
    bias = dot(d2, jnp.broadcast_to(bv_ref[...], (PAIR, PAIR)), NT)
    r_ref[...] = jnp.concatenate([bias[:half].reshape(n_seq, n_tok, PAIR), bias[half:].reshape(n_seq, n_tok, PAIR)], axis=1)


def score_kernel(scale, m_ref, z_ref, r_ref, e_ref, dp_ref, st_ref):
    rows = e_ref.shape[-1]
    for j in range(m_ref.shape[0]):
        t = dot(m_ref[j], z_ref[j], NT)
        s = t[:, :rows] * scale
        dp = t[:, rows:] + r_ref[j].T[0:1, :]
        mx = jnp.max(s, axis=0, keepdims=True)
        e = jnp.exp(s - mx)
        e_ref[j] = e
        dp_ref[j] = dp
        st_ref[j, 0:1, :] = mx
        st_ref[j, 1:2, :] = jnp.sum(e, axis=0, keepdims=True)
        st_ref[j, 2:3, :] = jnp.sum(e * dp, axis=0, keepdims=True)


def grad_kernel(scale, n_first, core_ref, m_ref, e_ref, dp_ref, s0_ref, s1_ref, s2_ref, s3_ref,
                q_ref, do_ref, wk_ref, wv_ref, bv_ref,
                pg_ref, mine_ref, theirs_ref, o_ref, dq_ref, dbv_ref, gp_scr, ps_scr):
    i = pl.program_id(0)
    n_heads, rows = gp_scr.shape[1], e_ref.shape[-1]
    n_tok = rows // n_heads
    width = m_ref.shape[-1]

    @pl.when(i < n_first)
    def _():
        ones = jnp.ones((m_ref.shape[1], PAIR), BF16)
        parts, sums = [], []
        for j in range(2):
            stats = [s0_ref[j], s1_ref[j], s2_ref[j], s3_ref[j]]
            top = functools.reduce(jnp.maximum, [s[0:1] for s in stats])
            fac = [jnp.exp(s[0:1] - top) for s in stats]
            total = functools.reduce(jnp.add, [f * s[1:2] for f, s in zip(fac, stats)])
            c = functools.reduce(jnp.add, [f * s[2:3] for f, s in zip(fac, stats)]) / total
            p = e_ref[j] * (fac[0] / total)
            g = p * (dp_ref[j] - c) * scale
            pg_ref[j, :, :rows] = g.astype(BF16)
            pg_ref[j, :, rows:] = p.astype(BF16)
            pg = pg_ref[j]
            parts.append(dot(pg, m_ref[j], TN).reshape(2, n_heads, n_tok, width))
            sums.append(dot(pg[:, rows:], ones, TN).reshape(n_heads, n_tok, PAIR))
        at = pl.ds(pl.multiple_of(i * 2 * n_tok, 2 * n_tok), 2 * n_tok)
        gp_scr[:, :, at, :] = jnp.concatenate(parts, axis=2).astype(BF16)
        ps_scr[:, at, :] = jnp.concatenate(sums, axis=1)

    @pl.when(i >= n_first)
    def _():
        k = i - n_first
        n_rows = gp_scr.shape[2]
        gm = gp_scr[0, pl.ds(2 * k, 2)].reshape(2 * n_rows, width)
        pm = gp_scr[1, pl.ds(2 * k, 2)].reshape(2 * n_rows, width)
        ps = join_heads(ps_scr[pl.ds(2 * k, 2)].reshape(2 * n_rows, PAIR))
        dwk = dot(gm, split_heads(q_ref[...]), TN)
        dwv = dot(pm, split_heads(do_ref[...]), TN)
        first = core_ref[0] == 0
        mine_ref[...] = jnp.where(first, dwk, dwv)
        theirs_ref[...] = jnp.where(first, dwv, dwk)
        dq_ref[...] = join_heads(dot(gm, wk_ref[...], NN))
        o_ref[...] = join_heads(dot(pm, wv_ref[...], NN)) + ps * bv_ref[...].astype(F32)
        dbv_ref[...] = jnp.broadcast_to(jnp.sum(ps * do_ref[...].astype(F32), axis=0, keepdims=True), dbv_ref.shape)


def mem_kernel(pg_ref, z_ref, dm_ref):
    for j in range(pg_ref.shape[0]):
        dm_ref[j] = dot(pg_ref[j], z_ref[j], NN).astype(BF16)


def params():
    return pltpu.CompilerParams(dimension_semantics=("arbitrary",), vmem_limit_bytes=VMEM_LIMIT)


def solution(mesh):
    act_spec = P("dp", None, None)
    mem_spec = P("dp", "cp", None)
    vec_out = P("dp")
    mat_out = P("dp", None)
    in_specs = (act_spec, mem_spec, P(), P(), P(), P(), P(), P(), P(), P(), P(), act_spec)
    out_specs = (act_spec, act_spec, mem_spec, vec_out, vec_out, mat_out, vec_out, mat_out, mat_out, vec_out, mat_out, vec_out)
    n_cp = mesh.shape["cp"]

    def swap(x, bit):
        return lax.ppermute(x, "cp", [(i, i ^ bit) for i in range(n_cp)])

    def device_step(hidden, memory, ln_gain, ln_bias, w_q, b_q, w_k, w_v, b_v, w_o, b_o, grad_y):
        n_seq, n_tok, width = hidden.shape
        n_fr = memory.shape[1]
        n_heads = width // HEAD
        n_pairs = n_heads // 2
        rows = n_heads * n_tok
        tokens = n_seq * n_tok
        scale = HEAD ** -0.5
        core = lax.axis_index("cp") % 2
        h2, gy2 = hidden.reshape(tokens, width), grad_y.reshape(tokens, width)
        row = lambda v: v.reshape(1, width)
        full = lambda *s: pl.BlockSpec(s, lambda i: (0,) * len(s))
        col = lambda r: pl.BlockSpec((r, PAIR), lambda i: (0, i))

        q, d_o, z, r = pl.pallas_call(
            front_kernel, grid=(n_pairs,), name="front",
            in_specs=[full(tokens, width), full(tokens, width), full(1, width), full(1, width), col(width), col(1),
                      col(width), col(width), col(1), pl.BlockSpec((PAIR, width), lambda i: (i, 0))],
            out_specs=[col(tokens), col(tokens),
                       pl.BlockSpec((n_seq, 2, 2 * n_tok, width), lambda i: (0, 0, i, 0)),
                       pl.BlockSpec((n_seq, 2 * n_tok, PAIR), lambda i: (0, i, 0))],
            out_shape=[jax.ShapeDtypeStruct((tokens, width), BF16), jax.ShapeDtypeStruct((tokens, width), BF16),
                       jax.ShapeDtypeStruct((n_seq, 2, rows, width), BF16), jax.ShapeDtypeStruct((n_seq, rows, PAIR), F32)],
            scratch_shapes=[pltpu.VMEM((tokens, width), BF16)], compiler_params=params(),
        )(h2, gy2, row(ln_gain), row(ln_bias), w_q, row(b_q), w_k, w_v, row(b_v), w_o)
        z = z.reshape(n_seq, 2 * rows, width)

        blk = 4
        seq = lambda *s: pl.BlockSpec((blk,) + s, lambda i: (i, 0, 0))
        e, dp, st = pl.pallas_call(
            functools.partial(score_kernel, scale), grid=(n_seq // blk,), name="score",
            in_specs=[seq(n_fr, width), seq(2 * rows, width), seq(rows, PAIR)],
            out_specs=[seq(n_fr, rows), seq(n_fr, rows), seq(8, rows)],
            out_shape=[jax.ShapeDtypeStruct((n_seq, n_fr, rows), F32), jax.ShapeDtypeStruct((n_seq, n_fr, rows), F32),
                       jax.ShapeDtypeStruct((n_seq, 8, rows), F32)],
            compiler_params=params(),
        )(memory, z, r)
        others = [swap(st, bit) for bit in (1, 2, 3)]

        n_first = n_seq // 2
        two = lambda *s: pl.BlockSpec((2,) + s, lambda i: (jnp.minimum(i, n_first - 1), 0, 0))
        late = lambda r_: pl.BlockSpec((r_, PAIR), lambda i: (0, jnp.maximum(i - n_first, 0)))
        pg, mine, theirs, o_part, dq_part, dbv_part = pl.pallas_call(
            functools.partial(grad_kernel, scale, n_first), grid=(n_first + n_pairs,), name="grad",
            in_specs=[pl.BlockSpec(memory_space=pltpu.SMEM), two(n_fr, width), two(n_fr, rows), two(n_fr, rows)]
            + [two(8, rows)] * 4 + [late(tokens), late(tokens), late(width), late(width), late(1)],
            out_specs=[two(n_fr, 2 * rows), late(width), late(width), late(tokens), late(tokens), late(8)],
            out_shape=[jax.ShapeDtypeStruct((n_seq, n_fr, 2 * rows), BF16),
                       jax.ShapeDtypeStruct((width, width), F32), jax.ShapeDtypeStruct((width, width), F32),
                       jax.ShapeDtypeStruct((tokens, width), F32), jax.ShapeDtypeStruct((tokens, width), F32),
                       jax.ShapeDtypeStruct((8, width), F32)],
            scratch_shapes=[pltpu.VMEM((2, n_heads, tokens, width), BF16), pltpu.VMEM((n_heads, tokens, PAIR), F32)],
            compiler_params=params(),
        )(core.reshape(1).astype(jnp.int32), memory, e, dp, st, *others, q, d_o, w_k, w_v, row(b_v))

        n_chunk = 4
        step = width // n_chunk
        dwk, dwv = [], []
        for k in range(n_chunk):
            sl = slice(k * step, (k + 1) * step)
            chip = mine[sl] + swap(theirs[sl], 1)
            fin = chip + swap(chip, 2)
            other = swap(fin, 1)
            dwk.append(jnp.where(core == 0, fin, other))
            dwv.append(jnp.where(core == 0, other, fin))
        grad_wk = jnp.concatenate(dwk, axis=0)
        grad_wv = jnp.concatenate(dwv, axis=0)

        me = lax.axis_index("cp")
        both = jnp.stack([o_part, dq_part]).reshape(2, 2, 2, tokens // 4, width)
        give = lax.dynamic_index_in_dim(both, 1 - me % 2, 2, keepdims=False)
        keep = lax.dynamic_index_in_dim(both, me % 2, 2, keepdims=False)
        half = keep + swap(give, 1)
        give = lax.dynamic_index_in_dim(half, 1 - me // 2, 1, keepdims=False)
        keep = lax.dynamic_index_in_dim(half, me // 2, 1, keepdims=False)
        done = keep + swap(give, 2)
        dbq_part = jnp.sum(done[1], axis=0)
        low = done.astype(BF16)
        mate = swap(low, 2)
        pair = jnp.where(me // 2 == 0, jnp.stack([low, mate], 1), jnp.stack([mate, low], 1))
        mate = swap(pair, 1)
        quad = jnp.where(me % 2 == 0, jnp.stack([pair, mate], 2), jnp.stack([mate, pair], 2))
        attn_out = quad[0].reshape(tokens, width)
        dq_low = quad[1].reshape(tokens, width)
        small = jnp.stack([dbq_part, dbv_part[0]])
        small = small + swap(small, 1)
        small = small + swap(small, 2)
        grad_bq, grad_bv = small[0], small[1]

        hidden_f32 = h2.astype(F32)
        centered = hidden_f32 - jnp.mean(hidden_f32, axis=-1, keepdims=True)
        inv_std = lax.rsqrt(jnp.mean(centered * centered, axis=-1, keepdims=True) + EPS)
        x_hat = centered * inv_std
        gain_f32 = ln_gain.astype(F32)
        x_norm = (x_hat * gain_f32 + ln_bias.astype(F32)).astype(BF16)
        out_y = (hidden_f32 + dot(attn_out, w_o, NN) + b_o.astype(F32)).astype(BF16)
        grad_wo = dot(attn_out, gy2, TN)
        grad_bo = jnp.sum(gy2, axis=0, dtype=F32)
        grad_wq = dot(x_norm, dq_low, TN)
        d_xnorm = dot(dq_low, w_q, NT)
        grad_ln_gain = jnp.sum(d_xnorm * x_hat, axis=0)
        grad_ln_bias = jnp.sum(d_xnorm, axis=0)
        d_hat = d_xnorm * gain_f32
        d_hidden = inv_std * (d_hat - jnp.mean(d_hat, axis=-1, keepdims=True) - x_hat * jnp.mean(d_hat * x_hat, axis=-1, keepdims=True))
        grad_h = (gy2.astype(F32) + d_hidden).astype(BF16)

        grad_mem = pl.pallas_call(
            mem_kernel, grid=(n_seq // blk,), name="mem",
            in_specs=[seq(n_fr, 2 * rows), seq(2 * rows, width)], out_specs=seq(n_fr, width),
            out_shape=jax.ShapeDtypeStruct((n_seq, n_fr, width), BF16), compiler_params=params(),
            cost_estimate=pl.CostEstimate(flops=4 * n_seq * n_fr * rows * width, bytes_accessed=40 << 20, transcendentals=0),
        )(pg, z)
        return (out_y.reshape(hidden.shape), grad_h.reshape(hidden.shape), grad_mem, grad_ln_gain, grad_ln_bias,
                grad_wq, grad_bq, grad_wk, grad_wv, grad_bv, grad_wo, grad_bo)

    return jax.shard_map(device_step, mesh=mesh, in_specs=in_specs, out_specs=out_specs, check_vma=False)
```

```python
import functools

import jax
import jax.numpy as jnp
from jax import lax
from jax.experimental import pallas as pl
from jax.experimental.pallas import tpu as pltpu
from jax.sharding import PartitionSpec as P

EPS = 1e-5
HEAD = 64
PAIR = 2 * HEAD
F32 = jnp.float32
BF16 = jnp.bfloat16
NT = (((1,), (1,)), ((), ()))
TN = (((0,), (0,)), ((), ()))
NN = (((1,), (0,)), ((), ()))
VMEM_LIMIT = 60 * 1024 * 1024


def dot(a, b, dims):
    return lax.dot_general(a, b, dims, preferred_element_type=F32)


def split_heads(x):
    low = lax.broadcasted_iota(jnp.int32, x.shape, 1) < HEAD
    zero = jnp.zeros_like(x)
    return jnp.concatenate([jnp.where(low, x, zero), jnp.where(low, zero, x)], axis=0)


def join_heads(x):
    rows = x.shape[0] // 2
    low = lax.broadcasted_iota(jnp.int32, (rows, x.shape[1]), 1) < HEAD
    return jnp.where(low, x[:rows], x[rows:])


def normalize(h_ref, vec_ref, x_scr):
    h = h_ref[...].astype(F32)
    c = h - jnp.mean(h, axis=-1, keepdims=True)
    inv = lax.rsqrt(jnp.mean(c * c, axis=-1, keepdims=True) + EPS)
    x_scr[...] = (c * inv * vec_ref[0:1, :] + vec_ref[1:2, :]).astype(BF16)


def pair_of(vec_ref, row, i):
    return vec_ref[row:row + 1, pl.ds(pl.multiple_of(i * PAIR, PAIR), PAIR)]


def place(z_scr, part, i, x, w_ref):
    n_seq = z_scr.shape[0]
    half = x.shape[0] // 2
    n_tok = half // n_seq
    step = 256
    at = pl.ds(pl.multiple_of(i * 2 * n_tok, 2 * n_tok), 2 * n_tok)
    for j in range(0, w_ref.shape[0], step):
        t = dot(x, w_ref[j:j + step, :], NT)
        t = jnp.concatenate([t[:half].reshape(n_seq, n_tok, step), t[half:].reshape(n_seq, n_tok, step)], axis=1)
        z_scr[:, part, at, j:j + step] = t.astype(BF16)


def score_kernel(scale, n_first, h_ref, gy_ref, vec_ref, wq_ref, wk_ref, wv_ref, wo_ref, m_ref,
                 q_ref, do_ref, e_ref, dp_ref, st_ref, x_scr, z_scr, r_scr):
    i = pl.program_id(0)
    n_seq, _, rows, width = z_scr.shape

    @pl.when(i == 0)
    def _():
        normalize(h_ref, vec_ref, x_scr)

    @pl.when(i < n_first)
    def _():
        q = (dot(x_scr[...], wq_ref[...], NN) + pair_of(vec_ref, 2, i)).astype(BF16)
        d = dot(gy_ref[...], wo_ref[...], NT).astype(BF16)
        q_ref[...] = q
        do_ref[...] = d
        q2, d2 = split_heads(q), split_heads(d)
        place(z_scr, 0, i, q2, wk_ref)
        place(z_scr, 1, i, d2, wv_ref)
        bias = dot(d2, jnp.broadcast_to(pair_of(vec_ref, 3, i).astype(BF16), (PAIR, PAIR)), NT)
        half = bias.shape[0] // 2
        n_tok = half // n_seq
        at = pl.ds(pl.multiple_of(i * 2 * n_tok, 2 * n_tok), 2 * n_tok)
        r_scr[:, at, :] = jnp.concatenate([bias[:half].reshape(n_seq, n_tok, PAIR), bias[half:].reshape(n_seq, n_tok, PAIR)], axis=1)

    @pl.when(i >= n_first)
    def _():
        for j in range(m_ref.shape[0]):
            b = (i - n_first) * m_ref.shape[0] + j
            t = dot(m_ref[j], z_scr[b].reshape(2 * rows, width), NT)
            s = t[:, :rows] * scale
            dp = t[:, rows:] + r_scr[b].T[0:1, :]
            mx = jnp.max(s, axis=0, keepdims=True)
            e = jnp.exp(s - mx)
            e_ref[j] = e
            dp_ref[j] = dp
            st_ref[0, pl.ds(b, 1), :] = mx
            st_ref[1, pl.ds(b, 1), :] = jnp.sum(e, axis=0, keepdims=True)
            st_ref[2, pl.ds(b, 1), :] = jnp.sum(e * dp, axis=0, keepdims=True)


def stats_kernel(n_cp, st_ref, out_ref, buf, send_sem, recv_sem):
    me = lax.axis_index("cp")
    peers = [lax.rem(me + d, n_cp) for d in range(1, n_cp)]
    barrier = pltpu.get_barrier_semaphore()
    for peer in peers:
        pl.semaphore_signal(barrier, inc=1, device_id={"cp": peer}, device_id_type=pl.DeviceIdType.MESH)
    pl.semaphore_wait(barrier, n_cp - 1)
    copies = []
    for k, peer in enumerate(peers):
        copies.append(pltpu.make_async_remote_copy(
            src_ref=st_ref, dst_ref=buf.at[k], send_sem=send_sem.at[k], recv_sem=recv_sem.at[k],
            device_id={"cp": peer}, device_id_type=pl.DeviceIdType.MESH))
    for c in copies:
        c.start()
    for k, c in enumerate(copies):
        c.wait()
    out_ref[...] = buf[...]


def grad_kernel(scale, n_first, core_ref, m_ref, e_ref, dp_ref, st_ref, other_ref,
                q_ref, do_ref, wk_ref, wv_ref, vec_ref,
                pg_ref, mine_ref, theirs_ref, o_ref, dq_ref, dbv_ref, gp_scr, ps_scr):
    i = pl.program_id(0)
    n_heads, rows = gp_scr.shape[1], e_ref.shape[-1]
    n_tok = rows // n_heads
    n_blk, _, width = m_ref.shape

    @pl.when(i < n_first)
    def _():
        ones = jnp.ones((m_ref.shape[1], PAIR), BF16)
        for half in range(n_blk // 2):
            parts, sums = [], []
            for j in (2 * half, 2 * half + 1):
                b = pl.ds(i * n_blk + j, 1)
                tops = [st_ref[0, b, :]] + [other_ref[k, 0, b, :] for k in range(other_ref.shape[0])]
                sums_l = [st_ref[1, b, :]] + [other_ref[k, 1, b, :] for k in range(other_ref.shape[0])]
                sums_c = [st_ref[2, b, :]] + [other_ref[k, 2, b, :] for k in range(other_ref.shape[0])]
                top = functools.reduce(jnp.maximum, tops)
                fac = [jnp.exp(t - top) for t in tops]
                total = functools.reduce(jnp.add, [f * v for f, v in zip(fac, sums_l)])
                c = functools.reduce(jnp.add, [f * v for f, v in zip(fac, sums_c)]) / total
                p = e_ref[j] * (fac[0] / total)
                g = p * (dp_ref[j] - c) * scale
                pg = jnp.concatenate([g.astype(BF16), p.astype(BF16)], axis=1)
                pg_ref[j] = pg
                parts.append(dot(pg, m_ref[j], TN).reshape(2, n_heads, n_tok, width))
                sums.append(dot(pg[:, rows:], ones, TN).reshape(n_heads, n_tok, PAIR))
            at = pl.ds(pl.multiple_of((i * n_blk + 2 * half) * n_tok, 2 * n_tok), 2 * n_tok)
            gp_scr[:, :, at, :] = jnp.concatenate(parts, axis=2).astype(BF16)
            ps_scr[:, at, :] = jnp.concatenate(sums, axis=1)

    @pl.when(i >= n_first)
    def _():
        k = i - n_first
        n_rows = gp_scr.shape[2]
        gm = gp_scr[0, pl.ds(2 * k, 2)].reshape(2 * n_rows, width)
        pm = gp_scr[1, pl.ds(2 * k, 2)].reshape(2 * n_rows, width)
        ps = join_heads(ps_scr[pl.ds(2 * k, 2)].reshape(2 * n_rows, PAIR))
        dwk = dot(gm, split_heads(q_ref[...]), TN)
        dwv = dot(pm, split_heads(do_ref[...]), TN)
        first = core_ref[0] == 0
        mine_ref[...] = jnp.where(first, dwk, dwv)
        theirs_ref[...] = jnp.where(first, dwv, dwk)
        dq_ref[...] = join_heads(dot(gm, wk_ref[...], NN))
        o_ref[...] = join_heads(dot(pm, wv_ref[...], NN)) + ps * pair_of(vec_ref, 3, k)
        dbv_ref[...] = jnp.broadcast_to(jnp.sum(ps * do_ref[...].astype(F32), axis=0, keepdims=True), dbv_ref.shape)


def mem_kernel(n_first, q_ref, do_ref, wk_ref, wv_ref, pg_ref, dm_ref, z_scr):
    i = pl.program_id(0)
    n_seq, _, rows, width = z_scr.shape

    @pl.when(i < n_first)
    def _():
        place(z_scr, 0, i, split_heads(q_ref[...]), wk_ref)
        place(z_scr, 1, i, split_heads(do_ref[...]), wv_ref)

    @pl.when(i >= n_first)
    def _():
        for j in range(pg_ref.shape[0]):
            b = (i - n_first) * pg_ref.shape[0] + j
            dm_ref[j] = dot(pg_ref[j], z_scr[b].reshape(2 * rows, width), NN).astype(BF16)


def params():
    return pltpu.CompilerParams(dimension_semantics=("arbitrary",), vmem_limit_bytes=VMEM_LIMIT)


def solution(mesh):
    act_spec = P("dp", None, None)
    mem_spec = P("dp", "cp", None)
    vec_out = P("dp")
    mat_out = P("dp", None)
    in_specs = (act_spec, mem_spec, P(), P(), P(), P(), P(), P(), P(), P(), P(), act_spec)
    out_specs = (act_spec, act_spec, mem_spec, vec_out, vec_out, mat_out, vec_out, mat_out, mat_out, vec_out, mat_out, vec_out)
    n_cp = mesh.shape["cp"]

    def swap(x, bit):
        return lax.ppermute(x, "cp", [(i, i ^ bit) for i in range(n_cp)])

    def device_step(hidden, memory, ln_gain, ln_bias, w_q, b_q, w_k, w_v, b_v, w_o, b_o, grad_y):
        n_seq, n_tok, width = hidden.shape
        n_fr = memory.shape[1]
        n_heads = width // HEAD
        n_pairs = n_heads // 2
        rows = n_heads * n_tok
        tokens = n_seq * n_tok
        scale = HEAD ** -0.5
        core = lax.axis_index("cp") % 2
        h2, gy2 = hidden.reshape(tokens, width), grad_y.reshape(tokens, width)
        vecs = jnp.stack([ln_gain, ln_bias, b_q, b_v]).astype(F32)
        full = lambda *s: pl.BlockSpec(s, lambda i: (0,) * len(s))
        blk = 4
        n_late = n_seq // blk
        col = lambda r: pl.BlockSpec((r, PAIR), lambda i: (0, jnp.minimum(i, n_pairs - 1)))
        seq = lambda *s: pl.BlockSpec((blk,) + s, lambda i: (jnp.maximum(i - n_pairs, 0), 0, 0))
        z_scr = pltpu.VMEM((n_seq, 2, rows, width), BF16)

        q, d_o, e, dp, st = pl.pallas_call(
            functools.partial(score_kernel, scale, n_pairs), grid=(n_pairs + n_late,), name="score",
            in_specs=[full(tokens, width), full(tokens, width), full(4, width), col(width),
                      col(width), col(width),
                      pl.BlockSpec((PAIR, width), lambda i: (jnp.minimum(i, n_pairs - 1), 0)), seq(n_fr, width)],
            out_specs=[col(tokens), col(tokens), seq(n_fr, rows), seq(n_fr, rows), full(3, n_seq, rows)],
            out_shape=[jax.ShapeDtypeStruct((tokens, width), BF16), jax.ShapeDtypeStruct((tokens, width), BF16),
                       jax.ShapeDtypeStruct((n_seq, n_fr, rows), F32), jax.ShapeDtypeStruct((n_seq, n_fr, rows), F32),
                       jax.ShapeDtypeStruct((3, n_seq, rows), F32)],
            scratch_shapes=[pltpu.VMEM((tokens, width), BF16), z_scr, pltpu.VMEM((n_seq, rows, PAIR), F32)],
            compiler_params=params(),
        )(h2, gy2, vecs, w_q, w_k, w_v, w_o, memory)

        others = pl.pallas_call(
            functools.partial(stats_kernel, n_cp), name="stats",
            in_specs=[pl.BlockSpec(memory_space=pltpu.VMEM)], out_specs=pl.BlockSpec(memory_space=pltpu.VMEM),
            out_shape=jax.ShapeDtypeStruct((n_cp - 1,) + st.shape, F32),
            scratch_shapes=[pltpu.VMEM((n_cp - 1,) + st.shape, F32), pltpu.SemaphoreType.DMA((n_cp - 1,)),
                            pltpu.SemaphoreType.DMA((n_cp - 1,))],
            compiler_params=pltpu.CompilerParams(collective_id=0, has_side_effects=True),
        )(st)

        two = lambda *s: pl.BlockSpec((blk,) + s, lambda i: (jnp.minimum(i, n_late - 1), 0, 0))
        late = lambda r_: pl.BlockSpec((r_, PAIR), lambda i: (0, jnp.maximum(i - n_late, 0)))
        pg, mine, theirs, o_part, dq_part, dbv_part = pl.pallas_call(
            functools.partial(grad_kernel, scale, n_late), grid=(n_late + n_pairs,), name="grad",
            in_specs=[pl.BlockSpec(memory_space=pltpu.SMEM), two(n_fr, width), two(n_fr, rows), two(n_fr, rows),
                      full(*st.shape), full(*others.shape)]
            + [late(tokens), late(tokens), late(width), late(width), full(4, width)],
            out_specs=[two(n_fr, 2 * rows), late(width), late(width), late(tokens), late(tokens), late(8)],
            out_shape=[jax.ShapeDtypeStruct((n_seq, n_fr, 2 * rows), BF16),
                       jax.ShapeDtypeStruct((width, width), F32), jax.ShapeDtypeStruct((width, width), F32),
                       jax.ShapeDtypeStruct((tokens, width), F32), jax.ShapeDtypeStruct((tokens, width), F32),
                       jax.ShapeDtypeStruct((8, width), F32)],
            scratch_shapes=[pltpu.VMEM((2, n_heads, tokens, width), BF16), pltpu.VMEM((n_heads, tokens, PAIR), F32)],
            compiler_params=params(),
        )(core.reshape(1).astype(jnp.int32), memory, e, dp, st, others, q, d_o, w_k, w_v, vecs)

        me = lax.axis_index("cp")
        both = jnp.stack([o_part, dq_part]).reshape(2, 2, 2, tokens // 4, width)
        give = lax.dynamic_index_in_dim(both, 1 - me % 2, 2, keepdims=False)
        keep = lax.dynamic_index_in_dim(both, me % 2, 2, keepdims=False)
        half = keep + swap(give, 1)
        give = lax.dynamic_index_in_dim(half, 1 - me // 2, 1, keepdims=False)
        keep = lax.dynamic_index_in_dim(half, me // 2, 1, keepdims=False)
        done = keep + swap(give, 2)
        dbq_part = jnp.sum(done[1], axis=0)
        low = done.astype(BF16)
        small = jnp.stack([dbq_part, dbv_part[0]])
        small = small + swap(small, 1)
        small = small + swap(small, 2)
        grad_bq, grad_bv = small[0], small[1]
        mate = swap(low, 2)
        pair = jnp.where(me // 2 == 0, jnp.stack([low, mate], 1), jnp.stack([mate, low], 1))
        mate = swap(pair, 1)
        quad = jnp.where(me % 2 == 0, jnp.stack([pair, mate], 2), jnp.stack([mate, pair], 2))
        attn_out = quad[0].reshape(tokens, width)
        dq_low = quad[1].reshape(tokens, width)

        n_chunk = 4
        step = width // n_chunk
        dwk, dwv, got = [], [], []
        for k in range(n_chunk):
            sl = slice(k * step, (k + 1) * step)
            chip = mine[sl] + swap(theirs[sl], 1)
            if k >= 1:
                chip, _, _ = lax.optimization_barrier((chip, quad if k > 1 else done, got[max(k - 2, 0)] if k > 1 else done))
            got.append(swap(chip, 2))
            fin = chip + got[-1]
            other = swap(fin, 1)
            dwk.append(jnp.where(core == 0, fin, other))
            dwv.append(jnp.where(core == 0, other, fin))
        grad_wk = jnp.concatenate(dwk, axis=0)
        grad_wv = jnp.concatenate(dwv, axis=0)

        hidden_f32 = h2.astype(F32)
        centered = hidden_f32 - jnp.mean(hidden_f32, axis=-1, keepdims=True)
        inv_std = lax.rsqrt(jnp.mean(centered * centered, axis=-1, keepdims=True) + EPS)
        x_hat = centered * inv_std
        gain_f32 = ln_gain.astype(F32)
        x_norm = (x_hat * gain_f32 + ln_bias.astype(F32)).astype(BF16)
        out_y = (hidden_f32 + dot(attn_out, w_o, NN) + b_o.astype(F32)).astype(BF16)
        grad_wo = dot(attn_out, gy2, TN)
        grad_bo = jnp.sum(gy2, axis=0, dtype=F32)
        grad_wq = dot(x_norm, dq_low, TN)
        d_xnorm = dot(dq_low, w_q, NT)
        grad_ln_gain = jnp.sum(d_xnorm * x_hat, axis=0)
        grad_ln_bias = jnp.sum(d_xnorm, axis=0)
        d_hat = d_xnorm * gain_f32
        d_hidden = inv_std * (d_hat - jnp.mean(d_hat, axis=-1, keepdims=True) - x_hat * jnp.mean(d_hat * x_hat, axis=-1, keepdims=True))
        grad_h = (gy2.astype(F32) + d_hidden).astype(BF16)

        grad_mem = pl.pallas_call(
            functools.partial(mem_kernel, n_pairs), grid=(n_pairs + n_late,), name="mem",
            in_specs=[col(tokens), col(tokens), col(width), col(width), seq(n_fr, 2 * rows)], out_specs=seq(n_fr, width),
            out_shape=jax.ShapeDtypeStruct((n_seq, n_fr, width), BF16), compiler_params=params(), scratch_shapes=[z_scr],
            cost_estimate=pl.CostEstimate(flops=8 * n_seq * n_fr * rows * width, bytes_accessed=40 << 20, transcendentals=0),
        )(q, d_o, w_k, w_v, pg)
        return (out_y.reshape(hidden.shape), grad_h.reshape(hidden.shape), grad_mem, grad_ln_gain, grad_ln_bias,
                grad_wq, grad_bq, grad_wk, grad_wv, grad_bv, grad_wo, grad_bo)

    return jax.shard_map(device_step, mesh=mesh, in_specs=in_specs, out_specs=out_specs, check_vma=False)
```

```python
import functools

import jax
import jax.numpy as jnp
from jax import lax
from jax.experimental import pallas as pl
from jax.experimental.pallas import tpu as pltpu
from jax.sharding import PartitionSpec as P

EPS = 1e-5
HEAD = 64
PAIR = 2 * HEAD
F32 = jnp.float32
BF16 = jnp.bfloat16
NT = (((1,), (1,)), ((), ()))
TN = (((0,), (0,)), ((), ()))
NN = (((1,), (0,)), ((), ()))
VMEM_LIMIT = 60 * 1024 * 1024


def dot(a, b, dims):
    return lax.dot_general(a, b, dims, preferred_element_type=F32)


def split_heads(x):
    low = lax.broadcasted_iota(jnp.int32, x.shape, 1) < HEAD
    zero = jnp.zeros_like(x)
    return jnp.concatenate([jnp.where(low, x, zero), jnp.where(low, zero, x)], axis=0)


def join_heads(x):
    rows = x.shape[0] // 2
    low = lax.broadcasted_iota(jnp.int32, (rows, x.shape[1]), 1) < HEAD
    return jnp.where(low, x[:rows], x[rows:])


def normalize(h_ref, vec_ref, x_scr):
    h = h_ref[...].astype(F32)
    c = h - jnp.mean(h, axis=-1, keepdims=True)
    inv = lax.rsqrt(jnp.mean(c * c, axis=-1, keepdims=True) + EPS)
    x_scr[...] = (c * inv * vec_ref[0:1, :] + vec_ref[1:2, :]).astype(BF16)


def pair_of(vec_ref, row, i):
    return vec_ref[row:row + 1, pl.ds(pl.multiple_of(i * PAIR, PAIR), PAIR)]


def place(z_scr, part, i, x, w_ref):
    n_seq = z_scr.shape[0]
    half = x.shape[0] // 2
    n_tok = half // n_seq
    step = 256
    at = pl.ds(pl.multiple_of(i * 2 * n_tok, 2 * n_tok), 2 * n_tok)
    for j in range(0, w_ref.shape[0], step):
        t = dot(x, w_ref[j:j + step, :], NT)
        t = jnp.concatenate([t[:half].reshape(n_seq, n_tok, step), t[half:].reshape(n_seq, n_tok, step)], axis=1)
        z_scr[:, part, at, j:j + step] = t.astype(BF16)


def score_kernel(scale, n_first, h_ref, gy_ref, vec_ref, wq_ref, wk_ref, wv_ref, wo_ref, m_ref,
                 q_ref, do_ref, e_ref, dp_ref, st_ref, x_scr, z_scr, r_scr):
    i = pl.program_id(0)
    n_seq, _, rows, width = z_scr.shape

    @pl.when(i == 0)
    def _():
        normalize(h_ref, vec_ref, x_scr)

    @pl.when(i < n_first)
    def _():
        q = (dot(x_scr[...], wq_ref[...], NN) + pair_of(vec_ref, 2, i)).astype(BF16)
        d = dot(gy_ref[...], wo_ref[...], NT).astype(BF16)
        q_ref[...] = q
        do_ref[...] = d
        q2, d2 = split_heads(q), split_heads(d)
        place(z_scr, 0, i, q2, wk_ref)
        place(z_scr, 1, i, d2, wv_ref)
        bias = dot(d2, jnp.broadcast_to(pair_of(vec_ref, 3, i).astype(BF16), (PAIR, PAIR)), NT)
        half = bias.shape[0] // 2
        n_tok = half // n_seq
        at = pl.ds(pl.multiple_of(i * 2 * n_tok, 2 * n_tok), 2 * n_tok)
        r_scr[:, at, :] = jnp.concatenate([bias[:half].reshape(n_seq, n_tok, PAIR), bias[half:].reshape(n_seq, n_tok, PAIR)], axis=1)

    @pl.when(i >= n_first)
    def _():
        for j in range(m_ref.shape[0]):
            b = (i - n_first) * m_ref.shape[0] + j
            t = dot(m_ref[j], z_scr[b].reshape(2 * rows, width), NT)
            s = t[:, :rows] * scale
            dp = t[:, rows:] + r_scr[b].T[0:1, :]
            mx = jnp.max(s, axis=0, keepdims=True)
            e = jnp.exp(s - mx)
            e_ref[j] = e
            dp_ref[j] = dp
            st_ref[0, pl.ds(b, 1), :] = mx
            st_ref[1, pl.ds(b, 1), :] = jnp.sum(e, axis=0, keepdims=True)
            st_ref[2, pl.ds(b, 1), :] = jnp.sum(e * dp, axis=0, keepdims=True)


def send(src, dst, sems, k, peer):
    return pltpu.make_async_remote_copy(
        src_ref=src, dst_ref=dst, send_sem=sems[0].at[k], recv_sem=sems[1].at[k],
        device_id={"cp": peer}, device_id_type=pl.DeviceIdType.MESH)


def grad_kernel(scale, n_first, n_cp, m_ref, e_ref, dp_ref, st_ref, q_ref, do_ref, wk_ref, wv_ref, vec_ref,
                pg_ref, chip0_ref, chip1_ref, chip2_ref, chip3_ref, oq_ref, small_ref,
                gp_scr, ps_scr, other, mine_oq, theirs_oq, got_oq, keep_x, give_x, got_x, full_oq, small_scr,
                mine_dw, theirs_dw, got_dw,
                st_s, st_r, rd_s, rd_r, rx_s, rx_r, ax_s, ax_r, ad_s, ad_r, dw_s, dw_r, sm_s, sm_r):
    i = pl.program_id(0)
    n_heads, rows = gp_scr.shape[1], e_ref.shape[-1]
    n_tok = rows // n_heads
    n_blk, _, width = m_ref.shape
    n_pairs = n_heads // 2
    quarter = keep_x.shape[2]
    halves = [slice(0, n_pairs // 2), slice(n_pairs // 2, n_pairs)]
    me = lax.axis_index("cp")
    core = lax.rem(me, 2)
    chip = lax.div(me, 2)
    mate = me + 1 - 2 * core
    across = me + 2 - 4 * chip
    first = core == 0
    left = chip == 0
    peers = [lax.rem(me + d, n_cp) for d in range(1, n_cp)]
    at_b, at_c = n_first, n_first + n_pairs
    at_end = at_c + n_pairs

    def stats_copy(k):
        return send(st_ref, other.at[k], (st_s, st_r), k, peers[k])

    def oq_mate(h):
        return send(theirs_oq.at[halves[h]], got_oq.at[halves[h]], (rd_s, rd_r), h, mate)

    def oq_across(h):
        return send(give_x.at[halves[h]], got_x.at[halves[h]], (rx_s, rx_r), h, across)

    def own_across(h):
        at = pl.ds(pl.multiple_of((2 * core + chip) * quarter, quarter), quarter)
        return send(full_oq.at[halves[h], :, at, :], full_oq.at[halves[h], :, at, :], (ax_s, ax_r), h, across)

    def half_mate(h):
        at = pl.ds(pl.multiple_of(core * 2 * quarter, quarter), 2 * quarter)
        return send(full_oq.at[halves[h], :, at, :], full_oq.at[halves[h], :, at, :], (ad_s, ad_r), h, mate)

    def dw_mate(k):
        return send(theirs_dw.at[k], got_dw.at[k], (dw_s, dw_r), k, mate)

    def small_copy(k):
        return send(small_scr.at[me], small_scr.at[me], (sm_s, sm_r), k, peers[k])

    def add_mate(h):
        c = oq_mate(h)
        c.wait()
        t = mine_oq[halves[h]] + got_oq[halves[h]]
        top, bottom = t[:, :, :quarter], t[:, :, quarter:]
        keep_x[halves[h]] = jnp.where(left, top, bottom)
        give_x[halves[h]] = jnp.where(left, bottom, top)

    def finish(h):
        c = oq_across(h)
        c.wait()
        t = keep_x[halves[h]] + got_x[halves[h]]
        at = pl.ds(pl.multiple_of((2 * core + chip) * quarter, quarter), quarter)
        full_oq[halves[h], :, at, :] = t.astype(BF16)
        small_scr[me, 0, halves[h], :] = jnp.sum(t[:, 1], axis=1)

    @pl.when(i == 0)
    def _():
        barrier = pltpu.get_barrier_semaphore()
        for peer in peers:
            pl.semaphore_signal(barrier, inc=1, device_id={"cp": peer}, device_id_type=pl.DeviceIdType.MESH)
        pl.semaphore_wait(barrier, n_cp - 1)
        for k in range(n_cp - 1):
            stats_copy(k).start()
        for k in range(n_cp - 1):
            stats_copy(k).wait()

    @pl.when(i < n_first)
    def _():
        ones = jnp.ones((m_ref.shape[1], PAIR), BF16)
        for half in range(n_blk // 2):
            parts, sums = [], []
            for j in (2 * half, 2 * half + 1):
                b = pl.ds(i * n_blk + j, 1)
                tops = [st_ref[0, b, :]] + [other[k, 0, b, :] for k in range(n_cp - 1)]
                sums_l = [st_ref[1, b, :]] + [other[k, 1, b, :] for k in range(n_cp - 1)]
                sums_c = [st_ref[2, b, :]] + [other[k, 2, b, :] for k in range(n_cp - 1)]
                top = functools.reduce(jnp.maximum, tops)
                fac = [jnp.exp(t - top) for t in tops]
                total = functools.reduce(jnp.add, [f * v for f, v in zip(fac, sums_l)])
                c = functools.reduce(jnp.add, [f * v for f, v in zip(fac, sums_c)]) / total
                p = e_ref[j] * (fac[0] / total)
                g = p * (dp_ref[j] - c) * scale
                pg = jnp.concatenate([g.astype(BF16), p.astype(BF16)], axis=1)
                pg_ref[j] = pg
                parts.append(dot(pg, m_ref[j], TN).reshape(2, n_heads, n_tok, width))
                sums.append(dot(pg[:, rows:], ones, TN).reshape(n_heads, n_tok, PAIR))
            at = pl.ds(pl.multiple_of((i * n_blk + 2 * half) * n_tok, 2 * n_tok), 2 * n_tok)
            gp_scr[:, :, at, :] = jnp.concatenate(parts, axis=2).astype(BF16)
            ps_scr[:, at, :] = jnp.concatenate(sums, axis=1)

    n_rows = gp_scr.shape[2]

    def stacked(part, k):
        return gp_scr[part, pl.ds(2 * k, 2)].reshape(2 * n_rows, width)

    @pl.when((i >= at_b) & (i < at_c))
    def _():
        k = i - at_b
        ps = join_heads(ps_scr[pl.ds(2 * k, 2)].reshape(2 * n_rows, PAIR))
        o = join_heads(dot(stacked(1, k), wv_ref[...], NN)) + ps * pair_of(vec_ref, 3, k)
        dq = join_heads(dot(stacked(0, k), wk_ref[...], NN))
        for part, t in enumerate((o, dq)):
            top, bottom = t[:n_rows // 2], t[n_rows // 2:]
            mine_oq[k, part] = jnp.where(first, top, bottom)
            theirs_oq[k, part] = jnp.where(first, bottom, top)

    @pl.when((i >= at_c) & (i < at_end))
    def _():
        k = i - at_c
        ps = join_heads(ps_scr[pl.ds(2 * k, 2)].reshape(2 * n_rows, PAIR))
        small_scr[me, 1, pl.ds(k, 1), :] = jnp.sum(ps * do_ref[...].astype(F32), axis=0, keepdims=True)
        dwk = dot(stacked(0, k), split_heads(q_ref[...]), TN)
        dwv = dot(stacked(1, k), split_heads(do_ref[...]), TN)
        mine_dw[k] = jnp.where(first, dwk, dwv)
        theirs_dw[k] = jnp.where(first, dwv, dwk)

    @pl.when((i >= at_c + 1) & (i < at_end + 1))
    def _():
        dw_mate(i - at_c - 1).start()

    @pl.when((i >= at_c + 4) & (i < at_end + 4))
    def _():
        k = i - at_c - 4
        dw_mate(k).wait()
        t = mine_dw[k] + got_dw[k]
        at = 0
        for ref in (chip0_ref, chip1_ref, chip2_ref, chip3_ref):
            ref[...] = t[at:at + ref.shape[0]]
            at += ref.shape[0]

    @pl.when(i == at_b + n_pairs // 2)
    def _():
        oq_mate(0).start()

    @pl.when(i == at_c - 1)
    def _():
        add_mate(0)

    @pl.when(i == at_c)
    def _():
        oq_across(0).start()
        oq_mate(1).start()

    @pl.when(i == at_c + 3)
    def _():
        add_mate(1)

    @pl.when(i == at_c + 4)
    def _():
        oq_across(1).start()

    @pl.when(i == at_end + 2)
    def _():
        finish(0)

    @pl.when(i == at_end + 3)
    def _():
        own_across(0).start()

    @pl.when(i == at_end + 4)
    def _():
        finish(1)

    @pl.when(i == at_end + 5)
    def _():
        own_across(1).start()
        for k in range(n_cp - 1):
            small_copy(k).start()
        own_across(0).wait()
        half_mate(0).start()
        own_across(1).wait()
        half_mate(1).start()
        for k in range(n_cp - 1):
            small_copy(k).wait()
        half_mate(0).wait()
        half_mate(1).wait()
        for k in range(n_pairs):
            oq_ref[:, :, k * PAIR:(k + 1) * PAIR] = full_oq[k]
        small_ref[...] = small_scr[0] + small_scr[1] + small_scr[2] + small_scr[3]


def mem_kernel(n_first, q_ref, do_ref, wk_ref, wv_ref, pg_ref, dm_ref, z_scr):
    i = pl.program_id(0)
    n_seq, _, rows, width = z_scr.shape

    @pl.when(i < n_first)
    def _():
        place(z_scr, 0, i, split_heads(q_ref[...]), wk_ref)
        place(z_scr, 1, i, split_heads(do_ref[...]), wv_ref)

    @pl.when(i >= n_first)
    def _():
        for j in range(pg_ref.shape[0]):
            b = (i - n_first) * pg_ref.shape[0] + j
            dm_ref[j] = dot(pg_ref[j], z_scr[b].reshape(2 * rows, width), NN).astype(BF16)


def params():
    return pltpu.CompilerParams(dimension_semantics=("arbitrary",), vmem_limit_bytes=VMEM_LIMIT)


def solution(mesh):
    act_spec = P("dp", None, None)
    mem_spec = P("dp", "cp", None)
    vec_out = P("dp")
    mat_out = P("dp", None)
    in_specs = (act_spec, mem_spec, P(), P(), P(), P(), P(), P(), P(), P(), P(), act_spec)
    out_specs = (act_spec, act_spec, mem_spec, vec_out, vec_out, mat_out, vec_out, mat_out, mat_out, vec_out, mat_out, vec_out)
    n_cp = mesh.shape["cp"]

    def swap(x, bit):
        return lax.ppermute(x, "cp", [(i, i ^ bit) for i in range(n_cp)])

    def device_step(hidden, memory, ln_gain, ln_bias, w_q, b_q, w_k, w_v, b_v, w_o, b_o, grad_y):
        n_seq, n_tok, width = hidden.shape
        n_fr = memory.shape[1]
        n_heads = width // HEAD
        n_pairs = n_heads // 2
        rows = n_heads * n_tok
        tokens = n_seq * n_tok
        scale = HEAD ** -0.5
        core = lax.axis_index("cp") % 2
        h2, gy2 = hidden.reshape(tokens, width), grad_y.reshape(tokens, width)
        vecs = jnp.stack([ln_gain, ln_bias, b_q, b_v]).astype(F32)
        full = lambda *s: pl.BlockSpec(s, lambda i: (0,) * len(s))
        blk = 4
        n_late = n_seq // blk
        col = lambda r: pl.BlockSpec((r, PAIR), lambda i: (0, jnp.minimum(i, n_pairs - 1)))
        seq = lambda *s: pl.BlockSpec((blk,) + s, lambda i: (jnp.maximum(i - n_pairs, 0), 0, 0))
        z_scr = pltpu.VMEM((n_seq, 2, rows, width), BF16)

        q, d_o, e, dp, st = pl.pallas_call(
            functools.partial(score_kernel, scale, n_pairs), grid=(n_pairs + n_late,), name="score",
            in_specs=[full(tokens, width), full(tokens, width), full(4, width), col(width),
                      col(width), col(width),
                      pl.BlockSpec((PAIR, width), lambda i: (jnp.minimum(i, n_pairs - 1), 0)), seq(n_fr, width)],
            out_specs=[col(tokens), col(tokens), seq(n_fr, rows), seq(n_fr, rows), full(3, n_seq, rows)],
            out_shape=[jax.ShapeDtypeStruct((tokens, width), BF16), jax.ShapeDtypeStruct((tokens, width), BF16),
                       jax.ShapeDtypeStruct((n_seq, n_fr, rows), F32), jax.ShapeDtypeStruct((n_seq, n_fr, rows), F32),
                       jax.ShapeDtypeStruct((3, n_seq, rows), F32)],
            scratch_shapes=[pltpu.VMEM((tokens, width), BF16), z_scr, pltpu.VMEM((n_seq, rows, PAIR), F32)],
            compiler_params=params(),
        )(h2, gy2, vecs, w_q, w_k, w_v, w_o, memory)

        first_seq = lambda *s: pl.BlockSpec((blk,) + s, lambda i: (jnp.minimum(i, n_late - 1), 0, 0))
        pair_at = lambda i, start: jnp.clip(i - start, 0, n_pairs - 1)
        at_b = lambda r_: pl.BlockSpec((r_, PAIR), lambda i: (0, pair_at(i, n_late)))
        at_c = lambda r_: pl.BlockSpec((r_, PAIR), lambda i: (0, pair_at(i, n_late + n_pairs)))
        at_d = lambda r_: pl.BlockSpec((r_, PAIR), lambda i: (0, pair_at(i, n_late + n_pairs + 4)))
        chunks = [width * 5 // 16, width * 5 // 16, width // 4, width // 8]
        quarter = tokens // 4
        sems = lambda n: [pltpu.SemaphoreType.DMA((n,))] * 2
        vm = lambda dt, *s: pltpu.VMEM(s, dt)
        pg, *rest = pl.pallas_call(
            functools.partial(grad_kernel, scale, n_late, n_cp), grid=(n_late + 2 * n_pairs + 6,), name="grad",
            in_specs=[first_seq(n_fr, width), first_seq(n_fr, rows), first_seq(n_fr, rows), full(*st.shape),
                      at_c(tokens), at_c(tokens), at_b(width), at_b(width), full(4, width)],
            out_specs=[first_seq(n_fr, 2 * rows)] + [at_d(c) for c in chunks] + [full(2, tokens, width), full(2, n_pairs, PAIR)],
            out_shape=[jax.ShapeDtypeStruct((n_seq, n_fr, 2 * rows), BF16)]
            + [jax.ShapeDtypeStruct((c, width), F32) for c in chunks]
            + [jax.ShapeDtypeStruct((2, tokens, width), BF16), jax.ShapeDtypeStruct((2, n_pairs, PAIR), F32)],
            scratch_shapes=[vm(BF16, 2, n_heads, tokens, width), vm(F32, n_heads, tokens, PAIR), vm(F32, n_cp - 1, *st.shape),
                            vm(F32, n_pairs, 2, 2 * quarter, PAIR), vm(F32, n_pairs, 2, 2 * quarter, PAIR),
                            vm(F32, n_pairs, 2, 2 * quarter, PAIR), vm(F32, n_pairs, 2, quarter, PAIR),
                            vm(F32, n_pairs, 2, quarter, PAIR), vm(F32, n_pairs, 2, quarter, PAIR),
                            vm(BF16, n_pairs, 2, tokens, PAIR), vm(F32, n_cp, 2, n_pairs, PAIR),
                            vm(F32, n_pairs, width, PAIR), vm(F32, n_pairs, width, PAIR), vm(F32, n_pairs, width, PAIR)]
            + sems(n_cp - 1) + sems(2) + sems(2) + sems(2) + sems(2) + sems(n_pairs) + sems(n_cp - 1),
            compiler_params=pltpu.CompilerParams(dimension_semantics=("arbitrary",), vmem_limit_bytes=VMEM_LIMIT,
                                                 collective_id=0, has_side_effects=True),
        )(memory, e, dp, st, q, d_o, w_k, w_v, vecs)
        chips, (oq, small) = rest[:4], rest[4:]
        attn_out, dq_low = oq[0], oq[1]
        small = small.reshape(2, width)
        grad_bq, grad_bv = small[0], small[1]

        dwk, dwv = [], []
        for c in chips:
            fin = c + swap(c, 2)
            other = swap(fin, 1)
            dwk.append(jnp.where(core == 0, fin, other))
            dwv.append(jnp.where(core == 0, other, fin))
        grad_wk = jnp.concatenate(dwk, axis=0)
        grad_wv = jnp.concatenate(dwv, axis=0)

        hidden_f32 = h2.astype(F32)
        centered = hidden_f32 - jnp.mean(hidden_f32, axis=-1, keepdims=True)
        inv_std = lax.rsqrt(jnp.mean(centered * centered, axis=-1, keepdims=True) + EPS)
        x_hat = centered * inv_std
        gain_f32 = ln_gain.astype(F32)
        x_norm = (x_hat * gain_f32 + ln_bias.astype(F32)).astype(BF16)
        out_y = (hidden_f32 + dot(attn_out, w_o, NN) + b_o.astype(F32)).astype(BF16)
        grad_wo = dot(attn_out, gy2, TN)
        grad_bo = jnp.sum(gy2, axis=0, dtype=F32)
        grad_wq = dot(x_norm, dq_low, TN)
        d_xnorm = dot(dq_low, w_q, NT)
        grad_ln_gain = jnp.sum(d_xnorm * x_hat, axis=0)
        grad_ln_bias = jnp.sum(d_xnorm, axis=0)
        d_hat = d_xnorm * gain_f32
        d_hidden = inv_std * (d_hat - jnp.mean(d_hat, axis=-1, keepdims=True) - x_hat * jnp.mean(d_hat * x_hat, axis=-1, keepdims=True))
        grad_h = (gy2.astype(F32) + d_hidden).astype(BF16)

        grad_mem = pl.pallas_call(
            functools.partial(mem_kernel, n_pairs), grid=(n_pairs + n_late,), name="mem",
            in_specs=[col(tokens), col(tokens), col(width), col(width), seq(n_fr, 2 * rows)], out_specs=seq(n_fr, width),
            out_shape=jax.ShapeDtypeStruct((n_seq, n_fr, width), BF16), compiler_params=params(), scratch_shapes=[z_scr],
            cost_estimate=pl.CostEstimate(flops=8 * n_seq * n_fr * rows * width, bytes_accessed=40 << 20, transcendentals=0),
        )(q, d_o, w_k, w_v, pg)
        return (out_y.reshape(hidden.shape), grad_h.reshape(hidden.shape), grad_mem, grad_ln_gain, grad_ln_bias,
                grad_wq, grad_bq, grad_wk, grad_wv, grad_bv, grad_wo, grad_bo)

    return jax.shard_map(device_step, mesh=mesh, in_specs=in_specs, out_specs=out_specs, check_vma=False)
```

```python
import functools

import jax
import jax.numpy as jnp
from jax import lax
from jax.experimental import pallas as pl
from jax.experimental.pallas import tpu as pltpu
from jax.sharding import PartitionSpec as P

EPS = 1e-5
HEAD = 64
PAIR = 2 * HEAD
F32 = jnp.float32
BF16 = jnp.bfloat16
NT = (((1,), (1,)), ((), ()))
TN = (((0,), (0,)), ((), ()))
NN = (((1,), (0,)), ((), ()))
VMEM_LIMIT = 67043328


def dot(a, b, dims):
    return lax.dot_general(a, b, dims, preferred_element_type=F32)


def split_heads(x, n_seq):
    x = x.reshape(n_seq, x.shape[0] // n_seq, PAIR)
    low = lax.broadcasted_iota(jnp.int32, x.shape, 2) < HEAD
    zero = jnp.zeros_like(x)
    both = jnp.concatenate([jnp.where(low, x, zero), jnp.where(low, zero, x)], axis=1)
    return both.astype(BF16).reshape(-1, PAIR)


def join_heads(x, n_seq):
    n_tok = x.shape[0] // (2 * n_seq)
    x = x.reshape(n_seq, 2 * n_tok, PAIR)
    low = lax.broadcasted_iota(jnp.int32, (n_seq, n_tok, PAIR), 2) < HEAD
    return jnp.where(low, x[:, :n_tok], x[:, n_tok:]).reshape(n_seq * n_tok, PAIR)


def normalize(h_ref, vec_ref, x_scr):
    h = h_ref[...].astype(F32)
    c = h - jnp.mean(h, axis=-1, keepdims=True)
    inv = lax.rsqrt(jnp.mean(c * c, axis=-1, keepdims=True) + EPS)
    x_scr[...] = (c * inv * vec_ref[0:1, :] + vec_ref[1:2, :]).astype(BF16)


def pair_of(vec_ref, row, i):
    return vec_ref[row:row + 1, pl.ds(pl.multiple_of(i * PAIR, PAIR), PAIR)]


def place(out_ref, part, i, x, weight):
    step = 256
    for j in range(0, out_ref.shape[3], step):
        out_ref[part, i, :, j:j + step] = dot(x, weight(j, step), NT).astype(BF16)


def send(src, dst, sems, k, peer):
    return pltpu.make_async_remote_copy(
        src_ref=src, dst_ref=dst, send_sem=sems[0].at[k], recv_sem=sems[1].at[k],
        device_id={"cp": peer}, device_id_type=pl.DeviceIdType.MESH)


def fused_kernel(scale, n_cp, h_ref, gy_ref, wq_ref, wk_ref, wv_ref, wo_ref, m_ref, gain_ref, bias_ref, bq_ref, bv_ref,
                 pg_ref, chip0_ref, chip1_ref, chip2_ref, chip3_ref, oq_ref, q2_out, d2_out, small_ref,
                 x_scr, gy_scr, vec_scr, zg_scr, m_scr, e_scr, dp_scr, wk_scr, wv_scr, ps_scr, q2_scr, d2_scr, st_scr, other,
                 mine_oq, theirs_oq, got_oq, keep_x, give_x, got_x, full_oq, small_scr, got_dw,
                 in_sem, w_sem, m_sem, q_sem, chip_sem, out_sem,
                 st_s, st_r, rd_s, rd_r, rx_s, rx_r, ax_s, ax_r, ad_s, ad_r, dw_s, dw_r, sm_s, sm_r):
    i = pl.program_id(0)
    _, n_pairs, n_rows, width = zg_scr.shape
    n_seq, n_fr, _ = m_scr.shape
    n_row = n_rows // n_seq
    rows = n_row * n_pairs
    n_blk = n_seq // n_pairs
    quarter = keep_x.shape[2]
    halves = [slice(0, n_pairs // 2), slice(n_pairs // 2, n_pairs)]
    me = lax.axis_index("cp")
    core = lax.rem(me, 2)
    chip = lax.div(me, 2)
    mate = me + 1 - 2 * core
    across = me + 2 - 4 * chip
    first = core == 0
    left = chip == 0
    peers = [lax.rem(me + d, n_cp) for d in range(1, n_cp)]
    at_s, at_a, at_b, at_c, at_end = (n_pairs * k for k in range(1, 6))
    wq_at, wo_at = n_seq - 2 * n_blk, n_seq - n_blk
    per_row = n_fr // PAIR

    def cols(k):
        return pl.ds(pl.multiple_of(k * PAIR, PAIR), PAIR)

    def seq_rows(b):
        return pl.ds(pl.multiple_of(b * n_row, n_row), n_row)

    def wo_rows(k):
        return lax.div(k, per_row), pl.ds(pl.multiple_of(lax.rem(k, per_row) * PAIR, PAIR), PAIR)

    def weight_copies(k):
        c = cols(k)
        block, r = wo_rows(k)
        return [pltpu.make_async_copy(wq_ref.at[:, :, c], m_scr.at[wq_at:wo_at, :, c], w_sem.at[0, k]),
                pltpu.make_async_copy(wo_ref.at[block, r, :], m_scr.at[wo_at + block, r, :], w_sem.at[1, k]),
                pltpu.make_async_copy(wk_ref.at[:, c], wk_scr.at[:, c], w_sem.at[2, k]),
                pltpu.make_async_copy(wv_ref.at[:, c], wv_scr.at[:, c], w_sem.at[3, k])]

    def mem_copy(g):
        at = pl.ds(g * n_blk, n_blk)
        return pltpu.make_async_copy(m_ref.at[at], m_scr.at[at], m_sem.at[g])

    def act_copies():
        return [pltpu.make_async_copy(h_ref, x_scr, in_sem.at[0]), pltpu.make_async_copy(gy_ref, gy_scr, in_sem.at[1])]

    def q_copies():
        return [pltpu.make_async_copy(q2_scr, q2_out, q_sem.at[0]), pltpu.make_async_copy(d2_scr, d2_out, q_sem.at[1])]

    def chip_copies(k):
        out, at = [], 0
        for n, ref in enumerate((chip0_ref, chip1_ref, chip2_ref, chip3_ref)):
            out.append(pltpu.make_async_copy(e_scr.at[k, at:at + ref.shape[0], :], ref.at[:, cols(k)], chip_sem.at[n, k]))
            at += ref.shape[0]
        return out

    def out_copies():
        return [pltpu.make_async_copy(full_oq.at[k, p], oq_ref.at[p, :, k * PAIR:(k + 1) * PAIR], out_sem.at[p, k])
                for k in range(n_pairs) for p in range(2)]

    def stats_copy(k):
        return send(st_scr, other.at[k], (st_s, st_r), k, peers[k])

    def oq_mate(h):
        return send(theirs_oq.at[halves[h]], got_oq.at[halves[h]], (rd_s, rd_r), h, mate)

    def oq_across(h):
        return send(give_x.at[halves[h]], got_x.at[halves[h]], (rx_s, rx_r), h, across)

    def own_across(h):
        at = pl.ds(pl.multiple_of((2 * core + chip) * quarter, quarter), quarter)
        return send(full_oq.at[halves[h], :, at, :], full_oq.at[halves[h], :, at, :], (ax_s, ax_r), h, across)

    def half_mate(h):
        at = pl.ds(pl.multiple_of(core * 2 * quarter, quarter), 2 * quarter)
        return send(full_oq.at[halves[h], :, at, :], full_oq.at[halves[h], :, at, :], (ad_s, ad_r), h, mate)

    def dw_mate(k):
        return send(dp_scr.at[k], got_dw.at[k], (dw_s, dw_r), k, mate)

    def small_copy(k):
        return send(small_scr.at[me], small_scr.at[me], (sm_s, sm_r), k, peers[k])

    def add_mate(h):
        oq_mate(h).wait()
        t = mine_oq[halves[h]] + got_oq[halves[h]]
        top, bottom = t[:, :, :quarter], t[:, :, quarter:]
        keep_x[halves[h]] = jnp.where(left, top, bottom)
        give_x[halves[h]] = jnp.where(left, bottom, top)

    def finish(h):
        oq_across(h).wait()
        t = keep_x[halves[h]] + got_x[halves[h]]
        at = pl.ds(pl.multiple_of((2 * core + chip) * quarter, quarter), quarter)
        full_oq[halves[h], :, at, :] = t.astype(BF16)
        small_scr[me, 0, halves[h], :] = jnp.sum(t[:, 1], axis=1)

    @pl.when(i == 0)
    def _():
        for c in act_copies():
            c.start()

        @pl.loop(0, n_pairs)
        def _(k):
            for c in weight_copies(k):
                c.start()

        barrier = pltpu.get_barrier_semaphore()
        for peer in peers:
            pl.semaphore_signal(barrier, inc=1, device_id={"cp": peer}, device_id_type=pl.DeviceIdType.MESH)
        for k, ref in enumerate((gain_ref, bias_ref, bq_ref, bv_ref)):
            vec_scr[k:k + 1, :] = ref[...].astype(F32).reshape(1, width)
        for c in act_copies():
            c.wait()
        normalize(x_scr, vec_scr, x_scr)

    @pl.when(i < at_s)
    def _():
        @pl.when((i > 0) & (i < n_pairs - 1))
        def _():
            mem_copy(i - 1).start()

        for c in weight_copies(i):
            c.wait()
        block, r = wo_rows(i)
        q = (dot(x_scr[...], m_scr[wq_at:wo_at, :, cols(i)].reshape(width, PAIR), NN) + pair_of(vec_scr, 2, i)).astype(BF16)
        d = dot(gy_scr[...], m_scr[wo_at + block, r, :], NT).astype(BF16)
        q2, d2 = split_heads(q.astype(F32), n_seq), split_heads(d.astype(F32), n_seq)
        q2_scr[i] = q2
        d2_scr[i] = d2
        place(zg_scr, 0, i, q2, lambda j, step: wk_scr[j:j + step, cols(i)])
        place(zg_scr, 1, i, d2, lambda j, step: wv_scr[j:j + step, cols(i)])
        ps_scr[i] = dot(d2, jnp.broadcast_to(pair_of(vec_scr, 3, i).astype(BF16), (PAIR, PAIR)), NT)

    @pl.when(i == at_s)
    def _():
        for g in (n_pairs - 2, n_pairs - 1):
            mem_copy(g).start()
        for c in q_copies():
            c.start()

    @pl.when((i >= at_s) & (i < at_a))
    def _():
        g = i - at_s
        mem_copy(g).wait()
        for j in range(n_blk):
            b = g * n_blk + j
            at = pl.ds(b, 1)
            t = dot(m_scr[b], zg_scr[:, :, seq_rows(b), :].reshape(2 * rows, width), NT)
            s = t[:, :rows] * scale
            dp = t[:, rows:] + ps_scr[:, seq_rows(b), :].reshape(rows, PAIR).T[0:1, :]
            mx = jnp.max(s, axis=0, keepdims=True)
            e = jnp.exp(s - mx)
            e_scr[g, j * n_fr:(j + 1) * n_fr, :] = e
            dp_scr[g, j * n_fr:(j + 1) * n_fr, :] = dp
            st_scr[0, at, :] = mx
            st_scr[1, at, :] = jnp.sum(e, axis=0, keepdims=True)
            st_scr[2, at, :] = jnp.sum(e * dp, axis=0, keepdims=True)

    @pl.when(i == at_a)
    def _():
        pl.semaphore_wait(pltpu.get_barrier_semaphore(), n_cp - 1)
        for k in range(n_cp - 1):
            stats_copy(k).start()
        for k in range(n_cp - 1):
            stats_copy(k).wait()

    @pl.when((i >= at_a) & (i < at_b))
    def _():
        g = i - at_a
        ones = jnp.ones((n_fr, PAIR), BF16)
        for j in range(n_blk):
            b = g * n_blk + j
            at = pl.ds(b, 1)
            tops = [st_scr[0, at, :]] + [other[k, 0, at, :] for k in range(n_cp - 1)]
            sums_l = [st_scr[1, at, :]] + [other[k, 1, at, :] for k in range(n_cp - 1)]
            sums_c = [st_scr[2, at, :]] + [other[k, 2, at, :] for k in range(n_cp - 1)]
            top = functools.reduce(jnp.maximum, tops)
            fac = [jnp.exp(t - top) for t in tops]
            total = functools.reduce(jnp.add, [f * v for f, v in zip(fac, sums_l)])
            c = functools.reduce(jnp.add, [f * v for f, v in zip(fac, sums_c)]) / total
            p = e_scr[g, j * n_fr:(j + 1) * n_fr, :] * (fac[0] / total)
            gr = p * (dp_scr[g, j * n_fr:(j + 1) * n_fr, :] - c) * scale
            pg = jnp.concatenate([gr.astype(BF16), p.astype(BF16)], axis=1)
            pg_ref[j] = pg
            pgt = pg.T
            step = 256
            for w in range(0, width, step):
                t = dot(pgt, m_scr[b, :, w:w + step], NN).astype(BF16)
                zg_scr[:, :, seq_rows(b), w:w + step] = t.reshape(2, n_pairs, n_row, step)
            ps_scr[:, seq_rows(b), :] = dot(pgt[rows:], ones, NN).reshape(n_pairs, n_row, PAIR)

    @pl.when((i >= at_b) & (i < at_c))
    def _():
        k = i - at_b
        o = join_heads(dot(zg_scr[1, k], wv_scr[:, cols(k)], NN), n_seq) + join_heads(ps_scr[k], n_seq) * pair_of(vec_scr, 3, k)
        dq = join_heads(dot(zg_scr[0, k], wk_scr[:, cols(k)], NN), n_seq)
        for part, t in enumerate((o, dq)):
            top, bottom = t[:t.shape[0] // 2], t[t.shape[0] // 2:]
            mine_oq[k, part] = jnp.where(first, top, bottom)
            theirs_oq[k, part] = jnp.where(first, bottom, top)

    @pl.when((i >= at_c) & (i < at_end))
    def _():
        k = i - at_c
        small_scr[me, 1, pl.ds(k, 1), :] = jnp.sum(ps_scr[k] * d2_scr[k].astype(F32), axis=0, keepdims=True)
        dwk = dot(zg_scr[0, k], q2_scr[k], TN)
        dwv = dot(zg_scr[1, k], d2_scr[k], TN)
        e_scr[k] = jnp.where(first, dwk, dwv)
        dp_scr[k] = jnp.where(first, dwv, dwk)

    @pl.when((i >= at_c + 1) & (i < at_end + 1))
    def _():
        dw_mate(i - at_c - 1).start()

    @pl.when((i >= at_c + 4) & (i < at_end + 4))
    def _():
        k = i - at_c - 4
        dw_mate(k).wait()
        e_scr[k] += got_dw[k]

    @pl.when((i >= at_c + 5) & (i < at_end + 5))
    def _():
        for c in chip_copies(i - at_c - 5):
            c.start()

    @pl.when(i == at_b + n_pairs // 2)
    def _():
        oq_mate(0).start()

    @pl.when(i == at_c - 1)
    def _():
        add_mate(0)

    @pl.when(i == at_c)
    def _():
        oq_across(0).start()
        oq_mate(1).start()

    @pl.when(i == at_c + 3)
    def _():
        add_mate(1)

    @pl.when(i == at_c + 4)
    def _():
        oq_across(1).start()

    @pl.when(i == at_end + 2)
    def _():
        finish(0)

    @pl.when(i == at_end + 3)
    def _():
        own_across(0).start()

    @pl.when(i == at_end + 4)
    def _():
        finish(1)

    @pl.when(i == at_end + 5)
    def _():
        own_across(1).start()
        for k in range(n_cp - 1):
            small_copy(k).start()
        own_across(0).wait()
        half_mate(0).start()
        own_across(1).wait()
        half_mate(1).start()
        for k in range(n_cp - 1):
            small_copy(k).wait()
        half_mate(0).wait()
        half_mate(1).wait()
        for c in out_copies():
            c.start()
        small_ref[...] = small_scr[0] + small_scr[1] + small_scr[2] + small_scr[3]

        @pl.loop(0, n_pairs)
        def _(k):
            for c in chip_copies(k):
                c.wait()

        for c in q_copies() + out_copies():
            c.wait()


def assemble_kernel(core_ref, fin_ref, other_ref, *refs):
    wk_ref, wv_ref = refs[-2:]
    first = core_ref[0] == 0
    wk_ref[...] = jnp.where(first, fin_ref[...], other_ref[...])
    wv_ref[...] = jnp.where(first, other_ref[...], fin_ref[...])


def assemble(core, fin, other, at, acc):
    n, width = fin.shape
    step = 192 if n % 192 == 0 and at % 192 == 0 else 64
    block = pl.BlockSpec((step, width), lambda i: (i, 0))
    out = pl.BlockSpec((step, width), lambda i: (at // step + i, 0))
    return pl.pallas_call(
        assemble_kernel, grid=(n // step,), name="assemble",
        in_specs=[pl.BlockSpec(memory_space=pltpu.SMEM), block, block] + [pl.BlockSpec(memory_space=pl.ANY)] * len(acc),
        out_specs=[out, out], out_shape=[jax.ShapeDtypeStruct((width, width), F32)] * 2,
        input_output_aliases={3: 0, 4: 1} if acc else {},
        compiler_params=pltpu.CompilerParams(dimension_semantics=("arbitrary",)),
    )(core, fin, other, *acc)


def mem_kernel(n_first, q2_ref, d2_ref, wk_ref, wv_ref, pg_ref, dm_ref, z_scr):
    i = pl.program_id(0)
    _, n_pairs, n_rows, width = z_scr.shape
    n_blk = pg_ref.shape[0]
    n_row = pg_ref.shape[2] // (2 * n_pairs)

    @pl.when(i < n_first)
    def _():
        place(z_scr, 0, i, q2_ref[0], lambda j, step: wk_ref[j:j + step, :])
        place(z_scr, 1, i, d2_ref[0], lambda j, step: wv_ref[j:j + step, :])

    @pl.when(i >= n_first)
    def _():
        for j in range(n_blk):
            b = (i - n_first) * n_blk + j
            at = pl.ds(pl.multiple_of(b * n_row, n_row), n_row)
            z = z_scr[:, :, at, :].reshape(pg_ref.shape[2], width)
            dm_ref[j] = dot(pg_ref[j], z, NN).astype(BF16)


def params():
    return pltpu.CompilerParams(dimension_semantics=("arbitrary",), vmem_limit_bytes=VMEM_LIMIT)


def solution(mesh):
    act_spec = P("dp", None, None)
    mem_spec = P("dp", "cp", None)
    vec_out = P("dp")
    mat_out = P("dp", None)
    in_specs = (act_spec, mem_spec, P(), P(), P(), P(), P(), P(), P(), P(), P(), act_spec)
    out_specs = (act_spec, act_spec, mem_spec, vec_out, vec_out, mat_out, vec_out, mat_out, mat_out, vec_out, mat_out, vec_out)
    n_cp = mesh.shape["cp"]

    def swap(x, bit):
        return lax.ppermute(x, "cp", [(i, i ^ bit) for i in range(n_cp)])

    def device_step(hidden, memory, ln_gain, ln_bias, w_q, b_q, w_k, w_v, b_v, w_o, b_o, grad_y):
        n_seq, n_tok, width = hidden.shape
        n_fr = memory.shape[1]
        n_heads = width // HEAD
        n_pairs = n_heads // 2
        rows = n_heads * n_tok
        tokens = n_seq * n_tok
        scale = HEAD ** -0.5
        core = lax.axis_index("cp") % 2
        h2, gy2 = hidden.reshape(tokens, width), grad_y.reshape(tokens, width)
        full = lambda *s: pl.BlockSpec(s, lambda i: (0,) * len(s))
        blk = n_seq // n_pairs
        quarter = tokens // 4
        chunks = [width * 3 // 8, width * 3 // 8, width * 3 // 16, width // 16]
        anywhere = pl.BlockSpec(memory_space=pl.ANY)
        vm = lambda dt, *s: pltpu.VMEM(s, dt)
        sems = lambda *n: pltpu.SemaphoreType.DMA(n)
        both = lambda n: [sems(n)] * 2
        pg, *rest = pl.pallas_call(
            functools.partial(fused_kernel, scale, n_cp), grid=(5 * n_pairs + 6,), name="fused",
            in_specs=[anywhere] * 7 + [full(width)] * 4,
            out_specs=[pl.BlockSpec((blk, n_fr, 2 * rows), lambda i: (jnp.clip(i - 2 * n_pairs, 0, n_pairs - 1), 0, 0))]
            + [anywhere] * 7 + [full(2, n_pairs, PAIR)],
            out_shape=[jax.ShapeDtypeStruct((n_seq, n_fr, 2 * rows), BF16)]
            + [jax.ShapeDtypeStruct((c, width), F32) for c in chunks]
            + [jax.ShapeDtypeStruct((2, tokens, width), BF16)]
            + [jax.ShapeDtypeStruct((n_pairs, 2 * tokens, PAIR), BF16)] * 2
            + [jax.ShapeDtypeStruct((2, n_pairs, PAIR), F32)],
            scratch_shapes=[vm(BF16, tokens, width), vm(BF16, tokens, width), vm(F32, 4, width),
                            vm(BF16, 2, n_pairs, 2 * tokens, width), vm(BF16, n_seq, n_fr, width),
                            vm(F32, n_pairs, blk * n_fr, rows), vm(F32, n_pairs, blk * n_fr, rows),
                            vm(BF16, width, width), vm(BF16, width, width), vm(F32, n_pairs, 2 * tokens, PAIR),
                            vm(BF16, n_pairs, 2 * tokens, PAIR), vm(BF16, n_pairs, 2 * tokens, PAIR),
                            vm(F32, 3, n_seq, rows), vm(F32, n_cp - 1, 3, n_seq, rows),
                            vm(F32, n_pairs, 2, 2 * quarter, PAIR), vm(F32, n_pairs, 2, 2 * quarter, PAIR),
                            vm(F32, n_pairs, 2, 2 * quarter, PAIR), vm(F32, n_pairs, 2, quarter, PAIR),
                            vm(F32, n_pairs, 2, quarter, PAIR), vm(F32, n_pairs, 2, quarter, PAIR),
                            vm(BF16, n_pairs, 2, tokens, PAIR), vm(F32, n_cp, 2, n_pairs, PAIR),
                            vm(F32, n_pairs, width, PAIR),
                            sems(2), sems(4, n_pairs), sems(n_pairs), sems(2), sems(4, n_pairs), sems(2, n_pairs)]
            + both(n_cp - 1) + both(2) + both(2) + both(2) + both(2) + both(n_pairs) + both(n_cp - 1),
            compiler_params=pltpu.CompilerParams(dimension_semantics=("arbitrary",), vmem_limit_bytes=VMEM_LIMIT,
                                                 collective_id=0, has_side_effects=True),
        )(h2, gy2, w_q.reshape(blk, n_fr, width), w_k, w_v, w_o.reshape(blk, n_fr, width), memory, ln_gain, ln_bias, b_q, b_v)
        chips, (oq, q2, d2, small) = rest[:4], rest[4:]
        attn_out, dq_low = oq[0], oq[1]
        small = small.reshape(2, width)
        grad_bq, grad_bv = small[0], small[1]

        got = [swap(c, 2) for c in chips]

        hidden_f32 = h2.astype(F32)
        centered = hidden_f32 - jnp.mean(hidden_f32, axis=-1, keepdims=True)
        inv_std = lax.rsqrt(jnp.mean(centered * centered, axis=-1, keepdims=True) + EPS)
        x_hat = centered * inv_std
        gain_f32 = ln_gain.astype(F32)
        x_norm = (x_hat * gain_f32 + ln_bias.astype(F32)).astype(BF16)
        out_y = (hidden_f32 + dot(attn_out, w_o, NN) + b_o.astype(F32)).astype(BF16)
        grad_wo = dot(attn_out, gy2, TN)
        grad_bo = jnp.sum(gy2, axis=0, dtype=F32)
        grad_wq = dot(x_norm, dq_low, TN)
        d_xnorm = dot(dq_low, w_q, NT)
        grad_ln_gain = jnp.sum(d_xnorm * x_hat, axis=0)
        grad_ln_bias = jnp.sum(d_xnorm, axis=0)
        d_hat = d_xnorm * gain_f32
        d_hidden = inv_std * (d_hat - jnp.mean(d_hat, axis=-1, keepdims=True) - x_hat * jnp.mean(d_hat * x_hat, axis=-1, keepdims=True))
        grad_h = (gy2.astype(F32) + d_hidden).astype(BF16)

        pair_block = pl.BlockSpec((1, 2 * tokens, PAIR), lambda i: (jnp.minimum(i, n_pairs - 1), 0, 0))
        col_block = pl.BlockSpec((width, PAIR), lambda i: (0, jnp.minimum(i, n_pairs - 1)))
        late = lambda *s: pl.BlockSpec((blk,) + s, lambda i: (jnp.maximum(i - n_pairs, 0), 0, 0))
        grad_mem = pl.pallas_call(
            functools.partial(mem_kernel, n_pairs), grid=(2 * n_pairs,), name="mem",
            in_specs=[pair_block, pair_block, col_block, col_block, late(n_fr, 2 * rows)], out_specs=late(n_fr, width),
            out_shape=jax.ShapeDtypeStruct((n_seq, n_fr, width), BF16), compiler_params=params(),
            scratch_shapes=[vm(BF16, 2, n_pairs, 2 * tokens, width)],
            cost_estimate=pl.CostEstimate(flops=8 * n_seq * n_fr * rows * width, bytes_accessed=40 << 20, transcendentals=0),
        )(q2, d2, w_k, w_v, pg)

        hidden_work = (out_y, grad_h, grad_mem, grad_ln_gain, grad_ln_bias, grad_wq, grad_wo, grad_bo)
        got[0], hidden_work = lax.optimization_barrier((got[0], hidden_work))
        out_y, grad_h, grad_mem, grad_ln_gain, grad_ln_bias, grad_wq, grad_wo, grad_bo = hidden_work
        core_arr = core.reshape(1).astype(jnp.int32)
        acc, at = (), 0
        for c, g in zip(chips, got):
            g, acc = lax.optimization_barrier((g, acc))
            fin = c + g
            acc = assemble(core_arr, fin, swap(fin, 1), at, acc)
            at += c.shape[0]
        grad_wk, grad_wv = acc
        return (out_y.reshape(hidden.shape), grad_h.reshape(hidden.shape), grad_mem, grad_ln_gain, grad_ln_bias,
                grad_wq, grad_bq, grad_wk, grad_wv, grad_bv, grad_wo, grad_bo)

    return jax.shard_map(device_step, mesh=mesh, in_specs=in_specs, out_specs=out_specs, check_vma=False)
```

```python
import functools

import jax
import jax.numpy as jnp
from jax import lax
from jax.experimental import pallas as pl
from jax.experimental.pallas import tpu as pltpu
from jax.sharding import PartitionSpec as P


EPS = 1e-5
HEAD = 64
PAIR = 2 * HEAD
F32 = jnp.float32
BF16 = jnp.bfloat16
NT = (((1,), (1,)), ((), ()))
TN = (((0,), (0,)), ((), ()))
NN = (((1,), (0,)), ((), ()))
VMEM_LIMIT = 67043328


def dot(a, b, dims):
    return lax.dot_general(a, b, dims, preferred_element_type=F32)


def split_heads(x, n_seq):
    x = x.reshape(n_seq, x.shape[0] // n_seq, PAIR)
    low = lax.broadcasted_iota(jnp.int32, x.shape, 2) < HEAD
    zero = jnp.zeros_like(x)
    both = jnp.concatenate([jnp.where(low, x, zero), jnp.where(low, zero, x)], axis=1)
    return both.astype(BF16).reshape(-1, PAIR)


def join_heads(x, n_seq):
    n_tok = x.shape[0] // (2 * n_seq)
    x = x.reshape(n_seq, 2 * n_tok, PAIR)
    low = lax.broadcasted_iota(jnp.int32, (n_seq, n_tok, PAIR), 2) < HEAD
    return jnp.where(low, x[:, :n_tok], x[:, n_tok:]).reshape(n_seq * n_tok, PAIR)


def normalize(h_ref, vec_ref, x_scr):
    h = h_ref[...].astype(F32)
    c = h - jnp.mean(h, axis=-1, keepdims=True)
    inv = lax.rsqrt(jnp.mean(c * c, axis=-1, keepdims=True) + EPS)
    x_scr[...] = (c * inv * vec_ref[0:1, :] + vec_ref[1:2, :]).astype(BF16)


def pair_of(vec_ref, row, i):
    return vec_ref[row:row + 1, pl.ds(pl.multiple_of(i * PAIR, PAIR), PAIR)]


def place(out_ref, part, i, x, weight):
    step = 256
    for j in range(0, out_ref.shape[3], step):
        out_ref[part, i, :, j:j + step] = dot(x, weight(j, step), NT).astype(BF16)


def send(src, dst, sems, k, peer):
    return pltpu.make_async_remote_copy(
        src_ref=src, dst_ref=dst, send_sem=sems[0].at[k], recv_sem=sems[1].at[k],
        device_id={"cp": peer}, device_id_type=pl.DeviceIdType.MESH)


def fused_kernel(scale, n_cp, h_ref, gy_ref, wq_ref, wk_ref, wv_ref, wo_ref, m_ref, gain_ref, bias_ref, bq_ref, bv_ref,
                 pg_ref, chip0_ref, chip1_ref, chip2_ref, chip3_ref, oq_ref, q2_out, d2_out, small_ref,
                 x_scr, gy_scr, vec_scr, zg_scr, m_scr, e_scr, dp_scr, wk_scr, wv_scr, ps_scr, q2_scr, d2_scr, st_scr, other,
                 mine_oq, theirs_oq, got_oq, keep_x, give_x, got_x, full_oq, small_scr, got_dw,
                 in_sem, w_sem, m_sem, q_sem, chip_sem, out_sem, pg_sem, pg_scr,
                 st_s, st_r, rd_s, rd_r, rx_s, rx_r, ax_s, ax_r, ad_s, ad_r, dw_s, dw_r, sm_s, sm_r):
    _, n_pairs, n_rows, width = zg_scr.shape
    n_seq, n_fr, _ = m_scr.shape
    n_row = n_rows // n_seq
    rows = n_row * n_pairs
    n_blk = n_seq // n_pairs
    quarter = keep_x.shape[2]
    halves = [slice(0, n_pairs // 2), slice(n_pairs // 2, n_pairs)]
    me = lax.axis_index("cp")
    core = lax.rem(me, 2)
    chip = lax.div(me, 2)
    mate = me + 1 - 2 * core
    across = me + 2 - 4 * chip
    first = core == 0
    left = chip == 0
    peers = [lax.rem(me + d, n_cp) for d in range(1, n_cp)]
    wq_at, wo_at = n_seq - 2 * n_blk, n_seq - n_blk
    per_row = n_fr // PAIR

    def cols(k):
        return pl.ds(pl.multiple_of(k * PAIR, PAIR), PAIR)

    def seq_rows(b):
        return pl.ds(pl.multiple_of(b * n_row, n_row), n_row)

    def wo_rows(k):
        return lax.div(k, per_row), pl.ds(pl.multiple_of(lax.rem(k, per_row) * PAIR, PAIR), PAIR)

    def weight_copies(k):
        c = cols(k)
        block, r = wo_rows(k)
        return [pltpu.make_async_copy(wq_ref.at[:, :, c], m_scr.at[wq_at:wo_at, :, c], w_sem.at[0, k]),
                pltpu.make_async_copy(wo_ref.at[block, r, :], m_scr.at[wo_at + block, r, :], w_sem.at[1, k]),
                pltpu.make_async_copy(wk_ref.at[:, c], wk_scr.at[:, c], w_sem.at[2, k]),
                pltpu.make_async_copy(wv_ref.at[:, c], wv_scr.at[:, c], w_sem.at[3, k])]

    def mem_copy(g):
        at = pl.ds(g * n_blk, n_blk)
        return pltpu.make_async_copy(m_ref.at[at], m_scr.at[at], m_sem.at[g])

    def act_copies():
        return [pltpu.make_async_copy(h_ref, x_scr, in_sem.at[0]), pltpu.make_async_copy(gy_ref, gy_scr, in_sem.at[1])]

    def q_copies():
        return [pltpu.make_async_copy(q2_scr, q2_out, q_sem.at[0]), pltpu.make_async_copy(d2_scr, d2_out, q_sem.at[1])]

    def chip_copies(k):
        out, at = [], 0
        for n, ref in enumerate((chip0_ref, chip1_ref, chip2_ref, chip3_ref)):
            out.append(pltpu.make_async_copy(e_scr.at[k, at:at + ref.shape[0], :], ref.at[:, cols(k)], chip_sem.at[n, k]))
            at += ref.shape[0]
        return out

    def out_copies():
        return [pltpu.make_async_copy(full_oq.at[k, p], oq_ref.at[p, :, k * PAIR:(k + 1) * PAIR], out_sem.at[p, k])
                for k in range(n_pairs) for p in range(2)]

    def pg_copy(g):
        slot = lax.rem(g, 2)
        return pltpu.make_async_copy(pg_scr.at[slot], pg_ref.at[pl.ds(g * n_blk, n_blk)], pg_sem.at[slot])

    def stats_copy(k):
        return send(st_scr, other.at[k], (st_s, st_r), k, peers[k])

    def oq_mate(h):
        return send(theirs_oq.at[halves[h]], got_oq.at[halves[h]], (rd_s, rd_r), h, mate)

    def oq_across(h):
        return send(give_x.at[halves[h]], got_x.at[halves[h]], (rx_s, rx_r), h, across)

    def own_across(h):
        at = pl.ds(pl.multiple_of((2 * core + chip) * quarter, quarter), quarter)
        return send(full_oq.at[halves[h], :, at, :], full_oq.at[halves[h], :, at, :], (ax_s, ax_r), h, across)

    def half_mate(h):
        at = pl.ds(pl.multiple_of(core * 2 * quarter, quarter), 2 * quarter)
        return send(full_oq.at[halves[h], :, at, :], full_oq.at[halves[h], :, at, :], (ad_s, ad_r), h, mate)

    def dw_mate(k):
        return send(dp_scr.at[k], got_dw.at[k], (dw_s, dw_r), k, mate)

    def small_copy(k):
        return send(small_scr.at[me], small_scr.at[me], (sm_s, sm_r), k, peers[k])

    def add_mate(h):
        oq_mate(h).wait()
        t = mine_oq[halves[h]] + got_oq[halves[h]]
        top, bottom = t[:, :, :quarter], t[:, :, quarter:]
        keep_x[halves[h]] = jnp.where(left, top, bottom)
        give_x[halves[h]] = jnp.where(left, bottom, top)

    def finish(h):
        oq_across(h).wait()
        t = keep_x[halves[h]] + got_x[halves[h]]
        at = pl.ds(pl.multiple_of((2 * core + chip) * quarter, quarter), quarter)
        full_oq[halves[h], :, at, :] = t.astype(BF16)
        small_scr[me, 0, halves[h], :] = jnp.sum(t[:, 1], axis=1)

    for c in act_copies():
        c.start()

    @pl.loop(0, n_pairs)
    def _(k):
        for c in weight_copies(k):
            c.start()

    barrier = pltpu.get_barrier_semaphore()
    for peer in peers:
        pl.semaphore_signal(barrier, inc=1, device_id={"cp": peer}, device_id_type=pl.DeviceIdType.MESH)
    for k, ref in enumerate((gain_ref, bias_ref, bq_ref, bv_ref)):
        vec_scr[k:k + 1, :] = ref[...].astype(F32).reshape(1, width)
    for c in act_copies():
        c.wait()
    normalize(x_scr, vec_scr, x_scr)

    @pl.loop(0, n_pairs)
    def _(i):
        @pl.when((i > 0) & (i < n_pairs - 1))
        def _():
            mem_copy(i - 1).start()

        for c in weight_copies(i):
            c.wait()
        block, r = wo_rows(i)
        q = (dot(x_scr[...], m_scr[wq_at:wo_at, :, cols(i)].reshape(width, PAIR), NN) + pair_of(vec_scr, 2, i)).astype(BF16)
        d = dot(gy_scr[...], m_scr[wo_at + block, r, :], NT).astype(BF16)
        q2, d2 = split_heads(q.astype(F32), n_seq), split_heads(d.astype(F32), n_seq)
        q2_scr[i] = q2
        d2_scr[i] = d2
        place(zg_scr, 0, i, q2, lambda j, step: wk_scr[j:j + step, cols(i)])
        place(zg_scr, 1, i, d2, lambda j, step: wv_scr[j:j + step, cols(i)])
        ps_scr[i] = dot(d2, jnp.broadcast_to(pair_of(vec_scr, 3, i).astype(BF16), (PAIR, PAIR)), NT)

    for g in (n_pairs - 2, n_pairs - 1):
        mem_copy(g).start()
    for c in q_copies():
        c.start()

    @pl.loop(0, n_pairs)
    def _(g):
        mem_copy(g).wait()
        for j in range(n_blk):
            b = g * n_blk + j
            at = pl.ds(b, 1)
            t = dot(m_scr[b], zg_scr[:, :, seq_rows(b), :].reshape(2 * rows, width), NT)
            s = t[:, :rows] * scale
            dp = t[:, rows:] + ps_scr[:, seq_rows(b), :].reshape(rows, PAIR).T[0:1, :]
            mx = jnp.max(s, axis=0, keepdims=True)
            e = jnp.exp(s - mx)
            e_scr[g, j * n_fr:(j + 1) * n_fr, :] = e
            dp_scr[g, j * n_fr:(j + 1) * n_fr, :] = dp
            st_scr[0, at, :] = mx
            st_scr[1, at, :] = jnp.sum(e, axis=0, keepdims=True)
            st_scr[2, at, :] = jnp.sum(e * dp, axis=0, keepdims=True)

    pl.semaphore_wait(barrier, n_cp - 1)
    for k in range(n_cp - 1):
        stats_copy(k).start()
    for k in range(n_cp - 1):
        stats_copy(k).wait()

    @pl.loop(0, n_pairs)
    def _(g):
        @pl.when(g >= 2)
        def _():
            pg_copy(g - 2).wait()

        slot = lax.rem(g, 2)
        ones = jnp.ones((n_fr, PAIR), BF16)
        for j in range(n_blk):
            b = g * n_blk + j
            at = pl.ds(b, 1)
            tops = [st_scr[0, at, :]] + [other[k, 0, at, :] for k in range(n_cp - 1)]
            sums_l = [st_scr[1, at, :]] + [other[k, 1, at, :] for k in range(n_cp - 1)]
            sums_c = [st_scr[2, at, :]] + [other[k, 2, at, :] for k in range(n_cp - 1)]
            top = functools.reduce(jnp.maximum, tops)
            fac = [jnp.exp(t - top) for t in tops]
            total = functools.reduce(jnp.add, [f * v for f, v in zip(fac, sums_l)])
            c = functools.reduce(jnp.add, [f * v for f, v in zip(fac, sums_c)]) / total
            p = e_scr[g, j * n_fr:(j + 1) * n_fr, :] * (fac[0] / total)
            gr = p * (dp_scr[g, j * n_fr:(j + 1) * n_fr, :] - c) * scale
            pg = jnp.concatenate([gr.astype(BF16), p.astype(BF16)], axis=1)
            pg_scr[slot, j] = pg
            pgt = pg.T
            step = 256
            for w in range(0, width, step):
                t = dot(pgt, m_scr[b, :, w:w + step], NN).astype(BF16)
                zg_scr[:, :, seq_rows(b), w:w + step] = t.reshape(2, n_pairs, n_row, step)
            ps_scr[:, seq_rows(b), :] = dot(pgt[rows:], ones, NN).reshape(n_pairs, n_row, PAIR)
        pg_copy(g).start()

    def o_and_dq(k):
        o = join_heads(dot(zg_scr[1, k], wv_scr[:, cols(k)], NN), n_seq) + join_heads(ps_scr[k], n_seq) * pair_of(vec_scr, 3, k)
        dq = join_heads(dot(zg_scr[0, k], wk_scr[:, cols(k)], NN), n_seq)
        for part, t in enumerate((o, dq)):
            top, bottom = t[:t.shape[0] // 2], t[t.shape[0] // 2:]
            mine_oq[k, part] = jnp.where(first, top, bottom)
            theirs_oq[k, part] = jnp.where(first, bottom, top)

    @pl.loop(0, n_pairs // 2)
    def _(k):
        o_and_dq(k)

    oq_mate(0).start()

    @pl.loop(n_pairs // 2, n_pairs)
    def _(k):
        o_and_dq(k)

    oq_mate(1).start()
    add_mate(0)
    oq_across(0).start()

    def close_dw(k):
        dw_mate(k).wait()
        e_scr[k] += got_dw[k]

    @pl.loop(0, n_pairs)
    def _(k):
        @pl.when(k >= 1)
        def _():
            dw_mate(k - 1).start()

        @pl.when(k == 3)
        def _():
            oq_across(1).start()

        @pl.when(k >= 5)
        def _():
            for c in chip_copies(k - 5):
                c.start()

        small_scr[me, 1, pl.ds(k, 1), :] = jnp.sum(ps_scr[k] * d2_scr[k].astype(F32), axis=0, keepdims=True)
        dwk = dot(zg_scr[0, k], q2_scr[k], TN)
        dwv = dot(zg_scr[1, k], d2_scr[k], TN)
        e_scr[k] = jnp.where(first, dwk, dwv)
        dp_scr[k] = jnp.where(first, dwv, dwk)

        @pl.when(k == 2)
        def _():
            add_mate(1)

        @pl.when(k >= 4)
        def _():
            close_dw(k - 4)

    dw_mate(n_pairs - 1).start()

    @pl.loop(n_pairs - 4, n_pairs)
    def _(k):
        close_dw(k)

    @pl.loop(n_pairs - 5, n_pairs)
    def _(k):
        for c in chip_copies(k):
            c.start()

    finish(0)
    own_across(0).start()
    finish(1)
    own_across(1).start()
    for k in range(n_cp - 1):
        small_copy(k).start()
    own_across(0).wait()
    half_mate(0).start()
    own_across(1).wait()
    half_mate(1).start()
    for k in range(n_cp - 1):
        small_copy(k).wait()
    small_ref[...] = small_scr[0] + small_scr[1] + small_scr[2] + small_scr[3]
    half_mate(0).wait()
    half_mate(1).wait()
    for c in out_copies():
        c.start()

    @pl.loop(0, n_pairs)
    def _(k):
        for c in chip_copies(k):
            c.wait()

    for g in (n_pairs - 2, n_pairs - 1):
        pg_copy(g).wait()
    for c in q_copies() + out_copies():
        c.wait()


def assemble_kernel(core_ref, fin_ref, other_ref, *refs):
    wk_ref, wv_ref = refs[-2:]
    first = core_ref[0] == 0
    wk_ref[...] = jnp.where(first, fin_ref[...], other_ref[...])
    wv_ref[...] = jnp.where(first, other_ref[...], fin_ref[...])


def assemble(core, fin, other, at, acc):
    n, width = fin.shape
    step = 192 if n % 192 == 0 and at % 192 == 0 else 64
    block = pl.BlockSpec((step, width), lambda i: (i, 0))
    out = pl.BlockSpec((step, width), lambda i: (at // step + i, 0))
    return pl.pallas_call(
        assemble_kernel, grid=(n // step,), name="assemble",
        in_specs=[pl.BlockSpec(memory_space=pltpu.SMEM), block, block] + [pl.BlockSpec(memory_space=pl.ANY)] * len(acc),
        out_specs=[out, out], out_shape=[jax.ShapeDtypeStruct((width, width), F32)] * 2,
        input_output_aliases={3: 0, 4: 1} if acc else {},
        compiler_params=pltpu.CompilerParams(dimension_semantics=("arbitrary",)),
    )(core, fin, other, *acc)


def mem_kernel(n_first, q2_ref, d2_ref, wk_ref, wv_ref, pg_ref, dm_ref, z_scr):
    i = pl.program_id(0)
    _, n_pairs, _, width = z_scr.shape
    n_blk = pg_ref.shape[0]
    n_row = pg_ref.shape[2] // (2 * n_pairs)

    @pl.when(i < n_first)
    def _():
        place(z_scr, 0, i, q2_ref[0], lambda j, step: wk_ref[j:j + step, :])
        place(z_scr, 1, i, d2_ref[0], lambda j, step: wv_ref[j:j + step, :])

    @pl.when(i >= n_first)
    def _():
        for j in range(n_blk):
            b = (i - n_first) * n_blk + j
            at = pl.ds(pl.multiple_of(b * n_row, n_row), n_row)
            z = z_scr[:, :, at, :].reshape(pg_ref.shape[2], width)
            dm_ref[j] = dot(pg_ref[j], z, NN).astype(BF16)


def params():
    return pltpu.CompilerParams(dimension_semantics=("arbitrary",), vmem_limit_bytes=VMEM_LIMIT)


def solution(mesh):
    act_spec = P("dp", None, None)
    mem_spec = P("dp", "cp", None)
    vec_out = P("dp")
    mat_out = P("dp", None)
    in_specs = (act_spec, mem_spec, P(), P(), P(), P(), P(), P(), P(), P(), P(), act_spec)
    out_specs = (act_spec, act_spec, mem_spec, vec_out, vec_out, mat_out, vec_out, mat_out, mat_out, vec_out, mat_out, vec_out)
    n_cp = mesh.shape["cp"]

    def swap(x, bit):
        return lax.ppermute(x, "cp", [(i, i ^ bit) for i in range(n_cp)])

    def device_step(hidden, memory, ln_gain, ln_bias, w_q, b_q, w_k, w_v, b_v, w_o, b_o, grad_y):
        n_seq, n_tok, width = hidden.shape
        n_fr = memory.shape[1]
        n_heads = width // HEAD
        n_pairs = n_heads // 2
        rows = n_heads * n_tok
        tokens = n_seq * n_tok
        scale = HEAD ** -0.5
        core = lax.axis_index("cp") % 2
        h2, gy2 = hidden.reshape(tokens, width), grad_y.reshape(tokens, width)
        blk = n_seq // n_pairs
        quarter = tokens // 4
        chunks = [width * 3 // 8, width * 3 // 8, width * 3 // 16, width // 16]
        anywhere = pl.BlockSpec(memory_space=pl.ANY)
        vm = lambda dt, *s: pltpu.VMEM(s, dt)
        sems = lambda *n: pltpu.SemaphoreType.DMA(n)
        both = lambda n: [sems(n)] * 2
        pg, *rest = pl.pallas_call(
            functools.partial(fused_kernel, scale, n_cp), name="fused",
            in_specs=[anywhere] * 7 + [pl.BlockSpec(memory_space=pltpu.VMEM)] * 4,
            out_specs=[anywhere] * 8 + [pl.BlockSpec(memory_space=pltpu.VMEM)],
            out_shape=[jax.ShapeDtypeStruct((n_seq, n_fr, 2 * rows), BF16)]
            + [jax.ShapeDtypeStruct((c, width), F32) for c in chunks]
            + [jax.ShapeDtypeStruct((2, tokens, width), BF16)]
            + [jax.ShapeDtypeStruct((n_pairs, 2 * tokens, PAIR), BF16)] * 2
            + [jax.ShapeDtypeStruct((2, n_pairs, PAIR), F32)],
            scratch_shapes=[vm(BF16, tokens, width), vm(BF16, tokens, width), vm(F32, 4, width),
                            vm(BF16, 2, n_pairs, 2 * tokens, width), vm(BF16, n_seq, n_fr, width),
                            vm(F32, n_pairs, blk * n_fr, rows), vm(F32, n_pairs, blk * n_fr, rows),
                            vm(BF16, width, width), vm(BF16, width, width), vm(F32, n_pairs, 2 * tokens, PAIR),
                            vm(BF16, n_pairs, 2 * tokens, PAIR), vm(BF16, n_pairs, 2 * tokens, PAIR),
                            vm(F32, 3, n_seq, rows), vm(F32, n_cp - 1, 3, n_seq, rows),
                            vm(F32, n_pairs, 2, 2 * quarter, PAIR), vm(F32, n_pairs, 2, 2 * quarter, PAIR),
                            vm(F32, n_pairs, 2, 2 * quarter, PAIR), vm(F32, n_pairs, 2, quarter, PAIR),
                            vm(F32, n_pairs, 2, quarter, PAIR), vm(F32, n_pairs, 2, quarter, PAIR),
                            vm(BF16, n_pairs, 2, tokens, PAIR), vm(F32, n_cp, 2, n_pairs, PAIR),
                            vm(F32, n_pairs, width, PAIR),
                            sems(2), sems(4, n_pairs), sems(n_pairs), sems(2), sems(4, n_pairs), sems(2, n_pairs),
                            sems(2), vm(BF16, 2, blk, n_fr, 2 * rows)]
            + both(n_cp - 1) + both(2) + both(2) + both(2) + both(2) + both(n_pairs) + both(n_cp - 1),
            compiler_params=pltpu.CompilerParams(vmem_limit_bytes=VMEM_LIMIT, collective_id=0, has_side_effects=True),
        )(h2, gy2, w_q.reshape(blk, n_fr, width), w_k, w_v, w_o.reshape(blk, n_fr, width), memory, ln_gain, ln_bias, b_q, b_v)
        chips, (oq, q2, d2, small) = rest[:4], rest[4:]
        attn_out, dq_low = oq[0], oq[1]
        small = small.reshape(2, width)
        grad_bq, grad_bv = small[0], small[1]

        got = []
        for c in chips:
            got.append(swap(c, 2))

        hidden_f32 = h2.astype(F32)
        centered = hidden_f32 - jnp.mean(hidden_f32, axis=-1, keepdims=True)
        inv_std = lax.rsqrt(jnp.mean(centered * centered, axis=-1, keepdims=True) + EPS)
        x_hat = centered * inv_std
        gain_f32 = ln_gain.astype(F32)
        x_norm = (x_hat * gain_f32 + ln_bias.astype(F32)).astype(BF16)
        out_y = (hidden_f32 + dot(attn_out, w_o, NN) + b_o.astype(F32)).astype(BF16)
        grad_wo = dot(attn_out, gy2, TN)
        grad_bo = jnp.sum(gy2, axis=0, dtype=F32)
        grad_wq = dot(x_norm, dq_low, TN)
        d_xnorm = dot(dq_low, w_q, NT)
        grad_ln_gain = jnp.sum(d_xnorm * x_hat, axis=0)
        grad_ln_bias = jnp.sum(d_xnorm, axis=0)
        d_hat = d_xnorm * gain_f32
        d_hidden = inv_std * (d_hat - jnp.mean(d_hat, axis=-1, keepdims=True) - x_hat * jnp.mean(d_hat * x_hat, axis=-1, keepdims=True))
        grad_h = (gy2.astype(F32) + d_hidden).astype(BF16)

        pair_block = pl.BlockSpec((1, 2 * tokens, PAIR), lambda i: (jnp.minimum(i, n_pairs - 1), 0, 0))
        col_block = pl.BlockSpec((width, PAIR), lambda i: (0, jnp.minimum(i, n_pairs - 1)))
        late = lambda *s: pl.BlockSpec((blk,) + s, lambda i: (jnp.maximum(i - n_pairs, 0), 0, 0))
        grad_mem = pl.pallas_call(
            functools.partial(mem_kernel, n_pairs), grid=(2 * n_pairs,), name="mem",
            in_specs=[pair_block, pair_block, col_block, col_block, late(n_fr, 2 * rows)], out_specs=late(n_fr, width),
            out_shape=jax.ShapeDtypeStruct((n_seq, n_fr, width), BF16), compiler_params=params(),
            scratch_shapes=[vm(BF16, 2, n_pairs, 2 * tokens, width)],
            cost_estimate=pl.CostEstimate(flops=8 * n_seq * n_fr * rows * width, bytes_accessed=40 << 20, transcendentals=0),
        )(q2, d2, w_k, w_v, pg)

        hidden_work = (out_y, grad_h, grad_mem, grad_ln_gain, grad_ln_bias, grad_wq, grad_wo, grad_bo)
        got[0], hidden_work = lax.optimization_barrier((got[0], hidden_work))
        out_y, grad_h, grad_mem, grad_ln_gain, grad_ln_bias, grad_wq, grad_wo, grad_bo = hidden_work
        core_arr = core.reshape(1).astype(jnp.int32)
        acc, at = (), 0
        for c, g in zip(chips, got):
            g, acc = lax.optimization_barrier((g, acc))
            fin = c + g
            acc = assemble(core_arr, fin, swap(fin, 1), at, acc)
            at += c.shape[0]
        grad_wk, grad_wv = acc
        return (out_y.reshape(hidden.shape), grad_h.reshape(hidden.shape), grad_mem, grad_ln_gain, grad_ln_bias,
                grad_wq, grad_bq, grad_wk, grad_wv, grad_bv, grad_wo, grad_bo)

    return jax.shard_map(device_step, mesh=mesh, in_specs=in_specs, out_specs=out_specs, check_vma=False)
```

```python
import functools

import jax
import jax.numpy as jnp
from jax import lax
from jax.experimental import pallas as pl
from jax.experimental.pallas import tpu as pltpu
from jax.sharding import PartitionSpec as P


EPS = 1e-5
HEAD = 64
PAIR = 2 * HEAD
F32 = jnp.float32
BF16 = jnp.bfloat16
NT = (((1,), (1,)), ((), ()))
TN = (((0,), (0,)), ((), ()))
NN = (((1,), (0,)), ((), ()))
VMEM_LIMIT = 67043328


def dot(a, b, dims):
    return lax.dot_general(a, b, dims, preferred_element_type=F32)


def split_heads(x, n_seq):
    x = x.reshape(n_seq, x.shape[0] // n_seq, PAIR)
    low = lax.broadcasted_iota(jnp.int32, x.shape, 2) < HEAD
    zero = jnp.zeros_like(x)
    both = jnp.concatenate([jnp.where(low, x, zero), jnp.where(low, zero, x)], axis=1)
    return both.astype(BF16).reshape(-1, PAIR)


def join_heads(x, n_seq):
    n_tok = x.shape[0] // (2 * n_seq)
    x = x.reshape(n_seq, 2 * n_tok, PAIR)
    low = lax.broadcasted_iota(jnp.int32, (n_seq, n_tok, PAIR), 2) < HEAD
    return jnp.where(low, x[:, :n_tok], x[:, n_tok:]).reshape(n_seq * n_tok, PAIR)


def normalize(h_ref, vec_ref, x_scr):
    h = h_ref[...].astype(F32)
    c = h - jnp.mean(h, axis=-1, keepdims=True)
    inv = lax.rsqrt(jnp.mean(c * c, axis=-1, keepdims=True) + EPS)
    x_scr[...] = (c * inv * vec_ref[0:1, :] + vec_ref[1:2, :]).astype(BF16)


def pair_of(vec_ref, row, i):
    return vec_ref[row:row + 1, pl.ds(pl.multiple_of(i * PAIR, PAIR), PAIR)]


def place(out_ref, part, i, x, weight):
    step = 256
    for j in range(0, out_ref.shape[3], step):
        out_ref[part, i, :, j:j + step] = dot(x, weight(j, step), NT).astype(BF16)


def send(src, dst, sems, k, peer):
    return pltpu.make_async_remote_copy(
        src_ref=src, dst_ref=dst, send_sem=sems[0].at[k], recv_sem=sems[1].at[k],
        device_id={"cp": peer}, device_id_type=pl.DeviceIdType.MESH)


def fused_kernel(scale, n_cp, h_ref, gy_ref, wq_ref, wk_ref, wv_ref, wo_ref, m_ref, gain_ref, bias_ref, bq_ref, bv_ref,
                 pg_ref, chip0_ref, chip1_ref, chip2_ref, chip3_ref, head_ref, head_got, oq_ref, q2_out, d2_out, small_ref,
                 x_scr, gy_scr, vec_scr, zg_scr, m_scr, e_scr, dp_scr, wk_scr, wv_scr, ps_scr, q2_scr, d2_scr, st_scr, other,
                 mine_oq, theirs_oq, got_oq, keep_x, give_x, got_x, full_oq, small_scr, got_dw,
                 in_sem, w_sem, m_sem, q_sem, chip_sem, head_sem, out_sem, pg_sem, pg_scr,
                 st_s, st_r, rd_s, rd_r, rx_s, rx_r, ax_s, ax_r, ad_s, ad_r, dw_s, dw_r, sm_s, sm_r, xd_s, xd_r):
    _, n_pairs, n_rows, width = zg_scr.shape
    n_seq, n_fr, _ = m_scr.shape
    n_row = n_rows // n_seq
    rows = n_row * n_pairs
    n_blk = n_seq // n_pairs
    quarter = keep_x.shape[2]
    n_part = rd_s.shape[0]
    n_each = n_pairs // n_part
    halves = [slice(h * n_each, (h + 1) * n_each) for h in range(n_part)]
    n_grp = st_scr.shape[0]
    per_grp = n_pairs // n_grp
    me = lax.axis_index("cp")
    core = lax.rem(me, 2)
    chip = lax.div(me, 2)
    mate = me + 1 - 2 * core
    across = me + 2 - 4 * chip
    first = core == 0
    left = chip == 0
    peers = [lax.rem(me + d, n_cp) for d in range(1, n_cp)]
    wq_at, wo_at = n_seq - 2 * n_blk, n_seq - n_blk
    per_row = n_fr // PAIR

    def cols(k):
        return pl.ds(pl.multiple_of(k * PAIR, PAIR), PAIR)

    def seq_rows(b):
        return pl.ds(pl.multiple_of(b * n_row, n_row), n_row)

    def wo_rows(k):
        return lax.div(k, per_row), pl.ds(pl.multiple_of(lax.rem(k, per_row) * PAIR, PAIR), PAIR)

    def weight_copies(k):
        c = cols(k)
        block, r = wo_rows(k)
        return [pltpu.make_async_copy(wq_ref.at[:, :, c], m_scr.at[wq_at:wo_at, :, c], w_sem.at[0, k]),
                pltpu.make_async_copy(wo_ref.at[block, r, :], m_scr.at[wo_at + block, r, :], w_sem.at[1, k]),
                pltpu.make_async_copy(wk_ref.at[:, c], wk_scr.at[:, c], w_sem.at[2, k]),
                pltpu.make_async_copy(wv_ref.at[:, c], wv_scr.at[:, c], w_sem.at[3, k])]

    def mem_copy(g):
        at = pl.ds(g * n_blk, n_blk)
        return pltpu.make_async_copy(m_ref.at[at], m_scr.at[at], m_sem.at[g])

    def act_copies():
        return [pltpu.make_async_copy(h_ref, x_scr, in_sem.at[0]), pltpu.make_async_copy(gy_ref, gy_scr, in_sem.at[1])]

    def q_copies():
        return [pltpu.make_async_copy(q2_scr, q2_out, q_sem.at[0]), pltpu.make_async_copy(d2_scr, d2_out, q_sem.at[1])]

    def chip_copies(k):
        out, at = [], 0
        for n, ref in enumerate((chip0_ref, chip1_ref, chip2_ref, chip3_ref)):
            out.append(pltpu.make_async_copy(e_scr.at[k, at:at + ref.shape[0], :], ref.at[:, cols(k - 1)], chip_sem.at[n, k]))
            at += ref.shape[0]
        return out

    def head_copy():
        return pltpu.make_async_copy(e_scr.at[0], head_ref, head_sem.at[0])

    def head_across():
        return send(e_scr.at[0], head_got, (xd_s, xd_r), 0, across)

    def out_copies():
        return [pltpu.make_async_copy(full_oq.at[k, p], oq_ref.at[p, :, k * PAIR:(k + 1) * PAIR], out_sem.at[p, k])
                for k in range(n_pairs) for p in range(2)]

    def pg_copy(g):
        slot = lax.rem(g, 2)
        return pltpu.make_async_copy(pg_scr.at[slot], pg_ref.at[pl.ds(g * n_blk, n_blk)], pg_sem.at[slot])

    def stats_copies(q):
        return [pltpu.make_async_remote_copy(
            src_ref=st_scr.at[q], dst_ref=other.at[k, q], send_sem=st_s.at[k, q], recv_sem=st_r.at[k, q],
            device_id={"cp": peers[k]}, device_id_type=pl.DeviceIdType.MESH) for k in range(n_cp - 1)]

    def oq_mate(h):
        return send(theirs_oq.at[halves[h]], got_oq.at[halves[h]], (rd_s, rd_r), h, mate)

    def oq_across(h):
        return send(give_x.at[halves[h]], got_x.at[halves[h]], (rx_s, rx_r), h, across)

    def own_across(h):
        at = pl.ds(pl.multiple_of((2 * core + chip) * quarter, quarter), quarter)
        return send(full_oq.at[halves[h], :, at, :], full_oq.at[halves[h], :, at, :], (ax_s, ax_r), h, across)

    def half_mate(h):
        at = pl.ds(pl.multiple_of(core * 2 * quarter, quarter), 2 * quarter)
        return send(full_oq.at[halves[h], :, at, :], full_oq.at[halves[h], :, at, :], (ad_s, ad_r), h, mate)

    def dw_mate(k):
        return send(dp_scr.at[k], got_dw.at[k], (dw_s, dw_r), k, mate)

    def small_copy(k):
        return send(small_scr.at[me], small_scr.at[me], (sm_s, sm_r), k, peers[k])

    def add_mate(h):
        oq_mate(h).wait()
        t = mine_oq[halves[h]] + got_oq[halves[h]]
        top, bottom = t[:, :, :quarter], t[:, :, quarter:]
        keep_x[halves[h]] = jnp.where(left, top, bottom)
        give_x[halves[h]] = jnp.where(left, bottom, top)

    def finish(h):
        oq_across(h).wait()
        t = keep_x[halves[h]] + got_x[halves[h]]
        at = pl.ds(pl.multiple_of((2 * core + chip) * quarter, quarter), quarter)
        full_oq[halves[h], :, at, :] = t.astype(BF16)
        small_scr[me, 0, halves[h], :] = jnp.sum(t[:, 1], axis=1)

    for c in act_copies():
        c.start()

    for k in range(2):
        for c in weight_copies(k):
            c.start()

    barrier = pltpu.get_barrier_semaphore()
    for peer in peers:
        pl.semaphore_signal(barrier, inc=1, device_id={"cp": peer}, device_id_type=pl.DeviceIdType.MESH)
    for k, ref in enumerate((gain_ref, bias_ref, bq_ref, bv_ref)):
        vec_scr[k:k + 1, :] = ref[...].astype(F32).reshape(1, width)
    for c in act_copies():
        c.wait()
    normalize(x_scr, vec_scr, x_scr)

    @pl.loop(0, n_pairs)
    def _(i):
        @pl.when(i < n_pairs - 2)
        def _():
            for c in weight_copies(i + 2):
                c.start()
            mem_copy(i).start()

        for c in weight_copies(i):
            c.wait()
        block, r = wo_rows(i)
        q = (dot(x_scr[...], m_scr[wq_at:wo_at, :, cols(i)].reshape(width, PAIR), NN) + pair_of(vec_scr, 2, i)).astype(BF16)
        d = dot(gy_scr[...], m_scr[wo_at + block, r, :], NT).astype(BF16)
        q2, d2 = split_heads(q.astype(F32), n_seq), split_heads(d.astype(F32), n_seq)
        q2_scr[i] = q2
        d2_scr[i] = d2
        place(zg_scr, 0, i, q2, lambda j, step: wk_scr[j:j + step, cols(i)])
        place(zg_scr, 1, i, d2, lambda j, step: wv_scr[j:j + step, cols(i)])
        ps_scr[i] = dot(d2, jnp.broadcast_to(pair_of(vec_scr, 3, i).astype(BF16), (PAIR, PAIR)), NT)

    for g in (n_pairs - 2, n_pairs - 1):
        mem_copy(g).start()
    for c in q_copies():
        c.start()

    pl.semaphore_wait(barrier, n_cp - 1)

    @pl.loop(0, n_pairs)
    def _(g):
        grp = lax.div(g, per_grp)

        @pl.when((g > 0) & (lax.rem(g, per_grp) == 0))
        def _():
            for c in stats_copies(grp - 1):
                c.start()

        mem_copy(g).wait()
        for j in range(n_blk):
            b = g * n_blk + j
            at = pl.ds(lax.rem(g, per_grp) * n_blk + j, 1)
            t = dot(m_scr[b], zg_scr[:, :, seq_rows(b), :].reshape(2 * rows, width), NT)
            s = t[:, :rows] * scale
            dp = t[:, rows:] + ps_scr[:, seq_rows(b), :].reshape(rows, PAIR).T[0:1, :]
            mx = jnp.max(s, axis=0, keepdims=True)
            e = jnp.exp(s - mx)
            e_scr[g, j * n_fr:(j + 1) * n_fr, :] = e
            dp_scr[g, j * n_fr:(j + 1) * n_fr, :] = dp
            st_scr[grp, 0, at, :] = mx
            st_scr[grp, 1, at, :] = jnp.sum(e, axis=0, keepdims=True)
            st_scr[grp, 2, at, :] = jnp.sum(e * dp, axis=0, keepdims=True)

    for c in stats_copies(n_grp - 1):
        c.start()

    @pl.loop(0, n_pairs)
    def _(g):
        grp = lax.div(g, per_grp)

        @pl.when(lax.rem(g, per_grp) == 0)
        def _():
            for c in stats_copies(grp):
                c.wait()

        @pl.when(g >= 2)
        def _():
            pg_copy(g - 2).wait()

        slot = lax.rem(g, 2)
        ones = jnp.ones((n_fr, PAIR), BF16)
        for j in range(n_blk):
            b = g * n_blk + j
            at = pl.ds(lax.rem(g, per_grp) * n_blk + j, 1)
            tops, sums_l, sums_c = ([st_scr[grp, n, at, :]] + [other[k, grp, n, at, :] for k in range(n_cp - 1)] for n in range(3))
            top = functools.reduce(jnp.maximum, tops)
            fac = [jnp.exp(t - top) for t in tops]
            total = functools.reduce(jnp.add, [f * v for f, v in zip(fac, sums_l)])
            c = functools.reduce(jnp.add, [f * v for f, v in zip(fac, sums_c)]) / total
            p = e_scr[g, j * n_fr:(j + 1) * n_fr, :] * (fac[0] / total)
            gr = p * (dp_scr[g, j * n_fr:(j + 1) * n_fr, :] - c) * scale
            pg = jnp.concatenate([gr.astype(BF16), p.astype(BF16)], axis=1)
            pg_scr[slot, j] = pg
            pgt = pg.T
            step = 256
            for w in range(0, width, step):
                t = dot(pgt, m_scr[b, :, w:w + step], NN).astype(BF16)
                zg_scr[:, :, seq_rows(b), w:w + step] = t.reshape(2, n_pairs, n_row, step)
            ps_scr[:, seq_rows(b), :] = dot(pgt[rows:], ones, NN).reshape(n_pairs, n_row, PAIR)
        pg_copy(g).start()

    def o_and_dq(k):
        o = join_heads(dot(zg_scr[1, k], wv_scr[:, cols(k)], NN), n_seq) + join_heads(ps_scr[k], n_seq) * pair_of(vec_scr, 3, k)
        dq = join_heads(dot(zg_scr[0, k], wk_scr[:, cols(k)], NN), n_seq)
        for part, t in enumerate((o, dq)):
            top, bottom = t[:t.shape[0] // 2], t[t.shape[0] // 2:]
            mine_oq[k, part] = jnp.where(first, top, bottom)
            theirs_oq[k, part] = jnp.where(first, bottom, top)

    for h in range(n_part):
        @pl.loop(h * n_each, (h + 1) * n_each)
        def _(k):
            o_and_dq(k)

        oq_mate(h).start()
        if h > 0:
            add_mate(h - 1)
            oq_across(h - 1).start()

    def close_dw(k):
        dw_mate(k).wait()
        e_scr[k] += got_dw[k]

    @pl.loop(0, n_pairs)
    def _(k):
        @pl.when(k >= 1)
        def _():
            dw_mate(k - 1).start()

        @pl.when(k == 2)
        def _():
            oq_across(n_part - 1).start()

        @pl.when(k == 5)
        def _():
            head_copy().start()

        @pl.when(k >= 6)
        def _():
            for c in chip_copies(k - 5):
                c.start()

        small_scr[me, 1, pl.ds(k, 1), :] = jnp.sum(ps_scr[k] * d2_scr[k].astype(F32), axis=0, keepdims=True)
        dwk = dot(zg_scr[0, k], q2_scr[k], TN)
        dwv = dot(zg_scr[1, k], d2_scr[k], TN)
        e_scr[k] = jnp.where(first, dwk, dwv)
        dp_scr[k] = jnp.where(first, dwv, dwk)

        @pl.when(k == 1)
        def _():
            add_mate(n_part - 1)

        @pl.when(k >= 4)
        def _():
            close_dw(k - 4)

    dw_mate(n_pairs - 1).start()

    @pl.loop(n_pairs - 4, n_pairs)
    def _(k):
        close_dw(k)

    @pl.loop(n_pairs - 5, n_pairs)
    def _(k):
        for c in chip_copies(k):
            c.start()

    for h in range(n_part):
        finish(h)
        own_across(h).start()
    for k in range(n_cp - 1):
        small_copy(k).start()
    head_across().start()
    for h in range(n_part):
        own_across(h).wait()
        half_mate(h).start()
    for k in range(n_cp - 1):
        small_copy(k).wait()
    small_ref[...] = small_scr[0] + small_scr[1] + small_scr[2] + small_scr[3]
    for h in range(n_part):
        half_mate(h).wait()
    for c in out_copies():
        c.start()

    @pl.loop(1, n_pairs)
    def _(k):
        for c in chip_copies(k):
            c.wait()

    head_copy().wait()
    for g in (n_pairs - 2, n_pairs - 1):
        pg_copy(g).wait()
    for c in q_copies() + out_copies():
        c.wait()
    head_across().wait()


def assemble_kernel(core_ref, own_ref, got_ref, own2_ref, got2_ref, head_ref, head2_ref, *refs):
    wk_ref, wv_ref = refs[-2:]
    first = core_ref[0] == 0
    mine, other = own_ref[...] + got_ref[...], own2_ref[...] + got2_ref[...]
    wk_ref[:, :PAIR] = jnp.where(first, head_ref[...], head2_ref[...])
    wv_ref[:, :PAIR] = jnp.where(first, head2_ref[...], head_ref[...])
    wk_ref[:, PAIR:] = jnp.where(first, mine, other)
    wv_ref[:, PAIR:] = jnp.where(first, other, mine)


def assemble(core, own, got, own2, got2, head, head2, at, acc):
    n, width = own.shape[0], own.shape[1] + PAIR
    step = next(k for k in (192, 128, 64) if n % k == 0 and at % k == 0)
    block = pl.BlockSpec((step, width - PAIR), lambda i: (i, 0))
    head_block = pl.BlockSpec((step, PAIR), lambda i: (at // step + i, 0))
    out = pl.BlockSpec((step, width), lambda i: (at // step + i, 0))
    return pl.pallas_call(
        assemble_kernel, grid=(n // step,), name="assemble",
        in_specs=[pl.BlockSpec(memory_space=pltpu.SMEM)] + [block] * 4 + [head_block] * 2
        + [pl.BlockSpec(memory_space=pl.ANY)] * len(acc),
        out_specs=[out, out], out_shape=[jax.ShapeDtypeStruct((width, width), F32)] * 2,
        input_output_aliases={7: 0, 8: 1} if acc else {},
        compiler_params=params(),
    )(core, own, got, own2, got2, head, head2, *acc)


def mem_kernel(n_first, q2_ref, d2_ref, wk_ref, wv_ref, pg_ref, dm_ref, z_scr):
    i = pl.program_id(0)
    _, n_pairs, _, width = z_scr.shape
    n_blk = pg_ref.shape[0]
    n_row = pg_ref.shape[2] // (2 * n_pairs)

    @pl.when(i < n_first)
    def _():
        place(z_scr, 0, i, q2_ref[0], lambda j, step: wk_ref[j:j + step, :])
        place(z_scr, 1, i, d2_ref[0], lambda j, step: wv_ref[j:j + step, :])

    @pl.when(i >= n_first)
    def _():
        for j in range(n_blk):
            b = (i - n_first) * n_blk + j
            at = pl.ds(pl.multiple_of(b * n_row, n_row), n_row)
            z = z_scr[:, :, at, :].reshape(pg_ref.shape[2], width)
            dm_ref[j] = dot(pg_ref[j], z, NN).astype(BF16)


def params():
    return pltpu.CompilerParams(dimension_semantics=("arbitrary",), vmem_limit_bytes=VMEM_LIMIT)


def solution(mesh):
    act_spec = P("dp", None, None)
    mem_spec = P("dp", "cp", None)
    vec_out = P("dp")
    mat_out = P("dp", None)
    in_specs = (act_spec, mem_spec, P(), P(), P(), P(), P(), P(), P(), P(), P(), act_spec)
    out_specs = (act_spec, act_spec, mem_spec, vec_out, vec_out, mat_out, vec_out, mat_out, mat_out, vec_out, mat_out, vec_out)
    n_cp = mesh.shape["cp"]

    def swap(x, bit):
        return lax.ppermute(x, "cp", [(i, i ^ bit) for i in range(n_cp)])

    def device_step(hidden, memory, ln_gain, ln_bias, w_q, b_q, w_k, w_v, b_v, w_o, b_o, grad_y):
        n_seq, n_tok, width = hidden.shape
        n_fr = memory.shape[1]
        n_heads = width // HEAD
        n_pairs = n_heads // 2
        rows = n_heads * n_tok
        tokens = n_seq * n_tok
        scale = HEAD ** -0.5
        core = lax.axis_index("cp") % 2
        h2, gy2 = hidden.reshape(tokens, width), grad_y.reshape(tokens, width)
        blk = n_seq // n_pairs
        quarter = tokens // 4
        chunks = [width * 3 // 8, width * 5 // 16, width * 3 // 16, width // 8]
        anywhere = pl.BlockSpec(memory_space=pl.ANY)
        vm = lambda dt, *s: pltpu.VMEM(s, dt)
        sems = lambda *n: pltpu.SemaphoreType.DMA(n)
        both = lambda n: [sems(n)] * 2
        pg, *rest = pl.pallas_call(
            functools.partial(fused_kernel, scale, n_cp), name="fused",
            in_specs=[anywhere] * 7 + [pl.BlockSpec(memory_space=pltpu.VMEM)] * 4,
            out_specs=[anywhere] * 10 + [pl.BlockSpec(memory_space=pltpu.VMEM)],
            out_shape=[jax.ShapeDtypeStruct((n_seq, n_fr, 2 * rows), BF16)]
            + [jax.ShapeDtypeStruct((c, width - PAIR), F32) for c in chunks]
            + [jax.ShapeDtypeStruct((width, PAIR), F32)] * 2
            + [jax.ShapeDtypeStruct((2, tokens, width), BF16)]
            + [jax.ShapeDtypeStruct((n_pairs, 2 * tokens, PAIR), BF16)] * 2
            + [jax.ShapeDtypeStruct((2, n_pairs, PAIR), F32)],
            scratch_shapes=[vm(BF16, tokens, width), vm(BF16, tokens, width), vm(F32, 4, width),
                            vm(BF16, 2, n_pairs, 2 * tokens, width), vm(BF16, n_seq, n_fr, width),
                            vm(F32, n_pairs, blk * n_fr, rows), vm(F32, n_pairs, blk * n_fr, rows),
                            vm(BF16, width, width), vm(BF16, width, width), vm(F32, n_pairs, 2 * tokens, PAIR),
                            vm(BF16, n_pairs, 2 * tokens, PAIR), vm(BF16, n_pairs, 2 * tokens, PAIR),
                            vm(F32, 4, 3, n_seq // 4, rows), vm(F32, n_cp - 1, 4, 3, n_seq // 4, rows),
                            vm(F32, n_pairs, 2, 2 * quarter, PAIR), vm(F32, n_pairs, 2, 2 * quarter, PAIR),
                            vm(F32, n_pairs, 2, 2 * quarter, PAIR), vm(F32, n_pairs, 2, quarter, PAIR),
                            vm(F32, n_pairs, 2, quarter, PAIR), vm(F32, n_pairs, 2, quarter, PAIR),
                            vm(BF16, n_pairs, 2, tokens, PAIR), vm(F32, n_cp, 2, n_pairs, PAIR),
                            vm(F32, n_pairs, width, PAIR),
                            sems(2), sems(4, n_pairs), sems(n_pairs), sems(2), sems(4, n_pairs), sems(1), sems(2, n_pairs),
                            sems(2), vm(BF16, 2, blk, n_fr, 2 * rows)]
            + [sems(n_cp - 1, 4)] * 2 + both(4) + both(4) + both(4) + both(4) + both(n_pairs) + both(n_cp - 1) + both(1),
            compiler_params=pltpu.CompilerParams(vmem_limit_bytes=VMEM_LIMIT, collective_id=0, has_side_effects=True),
        )(h2, gy2, w_q.reshape(blk, n_fr, width), w_k, w_v, w_o.reshape(blk, n_fr, width), memory, ln_gain, ln_bias, b_q, b_v)
        chips, (head, head_got, oq, q2, d2, small) = rest[:4], rest[4:]
        attn_out, dq_low = oq[0], oq[1]
        small = small.reshape(2, width)
        grad_bq, grad_bv = small[0], small[1]

        got, chips2 = [], []
        for c in chips:
            got.append(swap(c, 2))
        for c in chips:
            chips2.append(swap(c, 1))
        head = head + head_got
        head2 = swap(head, 1)

        hidden_f32 = h2.astype(F32)
        centered = hidden_f32 - jnp.mean(hidden_f32, axis=-1, keepdims=True)
        inv_std = lax.rsqrt(jnp.mean(centered * centered, axis=-1, keepdims=True) + EPS)
        x_hat = centered * inv_std
        gain_f32 = ln_gain.astype(F32)
        x_norm = (x_hat * gain_f32 + ln_bias.astype(F32)).astype(BF16)
        out_y = (hidden_f32 + dot(attn_out, w_o, NN) + b_o.astype(F32)).astype(BF16)
        grad_wo = dot(attn_out, gy2, TN)
        grad_bo = jnp.sum(gy2, axis=0, dtype=F32)
        grad_wq = dot(x_norm, dq_low, TN)
        d_xnorm = dot(dq_low, w_q, NT)
        grad_ln_gain = jnp.sum(d_xnorm * x_hat, axis=0)
        grad_ln_bias = jnp.sum(d_xnorm, axis=0)
        d_hat = d_xnorm * gain_f32
        d_hidden = inv_std * (d_hat - jnp.mean(d_hat, axis=-1, keepdims=True) - x_hat * jnp.mean(d_hat * x_hat, axis=-1, keepdims=True))
        grad_h = (gy2.astype(F32) + d_hidden).astype(BF16)

        pair_block = pl.BlockSpec((1, 2 * tokens, PAIR), lambda i: (jnp.minimum(i, n_pairs - 1), 0, 0))
        col_block = pl.BlockSpec((width, PAIR), lambda i: (0, jnp.minimum(i, n_pairs - 1)))
        late = lambda *s: pl.BlockSpec((blk,) + s, lambda i: (jnp.maximum(i - n_pairs, 0), 0, 0))
        grad_mem = pl.pallas_call(
            functools.partial(mem_kernel, n_pairs), grid=(2 * n_pairs,), name="mem",
            in_specs=[pair_block, pair_block, col_block, col_block, late(n_fr, 2 * rows)], out_specs=late(n_fr, width),
            out_shape=jax.ShapeDtypeStruct((n_seq, n_fr, width), BF16), compiler_params=params(),
            scratch_shapes=[vm(BF16, 2, n_pairs, 2 * tokens, width)],
            cost_estimate=pl.CostEstimate(flops=8 * n_seq * n_fr * rows * width, bytes_accessed=40 << 20, transcendentals=0),
        )(q2, d2, w_k, w_v, pg)

        hidden_work = (out_y, grad_h, grad_mem, grad_ln_gain, grad_ln_bias, grad_wq, grad_wo, grad_bo)
        got[0], hidden_work = lax.optimization_barrier((got[0], hidden_work))
        out_y, grad_h, grad_mem, grad_ln_gain, grad_ln_bias, grad_wq, grad_wo, grad_bo = hidden_work
        core_arr = core.reshape(1).astype(jnp.int32)
        acc, at = (), 0
        for c, c2, g in zip(chips, chips2, got):
            g, acc = lax.optimization_barrier((g, acc))
            acc = assemble(core_arr, c, g, c2, swap(g, 1), head, head2, at, acc)
            at += c.shape[0]
        grad_wk, grad_wv = acc
        return (out_y.reshape(hidden.shape), grad_h.reshape(hidden.shape), grad_mem, grad_ln_gain, grad_ln_bias,
                grad_wq, grad_bq, grad_wk, grad_wv, grad_bv, grad_wo, grad_bo)

    return jax.shard_map(device_step, mesh=mesh, in_specs=in_specs, out_specs=out_specs, check_vma=False)
```

```python
import functools

import jax
import jax.numpy as jnp
from jax import lax
from jax.experimental import pallas as pl
from jax.experimental.pallas import tpu as pltpu
from jax.sharding import PartitionSpec as P


EPS = 1e-5
HEAD = 64
PAIR = 2 * HEAD
F32 = jnp.float32
BF16 = jnp.bfloat16
NT = (((1,), (1,)), ((), ()))
TN = (((0,), (0,)), ((), ()))
NN = (((1,), (0,)), ((), ()))
VMEM_LIMIT = 67043328


def dot(a, b, dims):
    return lax.dot_general(a, b, dims, preferred_element_type=F32)


def split_heads(x, n_seq):
    x = x.reshape(n_seq, x.shape[0] // n_seq, PAIR)
    low = lax.broadcasted_iota(jnp.int32, x.shape, 2) < HEAD
    zero = jnp.zeros_like(x)
    both = jnp.concatenate([jnp.where(low, x, zero), jnp.where(low, zero, x)], axis=1)
    return both.astype(BF16).reshape(-1, PAIR)


def join_heads(x, n_seq):
    n_tok = x.shape[0] // (2 * n_seq)
    x = x.reshape(n_seq, 2 * n_tok, PAIR)
    low = lax.broadcasted_iota(jnp.int32, (n_seq, n_tok, PAIR), 2) < HEAD
    return jnp.where(low, x[:, :n_tok], x[:, n_tok:]).reshape(n_seq * n_tok, PAIR)


def normalize(h_ref, vec_ref, x_scr):
    h = h_ref[...].astype(F32)
    c = h - jnp.mean(h, axis=-1, keepdims=True)
    inv = lax.rsqrt(jnp.mean(c * c, axis=-1, keepdims=True) + EPS)
    x_scr[...] = (c * inv * vec_ref[0:1, :] + vec_ref[1:2, :]).astype(BF16)


def pair_of(vec_ref, row, i):
    return vec_ref[row:row + 1, pl.ds(pl.multiple_of(i * PAIR, PAIR), PAIR)]


def place(out_ref, part, i, x, weight):
    step = 256
    for j in range(0, out_ref.shape[3], step):
        out_ref[part, i, :, j:j + step] = dot(x, weight(j, step), NT).astype(BF16)


def send(src, dst, sems, k, peer):
    return pltpu.make_async_remote_copy(
        src_ref=src, dst_ref=dst, send_sem=sems[0].at[k], recv_sem=sems[1].at[k],
        device_id={"cp": peer}, device_id_type=pl.DeviceIdType.MESH)


def fused_kernel(scale, n_cp, h_ref, gy_ref, wq_ref, wk_ref, wv_ref, wo_ref, m_ref, *refs):
    fused_body(scale, n_cp, h_ref, gy_ref, wq_ref, wk_ref, wv_ref, wo_ref, m_ref, refs[:4], *refs[4:])


def fused_body(scale, n_cp, h_ref, gy_ref, wq_ref, wk_ref, wv_ref, wo_ref, m_ref, vec_refs,
                 pg_ref, chip0_ref, chip1_ref, chip2_ref, chip3_ref, head_ref, head_got, oq_ref, q2_out, d2_out, small_ref,
                 x_scr, gy_scr, raw0, raw1, raw2, raw3, vec_scr, zg_scr, m_scr, e_scr, dp_scr, wk_scr, wv_scr, ps_scr, q2_scr, d2_scr, st_scr, other,
                 mine_oq, theirs_oq, got_oq, keep_x, give_x, got_x, full_oq, small_scr, got_dw,
                 in_sem, w_sem, m_sem, q_sem, chip_sem, head_sem, out_sem, pg_sem, pg_scr,
                 st_s, st_r, rd_s, rd_r, rx_s, rx_r, ax_s, ax_r, ad_s, ad_r, dw_s, dw_r, sm_s, sm_r, xd_s, xd_r):
    _, n_pairs, n_rows, width = zg_scr.shape
    n_seq, n_fr, _ = m_scr.shape
    n_row = n_rows // n_seq
    rows = n_row * n_pairs
    n_blk = n_seq // n_pairs
    quarter = keep_x.shape[2]
    n_part = rd_s.shape[0]
    n_each = n_pairs // n_part
    halves = [slice(h * n_each, (h + 1) * n_each) for h in range(n_part)]
    n_grp = st_scr.shape[0]
    per_grp = n_pairs // n_grp
    me = lax.axis_index("cp")
    core = lax.rem(me, 2)
    chip = lax.div(me, 2)
    mate = me + 1 - 2 * core
    across = me + 2 - 4 * chip
    first = core == 0
    left = chip == 0
    peers = [lax.rem(me + d, n_cp) for d in range(1, n_cp)]
    wq_at, wo_at = n_seq - 2 * n_blk, n_seq - n_blk

    def cols(k):
        return pl.ds(pl.multiple_of(k * PAIR, PAIR), PAIR)

    def seq_rows(b):
        return pl.ds(pl.multiple_of(b * n_row, n_row), n_row)

    def wide(k):
        return pl.ds(pl.multiple_of(k * 2 * PAIR, 2 * PAIR), 2 * PAIR)

    def weight_copies(k):
        c = wide(k)
        return [pltpu.make_async_copy(wq_ref.at[:, :, c], m_scr.at[wq_at:wo_at, :, c], w_sem.at[0, k]),
                pltpu.make_async_copy(wo_ref.at[k], m_scr.at[wo_at + k], w_sem.at[1, k]),
                pltpu.make_async_copy(wk_ref.at[:, c], wk_scr.at[:, c], w_sem.at[2, k]),
                pltpu.make_async_copy(wv_ref.at[:, c], wv_scr.at[:, c], w_sem.at[3, k])]

    def mem_copy(g):
        at = pl.ds(g * n_blk, n_blk)
        return pltpu.make_async_copy(m_ref.at[at], m_scr.at[at], m_sem.at[g])

    def act_copies():
        return [pltpu.make_async_copy(src, dst, in_sem.at[k]) for k, (src, dst) in enumerate(
            zip((h_ref,) + tuple(vec_refs) + (gy_ref,), (x_scr, raw0, raw1, raw2, raw3, gy_scr)))]

    def q_copies():
        return [pltpu.make_async_copy(q2_scr, q2_out, q_sem.at[0]), pltpu.make_async_copy(d2_scr, d2_out, q_sem.at[1])]

    def chip_copies(k):
        out, at = [], 0
        for n, ref in enumerate((chip0_ref, chip1_ref, chip2_ref, chip3_ref)):
            out.append(pltpu.make_async_copy(e_scr.at[k, at:at + ref.shape[0], :], ref.at[:, cols(k - 1)], chip_sem.at[n, k]))
            at += ref.shape[0]
        return out

    def head_copy():
        return pltpu.make_async_copy(e_scr.at[0], head_ref, head_sem.at[0])

    def head_across():
        return send(e_scr.at[0], head_got, (xd_s, xd_r), 0, across)

    def out_copies():
        return [pltpu.make_async_copy(full_oq.at[k, p], oq_ref.at[p, :, k * PAIR:(k + 1) * PAIR], out_sem.at[p, k])
                for k in range(n_pairs) for p in range(2)]

    def pg_copy(g):
        slot = lax.rem(g, 2)
        return pltpu.make_async_copy(pg_scr.at[slot], pg_ref.at[pl.ds(g * n_blk, n_blk)], pg_sem.at[slot])

    def stats_copies(q):
        return [pltpu.make_async_remote_copy(
            src_ref=st_scr.at[q], dst_ref=other.at[k, q], send_sem=st_s.at[k, q], recv_sem=st_r.at[k, q],
            device_id={"cp": peers[k]}, device_id_type=pl.DeviceIdType.MESH) for k in range(n_cp - 1)]

    def oq_mate(h):
        return send(theirs_oq.at[halves[h]], got_oq.at[halves[h]], (rd_s, rd_r), h, mate)

    def oq_across(h):
        return send(give_x.at[halves[h]], got_x.at[halves[h]], (rx_s, rx_r), h, across)

    def own_across(h):
        at = pl.ds(pl.multiple_of((2 * core + chip) * quarter, quarter), quarter)
        return send(full_oq.at[halves[h], :, at, :], full_oq.at[halves[h], :, at, :], (ax_s, ax_r), h, across)

    def half_mate(h):
        at = pl.ds(pl.multiple_of(core * 2 * quarter, quarter), 2 * quarter)
        return send(full_oq.at[halves[h], :, at, :], full_oq.at[halves[h], :, at, :], (ad_s, ad_r), h, mate)

    def dw_mate(k):
        return send(dp_scr.at[k], got_dw.at[k], (dw_s, dw_r), k, mate)

    def small_copy(k):
        return send(small_scr.at[me], small_scr.at[me], (sm_s, sm_r), k, peers[k])

    def add_mate(h):
        oq_mate(h).wait()
        t = mine_oq[halves[h]] + got_oq[halves[h]]
        top, bottom = t[:, :, :quarter], t[:, :, quarter:]
        keep_x[halves[h]] = jnp.where(left, top, bottom)
        give_x[halves[h]] = jnp.where(left, bottom, top)

    def finish(h):
        oq_across(h).wait()
        t = keep_x[halves[h]] + got_x[halves[h]]
        at = pl.ds(pl.multiple_of((2 * core + chip) * quarter, quarter), quarter)
        full_oq[halves[h], :, at, :] = t.astype(BF16)
        small_scr[me, 0, halves[h], :] = jnp.sum(t[:, 1], axis=1)

    for c in act_copies():
        c.start()

    for k in range(2):
        for c in weight_copies(k):
            c.start()

    barrier = pltpu.get_barrier_semaphore()
    for peer in peers:
        pl.semaphore_signal(barrier, inc=1, device_id={"cp": peer}, device_id_type=pl.DeviceIdType.MESH)
    for c in act_copies():
        c.wait()
    for k, ref in enumerate((raw0, raw1, raw2, raw3)):
        vec_scr[k:k + 1, :] = ref[...].astype(F32).reshape(1, width)
    normalize(x_scr, vec_scr, x_scr)

    @pl.loop(0, n_pairs // 2)
    def _(i):
        for c in weight_copies(i):
            c.wait()

        @pl.when(i < n_pairs // 2 - 2)
        def _():
            for c in weight_copies(i + 2):
                c.start()

        @pl.when(i < n_pairs // 2 - 1)
        def _():
            mem_copy(2 * i).start()
            mem_copy(2 * i + 1).start()

        q = (dot(x_scr[...], m_scr[wq_at:wo_at, :, wide(i)].reshape(width, 2 * PAIR), NN) + vec_scr[2:3, wide(i)]).astype(BF16)
        d = dot(gy_scr[...], m_scr[wo_at + i], NT).astype(BF16)
        for p in range(2):
            k = 2 * i + p
            q2, d2 = (split_heads(t[:, p * PAIR:(p + 1) * PAIR].astype(F32), n_seq) for t in (q, d))
            q2_scr[k] = q2
            d2_scr[k] = d2
            place(zg_scr, 0, k, q2, lambda j, step: wk_scr[j:j + step, cols(k)])
            place(zg_scr, 1, k, d2, lambda j, step: wv_scr[j:j + step, cols(k)])
            ps_scr[k] = dot(d2, jnp.broadcast_to(pair_of(vec_scr, 3, k).astype(BF16), (PAIR, PAIR)), NT)

    for g in (n_pairs - 2, n_pairs - 1):
        mem_copy(g).start()
    for c in q_copies():
        c.start()

    pl.semaphore_wait(barrier, n_cp - 1)

    @pl.loop(0, n_pairs)
    def _(g):
        grp = lax.div(g, per_grp)

        @pl.when((g > 0) & (lax.rem(g, per_grp) == 0))
        def _():
            for c in stats_copies(grp - 1):
                c.start()

        mem_copy(g).wait()
        for j in range(n_blk):
            b = g * n_blk + j
            at = pl.ds(lax.rem(g, per_grp) * n_blk + j, 1)
            t = dot(m_scr[b], zg_scr[:, :, seq_rows(b), :].reshape(2 * rows, width), NT)
            s = t[:, :rows] * scale
            dp = t[:, rows:] + ps_scr[:, seq_rows(b), :].reshape(rows, PAIR).T[0:1, :]
            mx = jnp.max(s, axis=0, keepdims=True)
            e = jnp.exp(s - mx)
            e_scr[g, j * n_fr:(j + 1) * n_fr, :] = e
            dp_scr[g, j * n_fr:(j + 1) * n_fr, :] = dp
            st_scr[grp, 0, at, :] = mx
            st_scr[grp, 1, at, :] = jnp.sum(e, axis=0, keepdims=True)
            st_scr[grp, 2, at, :] = jnp.sum(e * dp, axis=0, keepdims=True)

    for c in stats_copies(n_grp - 1):
        c.start()

    @pl.loop(0, n_pairs)
    def _(g):
        grp = lax.div(g, per_grp)

        @pl.when(lax.rem(g, per_grp) == 0)
        def _():
            for c in stats_copies(grp):
                c.wait()

        @pl.when(g >= 2)
        def _():
            pg_copy(g - 2).wait()

        slot = lax.rem(g, 2)
        ones = jnp.ones((n_fr, PAIR), BF16)
        for j in range(n_blk):
            b = g * n_blk + j
            at = pl.ds(lax.rem(g, per_grp) * n_blk + j, 1)
            tops, sums_l, sums_c = ([st_scr[grp, n, at, :]] + [other[k, grp, n, at, :] for k in range(n_cp - 1)] for n in range(3))
            top = functools.reduce(jnp.maximum, tops)
            fac = [jnp.exp(t - top) for t in tops]
            total = functools.reduce(jnp.add, [f * v for f, v in zip(fac, sums_l)])
            c = functools.reduce(jnp.add, [f * v for f, v in zip(fac, sums_c)]) / total
            p = e_scr[g, j * n_fr:(j + 1) * n_fr, :] * (fac[0] / total)
            gr = p * (dp_scr[g, j * n_fr:(j + 1) * n_fr, :] - c) * scale
            pg = jnp.concatenate([gr.astype(BF16), p.astype(BF16)], axis=1)
            pg_scr[slot, j] = pg
            pgt = pg.T
            step = 256
            for w in range(0, width, step):
                t = dot(pgt, m_scr[b, :, w:w + step], NN).astype(BF16)
                zg_scr[:, :, seq_rows(b), w:w + step] = t.reshape(2, n_pairs, n_row, step)
            ps_scr[:, seq_rows(b), :] = dot(pgt[rows:], ones, NN).reshape(n_pairs, n_row, PAIR)
        pg_copy(g).start()

    def o_and_dq(k):
        o = join_heads(dot(zg_scr[1, k], wv_scr[:, cols(k)], NN), n_seq) + join_heads(ps_scr[k], n_seq) * pair_of(vec_scr, 3, k)
        dq = join_heads(dot(zg_scr[0, k], wk_scr[:, cols(k)], NN), n_seq)
        for part, t in enumerate((o, dq)):
            top, bottom = t[:t.shape[0] // 2], t[t.shape[0] // 2:]
            mine_oq[k, part] = jnp.where(first, top, bottom)
            theirs_oq[k, part] = jnp.where(first, bottom, top)

    lag = 2
    for h in range(n_part):
        for k in range(h * n_each, (h + 1) * n_each):
            o_and_dq(k)
        oq_mate(h).start()
        if h >= lag:
            add_mate(h - lag)
            oq_across(h - lag).start()

    def close_dw(k):
        dw_mate(k).wait()
        e_scr[k] += got_dw[k]

    @pl.loop(0, n_pairs)
    def _(k):
        @pl.when(k >= 1)
        def _():
            dw_mate(k - 1).start()

        for n in range(lag):
            @pl.when(k == n + 1)
            def _():
                oq_across(n_part - lag + n).start()

        @pl.when(k == 5)
        def _():
            head_copy().start()

        @pl.when(k >= 6)
        def _():
            for c in chip_copies(k - 5):
                c.start()

        small_scr[me, 1, pl.ds(k, 1), :] = jnp.sum(ps_scr[k] * d2_scr[k].astype(F32), axis=0, keepdims=True)
        dwk = dot(zg_scr[0, k], q2_scr[k], TN)
        dwv = dot(zg_scr[1, k], d2_scr[k], TN)
        e_scr[k] = jnp.where(first, dwk, dwv)
        dp_scr[k] = jnp.where(first, dwv, dwk)

        for n in range(lag):
            @pl.when(k == n)
            def _():
                add_mate(n_part - lag + n)

        @pl.when(k >= 4)
        def _():
            close_dw(k - 4)

    dw_mate(n_pairs - 1).start()

    @pl.loop(n_pairs - 4, n_pairs)
    def _(k):
        close_dw(k)

    @pl.loop(n_pairs - 5, n_pairs)
    def _(k):
        for c in chip_copies(k):
            c.start()

    for h in range(n_part):
        finish(h)
        own_across(h).start()
    for k in range(n_cp - 1):
        small_copy(k).start()
    head_across().start()
    for h in range(n_part):
        own_across(h).wait()
        half_mate(h).start()
    for k in range(n_cp - 1):
        small_copy(k).wait()
    small_ref[...] = small_scr[0] + small_scr[1] + small_scr[2] + small_scr[3]
    for h in range(n_part):
        half_mate(h).wait()
    for c in out_copies():
        c.start()

    @pl.loop(1, n_pairs)
    def _(k):
        for c in chip_copies(k):
            c.wait()

    head_copy().wait()
    for g in (n_pairs - 2, n_pairs - 1):
        pg_copy(g).wait()
    for c in q_copies() + out_copies():
        c.wait()
    head_across().wait()


def assemble_kernel(core_ref, own_ref, got_ref, own2_ref, got2_ref, head_ref, head2_ref, *refs):
    wk_ref, wv_ref = refs[-2:]
    first = core_ref[0] == 0
    mine, other = own_ref[...] + got_ref[...], own2_ref[...] + got2_ref[...]
    wk_ref[:, :PAIR] = jnp.where(first, head_ref[...], head2_ref[...])
    wv_ref[:, :PAIR] = jnp.where(first, head2_ref[...], head_ref[...])
    wk_ref[:, PAIR:] = jnp.where(first, mine, other)
    wv_ref[:, PAIR:] = jnp.where(first, other, mine)


def assemble(core, own, got, own2, got2, head, head2, at, acc):
    n, width = own.shape[0], own.shape[1] + PAIR
    step = next(k for k in (256, 192, 128, 64) if n % k == 0 and at % k == 0)
    block = pl.BlockSpec((step, width - PAIR), lambda i: (i, 0))
    head_block = pl.BlockSpec((step, PAIR), lambda i: (at // step + i, 0))
    out = pl.BlockSpec((step, width), lambda i: (at // step + i, 0))
    return pl.pallas_call(
        assemble_kernel, grid=(n // step,), name="assemble",
        in_specs=[pl.BlockSpec(memory_space=pltpu.SMEM)] + [block] * 4 + [head_block] * 2
        + [pl.BlockSpec(memory_space=pl.ANY)] * len(acc),
        out_specs=[out, out], out_shape=[jax.ShapeDtypeStruct((width, width), F32)] * 2,
        input_output_aliases={7: 0, 8: 1} if acc else {},
        compiler_params=params(),
    )(core, own, got, own2, got2, head, head2, *acc)


def mem_kernel(n_first, q2_ref, d2_ref, wk_ref, wv_ref, pg_ref, dm_ref, z_scr):
    i = pl.program_id(0)
    _, n_pairs, _, width = z_scr.shape
    n_blk = pg_ref.shape[0]
    n_row = pg_ref.shape[2] // (2 * n_pairs)

    @pl.when(i < n_first)
    def _():
        place(z_scr, 0, i, q2_ref[0], lambda j, step: wk_ref[j:j + step, :])
        place(z_scr, 1, i, d2_ref[0], lambda j, step: wv_ref[j:j + step, :])

    @pl.when(i >= n_first)
    def _():
        for j in range(n_blk):
            b = (i - n_first) * n_blk + j
            at = pl.ds(pl.multiple_of(b * n_row, n_row), n_row)
            z = z_scr[:, :, at, :].reshape(pg_ref.shape[2], width)
            dm_ref[j] = dot(pg_ref[j], z, NN).astype(BF16)


def params():
    return pltpu.CompilerParams(dimension_semantics=("arbitrary",), vmem_limit_bytes=VMEM_LIMIT)


def solution(mesh):
    act_spec = P("dp", None, None)
    mem_spec = P("dp", "cp", None)
    vec_out = P("dp")
    mat_out = P("dp", None)
    in_specs = (act_spec, mem_spec, P(), P(), P(), P(), P(), P(), P(), P(), P(), act_spec)
    out_specs = (act_spec, act_spec, mem_spec, vec_out, vec_out, mat_out, vec_out, mat_out, mat_out, vec_out, mat_out, vec_out)
    n_cp = mesh.shape["cp"]

    def swap(x, bit):
        return lax.ppermute(x, "cp", [(i, i ^ bit) for i in range(n_cp)])

    def device_step(hidden, memory, ln_gain, ln_bias, w_q, b_q, w_k, w_v, b_v, w_o, b_o, grad_y):
        n_seq, n_tok, width = hidden.shape
        n_fr = memory.shape[1]
        n_heads = width // HEAD
        n_pairs = n_heads // 2
        rows = n_heads * n_tok
        tokens = n_seq * n_tok
        scale = HEAD ** -0.5
        core = lax.axis_index("cp") % 2
        h2, gy2 = hidden.reshape(tokens, width), grad_y.reshape(tokens, width)
        blk = n_seq // n_pairs
        quarter = tokens // 4
        chunks = [width // 2, width // 4, width * 3 // 16, width // 16]
        anywhere = pl.BlockSpec(memory_space=pl.ANY)
        vm = lambda dt, *s: pltpu.VMEM(s, dt)
        sems = lambda *n: pltpu.SemaphoreType.DMA(n)
        both = lambda n: [sems(n)] * 2
        pg, *rest = pl.pallas_call(
            functools.partial(fused_kernel, scale, n_cp), name="fused",
            in_specs=[anywhere] * 11,
            out_specs=[anywhere] * 10 + [pl.BlockSpec(memory_space=pltpu.VMEM)],
            out_shape=[jax.ShapeDtypeStruct((n_seq, n_fr, 2 * rows), BF16)]
            + [jax.ShapeDtypeStruct((c, width - PAIR), F32) for c in chunks]
            + [jax.ShapeDtypeStruct((width, PAIR), F32)] * 2
            + [jax.ShapeDtypeStruct((2, tokens, width), BF16)]
            + [jax.ShapeDtypeStruct((n_pairs, 2 * tokens, PAIR), BF16)] * 2
            + [jax.ShapeDtypeStruct((2, n_pairs, PAIR), F32)],
            scratch_shapes=[vm(BF16, tokens, width), vm(BF16, tokens, width)] + [vm(BF16, width)] * 4 + [vm(F32, 4, width),
                            vm(BF16, 2, n_pairs, 2 * tokens, width), vm(BF16, n_seq, n_fr, width),
                            vm(F32, n_pairs, blk * n_fr, rows), vm(F32, n_pairs, blk * n_fr, rows),
                            vm(BF16, width, width), vm(BF16, width, width), vm(F32, n_pairs, 2 * tokens, PAIR),
                            vm(BF16, n_pairs, 2 * tokens, PAIR), vm(BF16, n_pairs, 2 * tokens, PAIR),
                            vm(F32, 4, 3, n_seq // 4, rows), vm(F32, n_cp - 1, 4, 3, n_seq // 4, rows),
                            vm(F32, n_pairs, 2, 2 * quarter, PAIR), vm(F32, n_pairs, 2, 2 * quarter, PAIR),
                            vm(F32, n_pairs, 2, 2 * quarter, PAIR), vm(F32, n_pairs, 2, quarter, PAIR),
                            vm(F32, n_pairs, 2, quarter, PAIR), vm(F32, n_pairs, 2, quarter, PAIR),
                            vm(BF16, n_pairs, 2, tokens, PAIR), vm(F32, n_cp, 2, n_pairs, PAIR),
                            vm(F32, n_pairs, width, PAIR),
                            sems(6), sems(4, n_pairs // 2), sems(n_pairs), sems(2), sems(4, n_pairs), sems(1), sems(2, n_pairs),
                            sems(2), vm(BF16, 2, blk, n_fr, 2 * rows)]
            + [sems(n_cp - 1, 4)] * 2 + both(n_pairs) + both(n_pairs) + both(n_pairs) + both(n_pairs) + both(n_pairs) + both(n_cp - 1) + both(1),
            compiler_params=pltpu.CompilerParams(vmem_limit_bytes=VMEM_LIMIT, collective_id=0, has_side_effects=True),
        )(h2, gy2, w_q.reshape(blk, n_fr, width), w_k, w_v, w_o.reshape(blk, n_fr, width), memory, ln_gain, ln_bias, b_q, b_v)
        chips, (head, head_got, oq, q2, d2, small) = rest[:4], rest[4:]
        attn_out, dq_low = oq[0], oq[1]
        small = small.reshape(2, width)
        grad_bq, grad_bv = small[0], small[1]

        got, chips2 = [], []
        for c in chips:
            got.append(swap(c, 2))
        for c in chips:
            chips2.append(swap(c, 1))
        head = head + head_got
        head2 = swap(head, 1)

        hidden_f32 = h2.astype(F32)
        centered = hidden_f32 - jnp.mean(hidden_f32, axis=-1, keepdims=True)
        inv_std = lax.rsqrt(jnp.mean(centered * centered, axis=-1, keepdims=True) + EPS)
        x_hat = centered * inv_std
        gain_f32 = ln_gain.astype(F32)
        x_norm = (x_hat * gain_f32 + ln_bias.astype(F32)).astype(BF16)
        out_y = (hidden_f32 + dot(attn_out, w_o, NN) + b_o.astype(F32)).astype(BF16)
        grad_wo = dot(attn_out, gy2, TN)
        grad_bo = jnp.sum(gy2, axis=0, dtype=F32)
        grad_wq = dot(x_norm, dq_low, TN)
        d_xnorm = dot(dq_low, w_q, NT)
        grad_ln_gain = jnp.sum(d_xnorm * x_hat, axis=0)
        grad_ln_bias = jnp.sum(d_xnorm, axis=0)
        d_hat = d_xnorm * gain_f32
        d_hidden = inv_std * (d_hat - jnp.mean(d_hat, axis=-1, keepdims=True) - x_hat * jnp.mean(d_hat * x_hat, axis=-1, keepdims=True))
        grad_h = (gy2.astype(F32) + d_hidden).astype(BF16)

        pair_block = pl.BlockSpec((1, 2 * tokens, PAIR), lambda i: (jnp.minimum(i, n_pairs - 1), 0, 0))
        col_block = pl.BlockSpec((width, PAIR), lambda i: (0, jnp.minimum(i, n_pairs - 1)))
        late = lambda *s: pl.BlockSpec((blk,) + s, lambda i: (jnp.maximum(i - n_pairs, 0), 0, 0))
        grad_mem = pl.pallas_call(
            functools.partial(mem_kernel, n_pairs), grid=(2 * n_pairs,), name="mem",
            in_specs=[pair_block, pair_block, col_block, col_block, late(n_fr, 2 * rows)], out_specs=late(n_fr, width),
            out_shape=jax.ShapeDtypeStruct((n_seq, n_fr, width), BF16), compiler_params=params(),
            scratch_shapes=[vm(BF16, 2, n_pairs, 2 * tokens, width)],
            cost_estimate=pl.CostEstimate(flops=8 * n_seq * n_fr * rows * width, bytes_accessed=40 << 20, transcendentals=0),
        )(q2, d2, w_k, w_v, pg)

        hidden_work = (out_y, grad_h, grad_mem, grad_ln_gain, grad_ln_bias, grad_wq, grad_wo, grad_bo)
        got[0], hidden_work = lax.optimization_barrier((got[0], hidden_work))
        out_y, grad_h, grad_mem, grad_ln_gain, grad_ln_bias, grad_wq, grad_wo, grad_bo = hidden_work
        core_arr = core.reshape(1).astype(jnp.int32)
        acc, at = (), 0
        for c, c2, g in zip(chips, chips2, got):
            g, acc = lax.optimization_barrier((g, acc))
            acc = assemble(core_arr, c, g, c2, swap(g, 1), head, head2, at, acc)
            at += c.shape[0]
        grad_wk, grad_wv = acc
        return (out_y.reshape(hidden.shape), grad_h.reshape(hidden.shape), grad_mem, grad_ln_gain, grad_ln_bias,
                grad_wq, grad_bq, grad_wk, grad_wv, grad_bv, grad_wo, grad_bo)

    return jax.shard_map(device_step, mesh=mesh, in_specs=in_specs, out_specs=out_specs, check_vma=False)
```

```python
import functools

import jax
import jax.numpy as jnp
from jax import lax
from jax.experimental import pallas as pl
from jax.experimental.pallas import tpu as pltpu
from jax.sharding import PartitionSpec as P


EPS = 1e-5
HEAD = 64
PAIR = 2 * HEAD
F32 = jnp.float32
BF16 = jnp.bfloat16
NT = (((1,), (1,)), ((), ()))
TN = (((0,), (0,)), ((), ()))
NN = (((1,), (0,)), ((), ()))
VMEM_LIMIT = 67043328


def dot(a, b, dims):
    return lax.dot_general(a, b, dims, preferred_element_type=F32)


def split_heads(x, n_seq):
    x = x.reshape(n_seq, x.shape[0] // n_seq, PAIR)
    low = lax.broadcasted_iota(jnp.int32, x.shape, 2) < HEAD
    zero = jnp.zeros_like(x)
    both = jnp.concatenate([jnp.where(low, x, zero), jnp.where(low, zero, x)], axis=1)
    return both.astype(BF16).reshape(-1, PAIR)


def join_heads(x, n_seq):
    n_tok = x.shape[0] // (2 * n_seq)
    x = x.reshape(n_seq, 2 * n_tok, PAIR)
    low = lax.broadcasted_iota(jnp.int32, (n_seq, n_tok, PAIR), 2) < HEAD
    return jnp.where(low, x[:, :n_tok], x[:, n_tok:]).reshape(n_seq * n_tok, PAIR)


def normalize(h_ref, vec_ref, x_scr):
    h = h_ref[...].astype(F32)
    c = h - jnp.mean(h, axis=-1, keepdims=True)
    inv = lax.rsqrt(jnp.mean(c * c, axis=-1, keepdims=True) + EPS)
    x_scr[...] = (c * inv * vec_ref[0:1, :] + vec_ref[1:2, :]).astype(BF16)


def pair_of(vec_ref, row, i):
    return vec_ref[row:row + 1, pl.ds(pl.multiple_of(i * PAIR, PAIR), PAIR)]


def place(out_ref, part, i, x, weight):
    step = 256
    for j in range(0, out_ref.shape[3], step):
        out_ref[part, i, :, j:j + step] = dot(x, weight(j, step), NT).astype(BF16)


def send(src, dst, sems, k, peer):
    return pltpu.make_async_remote_copy(
        src_ref=src, dst_ref=dst, send_sem=sems[0].at[k], recv_sem=sems[1].at[k],
        device_id={"cp": peer}, device_id_type=pl.DeviceIdType.MESH)


def fused_kernel(scale, n_cp, h_ref, gy_ref, wq_ref, wk_ref, wv_ref, wo_ref, m_ref, *refs):
    fused_body(scale, n_cp, h_ref, gy_ref, wq_ref, wk_ref, wv_ref, wo_ref, m_ref, refs[:4], *refs[4:])


def fused_body(scale, n_cp, h_ref, gy_ref, wq_ref, wk_ref, wv_ref, wo_ref, m_ref, vec_refs,
                 pg_ref, chip0_ref, chip1_ref, chip2_ref, chip3_ref, head_ref, head_got, oq_ref, q2_out, d2_out, small_ref,
                 x_scr, gy_scr, raw0, raw1, raw2, raw3, vec_scr, zg_scr, m_scr, e_scr, dp_scr, wk_scr, wv_scr, ps_scr, q2_scr, d2_scr, st_scr, other,
                 part_oq, got_oq, keep_x, give_x, got_x, full_oq, small_scr, got_dw,
                 in_sem, w_sem, m_sem, q_sem, chip_sem, head_sem, out_sem, pg_sem, pg_scr,
                 st_s, st_r, rd_s, rd_r, rx_s, rx_r, ax_s, ax_r, ad_s, ad_r, dw_s, dw_r, sm_s, sm_r, xd_s, xd_r):
    _, n_pairs, n_rows, width = zg_scr.shape
    n_seq, n_fr, _ = m_scr.shape
    n_row = n_rows // n_seq
    rows = n_row * n_pairs
    n_blk = n_seq // n_pairs
    share = keep_x.shape[3]
    group = 2 * share
    grp_seq = n_seq // st_scr.shape[0]
    n_grp = st_scr.shape[0]
    per_grp = n_pairs // n_grp
    me = lax.axis_index("cp")
    core = lax.rem(me, 2)
    chip = lax.div(me, 2)
    mate = me + 1 - 2 * core
    across = me + 2 - 4 * chip
    first = core == 0
    left = chip == 0
    peers = [lax.rem(me + d, n_cp) for d in range(1, n_cp)]
    wq_at, wo_at = n_seq - 2 * n_blk, n_seq - n_blk

    def cols(k):
        return pl.ds(pl.multiple_of(k * PAIR, PAIR), PAIR)

    def seq_rows(b):
        return pl.ds(pl.multiple_of(b * n_row, n_row), n_row)

    def wide(k):
        return pl.ds(pl.multiple_of(k * 2 * PAIR, 2 * PAIR), 2 * PAIR)

    def weight_copies(k):
        c = wide(k)
        return [pltpu.make_async_copy(wq_ref.at[:, :, c], m_scr.at[wq_at:wo_at, :, c], w_sem.at[0, k]),
                pltpu.make_async_copy(wo_ref.at[k], m_scr.at[wo_at + k], w_sem.at[1, k]),
                pltpu.make_async_copy(wk_ref.at[:, c], wk_scr.at[:, c], w_sem.at[2, k]),
                pltpu.make_async_copy(wv_ref.at[:, c], wv_scr.at[:, c], w_sem.at[3, k])]

    def mem_copy(g):
        at = pl.ds(g * n_blk, n_blk)
        return pltpu.make_async_copy(m_ref.at[at], m_scr.at[at], m_sem.at[g])

    def act_copies():
        return [pltpu.make_async_copy(src, dst, in_sem.at[k]) for k, (src, dst) in enumerate(
            zip((h_ref,) + tuple(vec_refs) + (gy_ref,), (x_scr, raw0, raw1, raw2, raw3, gy_scr)))]

    def q_copies():
        return [pltpu.make_async_copy(q2_scr, q2_out, q_sem.at[0]), pltpu.make_async_copy(d2_scr, d2_out, q_sem.at[1])]

    def chip_copies(k):
        out, at = [], 0
        for n, ref in enumerate((chip0_ref, chip1_ref, chip2_ref, chip3_ref)):
            out.append(pltpu.make_async_copy(e_scr.at[k, at:at + ref.shape[0], :], ref.at[:, cols(k - 1)], chip_sem.at[n, k]))
            at += ref.shape[0]
        return out

    def head_copy():
        return pltpu.make_async_copy(e_scr.at[0], head_ref, head_sem.at[0])

    def head_across():
        return send(e_scr.at[0], head_got, (xd_s, xd_r), 0, across)

    def out_copies():
        return [pltpu.make_async_copy(full_oq.at[k, p], oq_ref.at[p, :, k * PAIR:(k + 1) * PAIR], out_sem.at[p, k])
                for k in range(n_pairs) for p in range(2)]

    def pg_copy(g):
        slot = lax.rem(g, 2)
        return pltpu.make_async_copy(pg_scr.at[slot], pg_ref.at[pl.ds(g * n_blk, n_blk)], pg_sem.at[slot])

    def stats_copies(q):
        return [pltpu.make_async_remote_copy(
            src_ref=st_scr.at[q], dst_ref=other.at[k, q], send_sem=st_s.at[k, q], recv_sem=st_r.at[k, q],
            device_id={"cp": peers[k]}, device_id_type=pl.DeviceIdType.MESH) for k in range(n_cp - 1)]

    def oq_mate(g):
        j = lax.rem(g, 2)
        return send(part_oq.at[g], got_oq.at[j], (rd_s, rd_r), j, mate)

    def oq_across(j):
        return send(give_x.at[j], got_x.at[j], (rx_s, rx_r), j, across)

    def own_rows(j):
        return pl.ds(pl.multiple_of((2 * core + j) * group + chip * share, share), share)

    def own_across(j):
        at = own_rows(j)
        return send(full_oq.at[:, :, at, :], full_oq.at[:, :, at, :], (ax_s, ax_r), j, across)

    def group_mate(j):
        at = pl.ds(pl.multiple_of((2 * core + j) * group, group), group)
        return send(full_oq.at[:, :, at, :], full_oq.at[:, :, at, :], (ad_s, ad_r), j, mate)

    def dw_mate(k):
        return send(dp_scr.at[k], got_dw.at[k], (dw_s, dw_r), k, mate)

    def small_copy(k):
        return send(small_scr.at[me], small_scr.at[me], (sm_s, sm_r), k, peers[k])

    def take_group(g):
        @pl.when(core == lax.div(g, 2))
        def _():
            j = lax.rem(g, 2)
            oq_mate(g).wait_recv()
            t = part_oq[g] + got_oq[j]
            top, bottom = t[:, :, :share], t[:, :, share:]
            keep_x[j] = jnp.where(left, top, bottom)
            give_x[j] = jnp.where(left, bottom, top)
            oq_across(j).start()

    def finish(j):
        oq_across(j).wait()
        t = keep_x[j] + got_x[j]
        full_oq[:, :, own_rows(j), :] = t.astype(BF16)
        total = jnp.sum(t[:, 1], axis=1)
        small_scr[me, 0] = total if j == 0 else small_scr[me, 0] + total

    for c in act_copies():
        c.start()

    for c in weight_copies(0):
        c.start()

    barrier = pltpu.get_barrier_semaphore()
    for peer in peers:
        pl.semaphore_signal(barrier, inc=1, device_id={"cp": peer}, device_id_type=pl.DeviceIdType.MESH)
    for c in act_copies():
        c.wait()
    for k, ref in enumerate((raw0, raw1, raw2, raw3)):
        vec_scr[k:k + 1, :] = ref[...].astype(F32).reshape(1, width)
    normalize(x_scr, vec_scr, x_scr)

    @pl.loop(0, n_pairs // 2)
    def _(i):
        @pl.when(i < n_pairs // 2 - 1)
        def _():
            for c in weight_copies(i + 1):
                c.start()

        for c in weight_copies(i):
            c.wait()

        @pl.when(i < n_pairs // 2 - 1)
        def _():
            mem_copy(2 * i).start()
            mem_copy(2 * i + 1).start()

        q = (dot(x_scr[...], m_scr[wq_at:wo_at, :, wide(i)].reshape(width, 2 * PAIR), NN) + vec_scr[2:3, wide(i)]).astype(BF16)
        d = dot(gy_scr[...], m_scr[wo_at + i], NT).astype(BF16)
        for p in range(2):
            k = 2 * i + p
            q2, d2 = (split_heads(t[:, p * PAIR:(p + 1) * PAIR].astype(F32), n_seq) for t in (q, d))
            q2_scr[k] = q2
            d2_scr[k] = d2
            place(zg_scr, 0, k, q2, lambda j, step: wk_scr[j:j + step, cols(k)])
            place(zg_scr, 1, k, d2, lambda j, step: wv_scr[j:j + step, cols(k)])
            ps_scr[k] = dot(d2, jnp.broadcast_to(pair_of(vec_scr, 3, k).astype(BF16), (PAIR, PAIR)), NT)

    for g in (n_pairs - 2, n_pairs - 1):
        mem_copy(g).start()
    for c in q_copies():
        c.start()

    pl.semaphore_wait(barrier, n_cp - 1)

    @pl.loop(0, n_grp)
    def _(grp):
        @pl.when(grp > 0)
        def _():
            for c in stats_copies(grp - 1):
                c.start()

        for n in range(per_grp):
            mem_copy(grp * per_grp + n).wait()
        for j in range(per_grp * n_blk):
            g, r0 = grp * per_grp + j // n_blk, j % n_blk * n_fr
            b = grp * per_grp * n_blk + j
            t = dot(m_scr[b], zg_scr[:, :, seq_rows(b), :].reshape(2 * rows, width), NT)
            s = t[:, :rows] * scale
            dp = t[:, rows:] + ps_scr[:, seq_rows(b), :].reshape(rows, PAIR).T[0:1, :]
            mx = jnp.max(s, axis=0, keepdims=True)
            e = jnp.exp(s - mx)
            e_scr[g, r0:r0 + n_fr, :] = e
            dp_scr[g, r0:r0 + n_fr, :] = dp
            st_scr[grp, 0, j:j + 1, :] = mx
            st_scr[grp, 1, j:j + 1, :] = jnp.sum(e, axis=0, keepdims=True)
            st_scr[grp, 2, j:j + 1, :] = jnp.sum(e * dp, axis=0, keepdims=True)

    for c in stats_copies(n_grp - 1):
        c.start()

    @pl.loop(0, n_grp)
    def _(grp):
        for c in stats_copies(grp):
            c.wait()

        @pl.when(grp > 0)
        def _():
            for n in range(per_grp):
                pg_copy((grp - 1) * per_grp + n).wait()

        ones = jnp.ones((n_fr, PAIR), BF16)
        for j in range(per_grp * n_blk):
            g, r0 = grp * per_grp + j // n_blk, j % n_blk * n_fr
            b = grp * per_grp * n_blk + j
            tops, sums_l, sums_c = ([st_scr[grp, n, j:j + 1, :]] + [other[k, grp, n, j:j + 1, :] for k in range(n_cp - 1)]
                                    for n in range(3))
            top = functools.reduce(jnp.maximum, tops)
            fac = [jnp.exp(t - top) for t in tops]
            total = functools.reduce(jnp.add, [f * v for f, v in zip(fac, sums_l)])
            c = functools.reduce(jnp.add, [f * v for f, v in zip(fac, sums_c)]) / total
            p = e_scr[g, r0:r0 + n_fr, :] * (fac[0] / total)
            gr = p * (dp_scr[g, r0:r0 + n_fr, :] - c) * scale
            pg = jnp.concatenate([gr.astype(BF16), p.astype(BF16)], axis=1)
            pg_scr[j // n_blk, j % n_blk] = pg
            pgt = pg.T
            step = 256
            for w in range(0, width, step):
                t = dot(pgt, m_scr[b, :, w:w + step], NN).astype(BF16)
                zg_scr[:, :, seq_rows(b), w:w + step] = t.reshape(2, n_pairs, n_row, step)
            ps_scr[:, seq_rows(b), :] = dot(pgt[rows:], ones, NN).reshape(n_pairs, n_row, PAIR)
        for n in range(per_grp):
            pg_copy(grp * per_grp + n).start()

        @pl.when(grp > 0)
        def _():
            take_group(grp - 1)

        at = pl.ds(pl.multiple_of(grp * (grp_seq * n_row), grp_seq * n_row), grp_seq * n_row)
        for k in range(n_pairs):
            c = slice(k * PAIR, (k + 1) * PAIR)
            sums = join_heads(ps_scr[k, at, :], grp_seq)
            part_oq[grp, k, 0] = join_heads(dot(zg_scr[1, k, at, :], wv_scr[:, c], NN), grp_seq) + sums * vec_scr[3:4, c]
            part_oq[grp, k, 1] = join_heads(dot(zg_scr[0, k, at, :], wk_scr[:, c], NN), grp_seq)

        @pl.when(core != lax.div(grp, 2))
        def _():
            oq_mate(grp).start()

    def close_dw(k):
        dw_mate(k).wait()
        e_scr[k] += got_dw[k]

    @pl.loop(0, n_pairs)
    def _(k):
        @pl.when(k >= 1)
        def _():
            dw_mate(k - 1).start()

        @pl.when(k == 5)
        def _():
            head_copy().start()

        @pl.when(k >= 6)
        def _():
            for c in chip_copies(k - 5):
                c.start()

        small_scr[me, 1, pl.ds(k, 1), :] = jnp.sum(ps_scr[k] * d2_scr[k].astype(F32), axis=0, keepdims=True)
        dwk = dot(zg_scr[0, k], q2_scr[k], TN)
        dwv = dot(zg_scr[1, k], d2_scr[k], TN)
        e_scr[k] = jnp.where(first, dwk, dwv)
        dp_scr[k] = jnp.where(first, dwv, dwk)

        @pl.when(k == 2)
        def _():
            take_group(n_grp - 1)

        @pl.when(k >= 4)
        def _():
            close_dw(k - 4)

    dw_mate(n_pairs - 1).start()

    @pl.loop(n_pairs - 4, n_pairs)
    def _(k):
        close_dw(k)

    @pl.loop(n_pairs - 5, n_pairs)
    def _(k):
        for c in chip_copies(k):
            c.start()

    for j in range(2):
        finish(j)
        own_across(j).start()
    for k in range(n_cp - 1):
        small_copy(k).start()
    head_across().start()
    for j in range(2):
        own_across(j).wait()
        group_mate(j).start()
    for k in range(n_cp - 1):
        small_copy(k).wait()
    small_ref[...] = small_scr[0] + small_scr[1] + small_scr[2] + small_scr[3]
    for j in range(2):
        group_mate(j).wait()
        oq_mate(2 * (1 - core) + j).wait_send()
    for c in out_copies():
        c.start()

    @pl.loop(1, n_pairs)
    def _(k):
        for c in chip_copies(k):
            c.wait()

    head_copy().wait()
    for g in (n_pairs - 2, n_pairs - 1):
        pg_copy(g).wait()
    for c in q_copies() + out_copies():
        c.wait()
    head_across().wait()


def assemble_kernel(core_ref, own_ref, got_ref, own2_ref, got2_ref, head_ref, head2_ref, *refs):
    wk_ref, wv_ref = refs[-2:]
    first = core_ref[0] == 0
    mine, other = own_ref[...] + got_ref[...], own2_ref[...] + got2_ref[...]
    wk_ref[:, :PAIR] = jnp.where(first, head_ref[...], head2_ref[...])
    wv_ref[:, :PAIR] = jnp.where(first, head2_ref[...], head_ref[...])
    wk_ref[:, PAIR:] = jnp.where(first, mine, other)
    wv_ref[:, PAIR:] = jnp.where(first, other, mine)


def assemble(core, own, got, own2, got2, head, head2, at, acc):
    n, width = own.shape[0], own.shape[1] + PAIR
    step = next(k for k in (256, 192, 128, 64) if n % k == 0 and at % k == 0)
    block = pl.BlockSpec((step, width - PAIR), lambda i: (i, 0))
    head_block = pl.BlockSpec((step, PAIR), lambda i: (at // step + i, 0))
    out = pl.BlockSpec((step, width), lambda i: (at // step + i, 0))
    return pl.pallas_call(
        assemble_kernel, grid=(n // step,), name="assemble",
        in_specs=[pl.BlockSpec(memory_space=pltpu.SMEM)] + [block] * 4 + [head_block] * 2
        + [pl.BlockSpec(memory_space=pl.ANY)] * len(acc),
        out_specs=[out, out], out_shape=[jax.ShapeDtypeStruct((width, width), F32)] * 2,
        input_output_aliases={7: 0, 8: 1} if acc else {},
        compiler_params=params(),
    )(core, own, got, own2, got2, head, head2, *acc)


def mem_kernel(n_first, q2_ref, d2_ref, wk_ref, wv_ref, pg_ref, dm_ref, z_scr):
    i = pl.program_id(0)
    _, n_pairs, _, width = z_scr.shape
    n_blk = pg_ref.shape[0]
    n_row = pg_ref.shape[2] // (2 * n_pairs)

    @pl.when(i < n_first)
    def _():
        place(z_scr, 0, i, q2_ref[0], lambda j, step: wk_ref[j:j + step, :])
        place(z_scr, 1, i, d2_ref[0], lambda j, step: wv_ref[j:j + step, :])

    @pl.when(i >= n_first)
    def _():
        for j in range(n_blk):
            b = (i - n_first) * n_blk + j
            at = pl.ds(pl.multiple_of(b * n_row, n_row), n_row)
            z = z_scr[:, :, at, :].reshape(pg_ref.shape[2], width)
            dm_ref[j] = dot(pg_ref[j], z, NN).astype(BF16)


def params():
    return pltpu.CompilerParams(dimension_semantics=("arbitrary",), vmem_limit_bytes=VMEM_LIMIT)


def solution(mesh):
    act_spec = P("dp", None, None)
    mem_spec = P("dp", "cp", None)
    vec_out = P("dp")
    mat_out = P("dp", None)
    in_specs = (act_spec, mem_spec, P(), P(), P(), P(), P(), P(), P(), P(), P(), act_spec)
    out_specs = (act_spec, act_spec, mem_spec, vec_out, vec_out, mat_out, vec_out, mat_out, mat_out, vec_out, mat_out, vec_out)
    n_cp = mesh.shape["cp"]

    def swap(x, bit):
        return lax.ppermute(x, "cp", [(i, i ^ bit) for i in range(n_cp)])

    def device_step(hidden, memory, ln_gain, ln_bias, w_q, b_q, w_k, w_v, b_v, w_o, b_o, grad_y):
        n_seq, n_tok, width = hidden.shape
        n_fr = memory.shape[1]
        n_heads = width // HEAD
        n_pairs = n_heads // 2
        rows = n_heads * n_tok
        tokens = n_seq * n_tok
        scale = HEAD ** -0.5
        core = lax.axis_index("cp") % 2
        h2, gy2 = hidden.reshape(tokens, width), grad_y.reshape(tokens, width)
        blk = n_seq // n_pairs
        quarter = tokens // 4
        chunks = [width // 2, width // 4, width * 3 // 16, width // 16]
        anywhere = pl.BlockSpec(memory_space=pl.ANY)
        vm = lambda dt, *s: pltpu.VMEM(s, dt)
        sems = lambda *n: pltpu.SemaphoreType.DMA(n)
        both = lambda n: [sems(n)] * 2
        pg, *rest = pl.pallas_call(
            functools.partial(fused_kernel, scale, n_cp), name="fused",
            in_specs=[anywhere] * 11,
            out_specs=[anywhere] * 10 + [pl.BlockSpec(memory_space=pltpu.VMEM)],
            out_shape=[jax.ShapeDtypeStruct((n_seq, n_fr, 2 * rows), BF16)]
            + [jax.ShapeDtypeStruct((c, width - PAIR), F32) for c in chunks]
            + [jax.ShapeDtypeStruct((width, PAIR), F32)] * 2
            + [jax.ShapeDtypeStruct((2, tokens, width), BF16)]
            + [jax.ShapeDtypeStruct((n_pairs, 2 * tokens, PAIR), BF16)] * 2
            + [jax.ShapeDtypeStruct((2, n_pairs, PAIR), F32)],
            scratch_shapes=[vm(BF16, tokens, width), vm(BF16, tokens, width)] + [vm(BF16, width)] * 4 + [vm(F32, 4, width),
                            vm(BF16, 2, n_pairs, 2 * tokens, width), vm(BF16, n_seq, n_fr, width),
                            vm(F32, n_pairs, blk * n_fr, rows), vm(F32, n_pairs, blk * n_fr, rows),
                            vm(BF16, width, width), vm(BF16, width, width), vm(F32, n_pairs, 2 * tokens, PAIR),
                            vm(BF16, n_pairs, 2 * tokens, PAIR), vm(BF16, n_pairs, 2 * tokens, PAIR),
                            vm(F32, 4, 3, n_seq // 4, rows), vm(F32, n_cp - 1, 4, 3, n_seq // 4, rows),
                            vm(F32, 4, n_pairs, 2, quarter, PAIR), vm(F32, 2, n_pairs, 2, quarter, PAIR)]
            + [vm(F32, 2, n_pairs, 2, quarter // 2, PAIR)] * 3 + [
                            vm(BF16, n_pairs, 2, tokens, PAIR), vm(F32, n_cp, 2, n_pairs, PAIR),
                            vm(F32, n_pairs, width, PAIR),
                            sems(6), sems(4, n_pairs // 2), sems(n_pairs), sems(2), sems(4, n_pairs), sems(1), sems(2, n_pairs),
                            sems(2), vm(BF16, 2, blk, n_fr, 2 * rows)]
            + [sems(n_cp - 1, 4)] * 2 + both(2) + both(2) + both(2) + both(2) + both(n_pairs) + both(n_cp - 1) + both(1),
            compiler_params=pltpu.CompilerParams(vmem_limit_bytes=VMEM_LIMIT, collective_id=0, has_side_effects=True),
        )(h2, gy2, w_q.reshape(blk, n_fr, width), w_k, w_v, w_o.reshape(blk, n_fr, width), memory, ln_gain, ln_bias, b_q, b_v)
        chips, (head, head_got, oq, q2, d2, small) = rest[:4], rest[4:]
        attn_out, dq_low = oq[0], oq[1]
        small = small.reshape(2, width)
        grad_bq, grad_bv = small[0], small[1]

        got, chips2 = [], []
        for c in chips:
            got.append(swap(c, 2))
        for c in chips:
            chips2.append(swap(c, 1))
        head = head + head_got
        head2 = swap(head, 1)

        hidden_f32 = h2.astype(F32)
        centered = hidden_f32 - jnp.mean(hidden_f32, axis=-1, keepdims=True)
        inv_std = lax.rsqrt(jnp.mean(centered * centered, axis=-1, keepdims=True) + EPS)
        x_hat = centered * inv_std
        gain_f32 = ln_gain.astype(F32)
        x_norm = (x_hat * gain_f32 + ln_bias.astype(F32)).astype(BF16)
        out_y = (hidden_f32 + dot(attn_out, w_o, NN) + b_o.astype(F32)).astype(BF16)
        grad_wo = dot(attn_out, gy2, TN)
        grad_bo = jnp.sum(gy2, axis=0, dtype=F32)
        grad_wq = dot(x_norm, dq_low, TN)
        d_xnorm = dot(dq_low, w_q, NT)
        grad_ln_gain = jnp.sum(d_xnorm * x_hat, axis=0)
        grad_ln_bias = jnp.sum(d_xnorm, axis=0)
        d_hat = d_xnorm * gain_f32
        d_hidden = inv_std * (d_hat - jnp.mean(d_hat, axis=-1, keepdims=True) - x_hat * jnp.mean(d_hat * x_hat, axis=-1, keepdims=True))
        grad_h = (gy2.astype(F32) + d_hidden).astype(BF16)

        pair_block = pl.BlockSpec((1, 2 * tokens, PAIR), lambda i: (jnp.minimum(i, n_pairs - 1), 0, 0))
        col_block = pl.BlockSpec((width, PAIR), lambda i: (0, jnp.minimum(i, n_pairs - 1)))
        late = lambda *s: pl.BlockSpec((blk,) + s, lambda i: (jnp.maximum(i - n_pairs, 0), 0, 0))
        grad_mem = pl.pallas_call(
            functools.partial(mem_kernel, n_pairs), grid=(2 * n_pairs,), name="mem",
            in_specs=[pair_block, pair_block, col_block, col_block, late(n_fr, 2 * rows)], out_specs=late(n_fr, width),
            out_shape=jax.ShapeDtypeStruct((n_seq, n_fr, width), BF16), compiler_params=params(),
            scratch_shapes=[vm(BF16, 2, n_pairs, 2 * tokens, width)],
            cost_estimate=pl.CostEstimate(flops=8 * n_seq * n_fr * rows * width, bytes_accessed=40 << 20, transcendentals=0),
        )(q2, d2, w_k, w_v, pg)

        hidden_work = (out_y, grad_h, grad_mem, grad_ln_gain, grad_ln_bias, grad_wq, grad_wo, grad_bo)
        got[0], hidden_work = lax.optimization_barrier((got[0], hidden_work))
        out_y, grad_h, grad_mem, grad_ln_gain, grad_ln_bias, grad_wq, grad_wo, grad_bo = hidden_work
        core_arr = core.reshape(1).astype(jnp.int32)
        acc, at = (), 0
        for c, c2, g in zip(chips, chips2, got):
            g, acc = lax.optimization_barrier((g, acc))
            acc = assemble(core_arr, c, g, c2, swap(g, 1), head, head2, at, acc)
            at += c.shape[0]
        grad_wk, grad_wv = acc
        return (out_y.reshape(hidden.shape), grad_h.reshape(hidden.shape), grad_mem, grad_ln_gain, grad_ln_bias,
                grad_wq, grad_bq, grad_wk, grad_wv, grad_bv, grad_wo, grad_bo)

    return jax.shard_map(device_step, mesh=mesh, in_specs=in_specs, out_specs=out_specs, check_vma=False)
```

```python
import functools

import jax
import jax.numpy as jnp
from jax import lax
from jax.experimental import pallas as pl
from jax.experimental.pallas import tpu as pltpu
from jax.sharding import PartitionSpec as P


EPS = 1e-5
HEAD = 64
PAIR = 2 * HEAD
F32 = jnp.float32
BF16 = jnp.bfloat16
NT = (((1,), (1,)), ((), ()))
TN = (((0,), (0,)), ((), ()))
NN = (((1,), (0,)), ((), ()))
VMEM_LIMIT = 67043328


def dot(a, b, dims):
    return lax.dot_general(a, b, dims, preferred_element_type=F32)


def split_heads(x, n_seq):
    x = x.reshape(n_seq, x.shape[0] // n_seq, PAIR)
    low = lax.broadcasted_iota(jnp.int32, x.shape, 2) < HEAD
    zero = jnp.zeros_like(x)
    both = jnp.concatenate([jnp.where(low, x, zero), jnp.where(low, zero, x)], axis=1)
    return both.astype(BF16).reshape(-1, PAIR)


def join_heads(x, n_seq):
    n_tok = x.shape[0] // (2 * n_seq)
    x = x.reshape(n_seq, 2 * n_tok, PAIR)
    low = lax.broadcasted_iota(jnp.int32, (n_seq, n_tok, PAIR), 2) < HEAD
    return jnp.where(low, x[:, :n_tok], x[:, n_tok:]).reshape(n_seq * n_tok, PAIR)


def normalize(h_ref, vec_ref, x_scr):
    h = h_ref[...].astype(F32)
    c = h - jnp.mean(h, axis=-1, keepdims=True)
    inv = lax.rsqrt(jnp.mean(c * c, axis=-1, keepdims=True) + EPS)
    x_scr[...] = (c * inv * vec_ref[0:1, :] + vec_ref[1:2, :]).astype(BF16)


def pair_of(vec_ref, row, i):
    return vec_ref[row:row + 1, pl.ds(pl.multiple_of(i * PAIR, PAIR), PAIR)]


def place(out_ref, part, i, x, weight):
    step = 256
    for j in range(0, out_ref.shape[3], step):
        out_ref[part, i, :, j:j + step] = dot(x, weight(j, step), NT).astype(BF16)


def send(src, dst, sems, k, peer):
    return pltpu.make_async_remote_copy(
        src_ref=src, dst_ref=dst, send_sem=sems[0].at[k], recv_sem=sems[1].at[k],
        device_id={"cp": peer}, device_id_type=pl.DeviceIdType.MESH)


def fused_kernel(scale, n_cp, h_ref, gy_ref, wq_ref, wk_ref, wv_ref, wo_ref, m_ref, *refs):
    fused_body(scale, n_cp, h_ref, gy_ref, wq_ref, wk_ref, wv_ref, wo_ref, m_ref, refs[:4], *refs[4:])


def fused_body(scale, n_cp, h_ref, gy_ref, wq_ref, wk_ref, wv_ref, wo_ref, m_ref, vec_refs,
                 pg_ref, chip0_ref, chip1_ref, chip2_ref, chip3_ref, head_ref, head_got, oq_ref, q2_out, d2_out, small_ref,
                 x_scr, gy_scr, raw0, raw1, raw2, raw3, vec_scr, zg_scr, m_scr, e_scr, dp_scr, wk_scr, wv_scr, ps_scr, q2_scr, d2_scr, st_scr, other,
                 part_oq, got_oq, keep_x, give_x, got_x, full_oq, small_scr, got_dw,
                 in_sem, w_sem, m_sem, q_sem, chip_sem, head_sem, out_sem, pg_sem, pg_scr,
                 st_s, st_r, rd_s, rd_r, rx_s, rx_r, ax_s, ax_r, ad_s, ad_r, dw_s, dw_r, sm_s, sm_r, xd_s, xd_r):
    _, n_pairs, n_rows, width = zg_scr.shape
    n_seq, n_fr, _ = m_scr.shape
    n_row = n_rows // n_seq
    rows = n_row * n_pairs
    n_blk = n_seq // n_pairs
    share = keep_x.shape[3]
    group = 2 * share
    grp_seq = n_seq // st_scr.shape[0]
    n_grp = st_scr.shape[0]
    per_grp = n_pairs // n_grp
    me = lax.axis_index("cp")
    core = lax.rem(me, 2)
    chip = lax.div(me, 2)
    mate = me + 1 - 2 * core
    across = me + 2 - 4 * chip
    first = core == 0
    left = chip == 0
    peers = [lax.rem(me + d, n_cp) for d in range(1, n_cp)]
    wq_at, wo_at = n_seq - 2 * n_blk, n_seq - n_blk

    def cols(k):
        return pl.ds(pl.multiple_of(k * PAIR, PAIR), PAIR)

    def seq_rows(b):
        return pl.ds(pl.multiple_of(b * n_row, n_row), n_row)

    def wide(k):
        return pl.ds(pl.multiple_of(k * 2 * PAIR, 2 * PAIR), 2 * PAIR)

    def weight_copies(k):
        c = wide(k)
        return [pltpu.make_async_copy(wq_ref.at[:, :, c], m_scr.at[wq_at:wo_at, :, c], w_sem.at[0, k]),
                pltpu.make_async_copy(wo_ref.at[k], m_scr.at[wo_at + k], w_sem.at[1, k]),
                pltpu.make_async_copy(wk_ref.at[:, c], wk_scr.at[:, c], w_sem.at[2, k]),
                pltpu.make_async_copy(wv_ref.at[:, c], wv_scr.at[:, c], w_sem.at[3, k])]

    def mem_copy(g):
        at = pl.ds(g * n_blk, n_blk)
        return pltpu.make_async_copy(m_ref.at[at], m_scr.at[at], m_sem.at[g])

    def act_copies():
        return [pltpu.make_async_copy(src, dst, in_sem.at[k]) for k, (src, dst) in enumerate(
            zip((h_ref,) + tuple(vec_refs) + (gy_ref,), (x_scr, raw0, raw1, raw2, raw3, gy_scr)))]

    def q_copies():
        return [pltpu.make_async_copy(q2_scr, q2_out, q_sem.at[0]), pltpu.make_async_copy(d2_scr, d2_out, q_sem.at[1])]

    def chip_copies(k):
        out, at = [], 0
        for n, ref in enumerate((chip0_ref, chip1_ref, chip2_ref, chip3_ref)):
            out.append(pltpu.make_async_copy(e_scr.at[k, at:at + ref.shape[0], :], ref.at[:, cols(k - 1)], chip_sem.at[n, k]))
            at += ref.shape[0]
        return out

    def head_copy():
        return pltpu.make_async_copy(e_scr.at[0], head_ref, head_sem.at[0])

    def head_across(n):
        at = slice(n * width // 2, (n + 1) * width // 2)
        return send(e_scr.at[0, at], head_got.at[at], (xd_s, xd_r), n, across)

    def out_copies():
        return [pltpu.make_async_copy(full_oq.at[k, p], oq_ref.at[p, :, k * PAIR:(k + 1) * PAIR], out_sem.at[p, k])
                for k in range(n_pairs) for p in range(2)]

    def pg_copy(g):
        slot = lax.rem(g, 2)
        return pltpu.make_async_copy(pg_scr.at[slot], pg_ref.at[pl.ds(g * n_blk, n_blk)], pg_sem.at[slot])

    def stats_copies(q):
        return [pltpu.make_async_remote_copy(
            src_ref=st_scr.at[q], dst_ref=other.at[k, q], send_sem=st_s.at[k, q], recv_sem=st_r.at[k, q],
            device_id={"cp": peers[k]}, device_id_type=pl.DeviceIdType.MESH) for k in range(n_cp - 1)]

    def oq_mate(g):
        j = lax.rem(g, 2)
        return send(part_oq.at[g], got_oq.at[j], (rd_s, rd_r), j, mate)

    def oq_across(j):
        return send(give_x.at[j], got_x.at[j], (rx_s, rx_r), j, across)

    def own_rows(j):
        return pl.ds(pl.multiple_of((2 * core + j) * group + chip * share, share), share)

    def own_across(j):
        at = own_rows(j)
        return send(full_oq.at[:, :, at, :], full_oq.at[:, :, at, :], (ax_s, ax_r), j, across)

    def group_mate(j):
        at = pl.ds(pl.multiple_of((2 * core + j) * group, group), group)
        return send(full_oq.at[:, :, at, :], full_oq.at[:, :, at, :], (ad_s, ad_r), j, mate)

    def dw_mate(k):
        return send(dp_scr.at[k], got_dw.at[k], (dw_s, dw_r), k, mate)

    def small_copy(k):
        return send(small_scr.at[me], small_scr.at[me], (sm_s, sm_r), k, peers[k])

    def take_group(g):
        @pl.when(core == lax.div(g, 2))
        def _():
            j = lax.rem(g, 2)
            oq_mate(g).wait_recv()
            t = part_oq[g] + got_oq[j]
            top, bottom = t[:, :, :share], t[:, :, share:]
            keep_x[j] = jnp.where(left, top, bottom)
            give_x[j] = jnp.where(left, bottom, top)
            oq_across(j).start()

    def finish(j):
        oq_across(j).wait()
        t = keep_x[j] + got_x[j]
        full_oq[:, :, own_rows(j), :] = t.astype(BF16)
        total = jnp.sum(t[:, 1], axis=1)
        small_scr[me, 0] = total if j == 0 else small_scr[me, 0] + total

    for c in act_copies():
        c.start()

    for c in weight_copies(0):
        c.start()

    barrier = pltpu.get_barrier_semaphore()
    for peer in peers:
        pl.semaphore_signal(barrier, inc=1, device_id={"cp": peer}, device_id_type=pl.DeviceIdType.MESH)
    for c in act_copies():
        c.wait()
    for k, ref in enumerate((raw0, raw1, raw2, raw3)):
        vec_scr[k:k + 1, :] = ref[...].astype(F32).reshape(1, width)
    normalize(x_scr, vec_scr, x_scr)

    @pl.loop(0, n_pairs // 2)
    def _(i):
        @pl.when(i < n_pairs // 2 - 1)
        def _():
            for c in weight_copies(i + 1):
                c.start()

        for c in weight_copies(i):
            c.wait()

        @pl.when(i < n_pairs // 2 - 1)
        def _():
            mem_copy(2 * i).start()
            mem_copy(2 * i + 1).start()

        q = (dot(x_scr[...], m_scr[wq_at:wo_at, :, wide(i)].reshape(width, 2 * PAIR), NN) + vec_scr[2:3, wide(i)]).astype(BF16)
        d = dot(gy_scr[...], m_scr[wo_at + i], NT).astype(BF16)
        for p in range(2):
            k = 2 * i + p
            q2, d2 = (split_heads(t[:, p * PAIR:(p + 1) * PAIR].astype(F32), n_seq) for t in (q, d))
            q2_scr[k] = q2
            d2_scr[k] = d2
            place(zg_scr, 0, k, q2, lambda j, step: wk_scr[j:j + step, cols(k)])
            place(zg_scr, 1, k, d2, lambda j, step: wv_scr[j:j + step, cols(k)])
            ps_scr[k] = dot(d2, jnp.broadcast_to(pair_of(vec_scr, 3, k).astype(BF16), (PAIR, PAIR)), NT)

    for g in (n_pairs - 2, n_pairs - 1):
        mem_copy(g).start()
    for c in q_copies():
        c.start()

    pl.semaphore_wait(barrier, n_cp - 1)

    @pl.loop(0, n_grp)
    def _(grp):
        @pl.when(grp > 0)
        def _():
            for c in stats_copies(grp - 1):
                c.start()

        for n in range(per_grp):
            mem_copy(grp * per_grp + n).wait()
        for j in range(per_grp * n_blk):
            g, r0 = grp * per_grp + j // n_blk, j % n_blk * n_fr
            b = grp * per_grp * n_blk + j
            t = dot(m_scr[b], zg_scr[:, :, seq_rows(b), :].reshape(2 * rows, width), NT)
            s = t[:, :rows] * scale
            dp = t[:, rows:] + ps_scr[:, seq_rows(b), :].reshape(rows, PAIR).T[0:1, :]
            mx = jnp.max(s, axis=0, keepdims=True)
            e = jnp.exp(s - mx)
            e_scr[g, r0:r0 + n_fr, :] = e
            dp_scr[g, r0:r0 + n_fr, :] = dp
            st_scr[grp, 0, j:j + 1, :] = mx
            st_scr[grp, 1, j:j + 1, :] = jnp.sum(e, axis=0, keepdims=True)
            st_scr[grp, 2, j:j + 1, :] = jnp.sum(e * dp, axis=0, keepdims=True)

    for c in stats_copies(n_grp - 1):
        c.start()

    @pl.loop(0, n_grp)
    def _(grp):
        for c in stats_copies(grp):
            c.wait()

        @pl.when(grp > 0)
        def _():
            for n in range(per_grp):
                pg_copy((grp - 1) * per_grp + n).wait()

        ones = jnp.ones((n_fr, PAIR), BF16)
        for j in range(per_grp * n_blk):
            g, r0 = grp * per_grp + j // n_blk, j % n_blk * n_fr
            b = grp * per_grp * n_blk + j
            tops, sums_l, sums_c = ([st_scr[grp, n, j:j + 1, :]] + [other[k, grp, n, j:j + 1, :] for k in range(n_cp - 1)]
                                    for n in range(3))
            top = functools.reduce(jnp.maximum, tops)
            fac = [jnp.exp(t - top) for t in tops]
            total = functools.reduce(jnp.add, [f * v for f, v in zip(fac, sums_l)])
            c = functools.reduce(jnp.add, [f * v for f, v in zip(fac, sums_c)]) / total
            p = e_scr[g, r0:r0 + n_fr, :] * (fac[0] / total)
            gr = p * (dp_scr[g, r0:r0 + n_fr, :] - c) * scale
            pg = jnp.concatenate([gr.astype(BF16), p.astype(BF16)], axis=1)
            pg_scr[j // n_blk, j % n_blk] = pg
            pgt = pg.T
            step = 256
            for w in range(0, width, step):
                t = dot(pgt, m_scr[b, :, w:w + step], NN).astype(BF16)
                zg_scr[:, :, seq_rows(b), w:w + step] = t.reshape(2, n_pairs, n_row, step)
            ps_scr[:, seq_rows(b), :] = dot(pgt[rows:], ones, NN).reshape(n_pairs, n_row, PAIR)
        for n in range(per_grp):
            pg_copy(grp * per_grp + n).start()

        @pl.when(grp > 0)
        def _():
            take_group(grp - 1)

        at = pl.ds(pl.multiple_of(grp * (grp_seq * n_row), grp_seq * n_row), grp_seq * n_row)
        for k in range(n_pairs):
            c = slice(k * PAIR, (k + 1) * PAIR)
            sums = join_heads(ps_scr[k, at, :], grp_seq)
            part_oq[grp, k, 0] = join_heads(dot(zg_scr[1, k, at, :], wv_scr[:, c], NN), grp_seq) + sums * vec_scr[3:4, c]
            part_oq[grp, k, 1] = join_heads(dot(zg_scr[0, k, at, :], wk_scr[:, c], NN), grp_seq)

        @pl.when(core != lax.div(grp, 2))
        def _():
            oq_mate(grp).start()

    def close_dw(k):
        dw_mate(k).wait()
        e_scr[k] += got_dw[k]

    @pl.loop(0, n_pairs)
    def _(k):
        @pl.when(k >= 1)
        def _():
            dw_mate(k - 1).start()

        @pl.when(k == 5)
        def _():
            head_copy().start()
            head_across(0).start()

        @pl.when(k >= 6)
        def _():
            for c in chip_copies(k - 5):
                c.start()

        small_scr[me, 1, pl.ds(k, 1), :] = jnp.sum(ps_scr[k] * d2_scr[k].astype(F32), axis=0, keepdims=True)
        dwk = dot(zg_scr[0, k], q2_scr[k], TN)
        dwv = dot(zg_scr[1, k], d2_scr[k], TN)
        e_scr[k] = jnp.where(first, dwk, dwv)
        dp_scr[k] = jnp.where(first, dwv, dwk)

        @pl.when(k == 2)
        def _():
            take_group(n_grp - 1)

        @pl.when(k >= 4)
        def _():
            close_dw(k - 4)

        @pl.when(k == 6)
        def _():
            finish(0)

        @pl.when(k == 7)
        def _():
            own_across(0).start()

    dw_mate(n_pairs - 1).start()
    finish(1)
    own_across(1).start()

    @pl.loop(n_pairs - 4, n_pairs)
    def _(k):
        close_dw(k)

    @pl.loop(n_pairs - 5, n_pairs)
    def _(k):
        for c in chip_copies(k):
            c.start()

    for k in range(n_cp - 1):
        small_copy(k).start()
    head_across(1).start()
    for j in range(2):
        own_across(j).wait()
        group_mate(j).start()
    for k in range(n_cp - 1):
        small_copy(k).wait()
    small_ref[...] = small_scr[0] + small_scr[1] + small_scr[2] + small_scr[3]
    for j in range(2):
        group_mate(j).wait()
        oq_mate(2 * (1 - core) + j).wait_send()
    for c in out_copies():
        c.start()

    @pl.loop(1, n_pairs)
    def _(k):
        for c in chip_copies(k):
            c.wait()

    head_copy().wait()
    for g in (n_pairs - 2, n_pairs - 1):
        pg_copy(g).wait()
    for c in q_copies() + out_copies():
        c.wait()
    head_across(0).wait()
    head_across(1).wait()


def assemble_kernel(core_ref, own_ref, got_ref, own2_ref, got2_ref, head_ref, head2_ref, *refs):
    wk_ref, wv_ref = refs[-2:]
    first = core_ref[0] == 0
    mine, other = own_ref[...] + got_ref[...], own2_ref[...] + got2_ref[...]
    wk_ref[:, :PAIR] = jnp.where(first, head_ref[...], head2_ref[...])
    wv_ref[:, :PAIR] = jnp.where(first, head2_ref[...], head_ref[...])
    wk_ref[:, PAIR:] = jnp.where(first, mine, other)
    wv_ref[:, PAIR:] = jnp.where(first, other, mine)


def assemble(core, own, got, own2, got2, head, head2, at, acc):
    n, width = own.shape[0], own.shape[1] + PAIR
    step = next(k for k in (256, 192, 128, 64) if n % k == 0 and at % k == 0)
    block = pl.BlockSpec((step, width - PAIR), lambda i: (i, 0))
    head_block = pl.BlockSpec((step, PAIR), lambda i: (at // step + i, 0))
    out = pl.BlockSpec((step, width), lambda i: (at // step + i, 0))
    return pl.pallas_call(
        assemble_kernel, grid=(n // step,), name="assemble",
        in_specs=[pl.BlockSpec(memory_space=pltpu.SMEM)] + [block] * 4 + [head_block] * 2
        + [pl.BlockSpec(memory_space=pl.ANY)] * len(acc),
        out_specs=[out, out], out_shape=[jax.ShapeDtypeStruct((width, width), F32)] * 2,
        input_output_aliases={7: 0, 8: 1} if acc else {},
        compiler_params=params(),
    )(core, own, got, own2, got2, head, head2, *acc)


def mem_kernel(n_first, q2_ref, d2_ref, wk_ref, wv_ref, pg_ref, dm_ref, z_scr):
    i = pl.program_id(0)
    _, n_pairs, _, width = z_scr.shape
    n_blk = pg_ref.shape[0]
    n_row = pg_ref.shape[2] // (2 * n_pairs)

    @pl.when(i < n_first)
    def _():
        place(z_scr, 0, i, q2_ref[0], lambda j, step: wk_ref[j:j + step, :])
        place(z_scr, 1, i, d2_ref[0], lambda j, step: wv_ref[j:j + step, :])

    @pl.when(i >= n_first)
    def _():
        for j in range(n_blk):
            b = (i - n_first) * n_blk + j
            at = pl.ds(pl.multiple_of(b * n_row, n_row), n_row)
            z = z_scr[:, :, at, :].reshape(pg_ref.shape[2], width)
            dm_ref[j] = dot(pg_ref[j], z, NN).astype(BF16)


def params():
    return pltpu.CompilerParams(dimension_semantics=("arbitrary",), vmem_limit_bytes=VMEM_LIMIT)


def solution(mesh):
    act_spec = P("dp", None, None)
    mem_spec = P("dp", "cp", None)
    vec_out = P("dp")
    mat_out = P("dp", None)
    in_specs = (act_spec, mem_spec, P(), P(), P(), P(), P(), P(), P(), P(), P(), act_spec)
    out_specs = (act_spec, act_spec, mem_spec, vec_out, vec_out, mat_out, vec_out, mat_out, mat_out, vec_out, mat_out, vec_out)
    n_cp = mesh.shape["cp"]

    def swap(x, bit):
        return lax.ppermute(x, "cp", [(i, i ^ bit) for i in range(n_cp)])

    def device_step(hidden, memory, ln_gain, ln_bias, w_q, b_q, w_k, w_v, b_v, w_o, b_o, grad_y):
        n_seq, n_tok, width = hidden.shape
        n_fr = memory.shape[1]
        n_heads = width // HEAD
        n_pairs = n_heads // 2
        rows = n_heads * n_tok
        tokens = n_seq * n_tok
        scale = HEAD ** -0.5
        core = lax.axis_index("cp") % 2
        h2, gy2 = hidden.reshape(tokens, width), grad_y.reshape(tokens, width)
        blk = n_seq // n_pairs
        quarter = tokens // 4
        chunks = [width * 9 // 16, width // 4, width // 8, width // 16]
        anywhere = pl.BlockSpec(memory_space=pl.ANY)
        vm = lambda dt, *s: pltpu.VMEM(s, dt)
        sems = lambda *n: pltpu.SemaphoreType.DMA(n)
        both = lambda n: [sems(n)] * 2
        pg, *rest = pl.pallas_call(
            functools.partial(fused_kernel, scale, n_cp), name="fused",
            in_specs=[anywhere] * 11,
            out_specs=[anywhere] * 10 + [pl.BlockSpec(memory_space=pltpu.VMEM)],
            out_shape=[jax.ShapeDtypeStruct((n_seq, n_fr, 2 * rows), BF16)]
            + [jax.ShapeDtypeStruct((c, width - PAIR), F32) for c in chunks]
            + [jax.ShapeDtypeStruct((width, PAIR), F32)] * 2
            + [jax.ShapeDtypeStruct((2, tokens, width), BF16)]
            + [jax.ShapeDtypeStruct((n_pairs, 2 * tokens, PAIR), BF16)] * 2
            + [jax.ShapeDtypeStruct((2, n_pairs, PAIR), F32)],
            scratch_shapes=[vm(BF16, tokens, width), vm(BF16, tokens, width)] + [vm(BF16, width)] * 4 + [vm(F32, 4, width),
                            vm(BF16, 2, n_pairs, 2 * tokens, width), vm(BF16, n_seq, n_fr, width),
                            vm(F32, n_pairs, blk * n_fr, rows), vm(F32, n_pairs, blk * n_fr, rows),
                            vm(BF16, width, width), vm(BF16, width, width), vm(F32, n_pairs, 2 * tokens, PAIR),
                            vm(BF16, n_pairs, 2 * tokens, PAIR), vm(BF16, n_pairs, 2 * tokens, PAIR),
                            vm(F32, 4, 3, n_seq // 4, rows), vm(F32, n_cp - 1, 4, 3, n_seq // 4, rows),
                            vm(F32, 4, n_pairs, 2, quarter, PAIR), vm(F32, 2, n_pairs, 2, quarter, PAIR)]
            + [vm(F32, 2, n_pairs, 2, quarter // 2, PAIR)] * 3 + [
                            vm(BF16, n_pairs, 2, tokens, PAIR), vm(F32, n_cp, 2, n_pairs, PAIR),
                            vm(F32, n_pairs, width, PAIR),
                            sems(6), sems(4, n_pairs // 2), sems(n_pairs), sems(2), sems(4, n_pairs), sems(1), sems(2, n_pairs),
                            sems(2), vm(BF16, 2, blk, n_fr, 2 * rows)]
            + [sems(n_cp - 1, 4)] * 2 + both(2) + both(2) + both(2) + both(2) + both(n_pairs) + both(n_cp - 1) + both(2),
            compiler_params=pltpu.CompilerParams(vmem_limit_bytes=VMEM_LIMIT, collective_id=0, has_side_effects=True),
        )(h2, gy2, w_q.reshape(blk, n_fr, width), w_k, w_v, w_o.reshape(blk, n_fr, width), memory, ln_gain, ln_bias, b_q, b_v)
        chips, (head, head_got, oq, q2, d2, small) = rest[:4], rest[4:]
        attn_out, dq_low = oq[0], oq[1]
        small = small.reshape(2, width)
        grad_bq, grad_bv = small[0], small[1]

        got, chips2 = [], []
        for c in chips:
            got.append(swap(c, 2))
        for c in chips:
            chips2.append(swap(c, 1))
        head = head + head_got
        head2 = swap(head, 1)

        hidden_f32 = h2.astype(F32)
        centered = hidden_f32 - jnp.mean(hidden_f32, axis=-1, keepdims=True)
        inv_std = lax.rsqrt(jnp.mean(centered * centered, axis=-1, keepdims=True) + EPS)
        x_hat = centered * inv_std
        gain_f32 = ln_gain.astype(F32)
        x_norm = (x_hat * gain_f32 + ln_bias.astype(F32)).astype(BF16)
        out_y = (hidden_f32 + dot(attn_out, w_o, NN) + b_o.astype(F32)).astype(BF16)
        grad_wo = dot(attn_out, gy2, TN)
        grad_bo = jnp.sum(gy2, axis=0, dtype=F32)
        grad_wq = dot(x_norm, dq_low, TN)
        d_xnorm = dot(dq_low, w_q, NT)
        grad_ln_gain = jnp.sum(d_xnorm * x_hat, axis=0)
        grad_ln_bias = jnp.sum(d_xnorm, axis=0)
        d_hat = d_xnorm * gain_f32
        d_hidden = inv_std * (d_hat - jnp.mean(d_hat, axis=-1, keepdims=True) - x_hat * jnp.mean(d_hat * x_hat, axis=-1, keepdims=True))
        grad_h = (gy2.astype(F32) + d_hidden).astype(BF16)

        pair_block = pl.BlockSpec((1, 2 * tokens, PAIR), lambda i: (jnp.minimum(i, n_pairs - 1), 0, 0))
        col_block = pl.BlockSpec((width, PAIR), lambda i: (0, jnp.minimum(i, n_pairs - 1)))
        late = lambda *s: pl.BlockSpec((blk,) + s, lambda i: (jnp.maximum(i - n_pairs, 0), 0, 0))
        grad_mem = pl.pallas_call(
            functools.partial(mem_kernel, n_pairs), grid=(2 * n_pairs,), name="mem",
            in_specs=[pair_block, pair_block, col_block, col_block, late(n_fr, 2 * rows)], out_specs=late(n_fr, width),
            out_shape=jax.ShapeDtypeStruct((n_seq, n_fr, width), BF16), compiler_params=params(),
            scratch_shapes=[vm(BF16, 2, n_pairs, 2 * tokens, width)],
            cost_estimate=pl.CostEstimate(flops=8 * n_seq * n_fr * rows * width, bytes_accessed=40 << 20, transcendentals=0),
        )(q2, d2, w_k, w_v, pg)

        hidden_work = (out_y, grad_h, grad_mem, grad_ln_gain, grad_ln_bias, grad_wq, grad_wo, grad_bo)
        got[0], hidden_work = lax.optimization_barrier((got[0], hidden_work))
        out_y, grad_h, grad_mem, grad_ln_gain, grad_ln_bias, grad_wq, grad_wo, grad_bo = hidden_work
        core_arr = core.reshape(1).astype(jnp.int32)
        acc, at = (), 0
        for c, c2, g in zip(chips, chips2, got):
            g, acc = lax.optimization_barrier((g, acc))
            acc = assemble(core_arr, c, g, c2, swap(g, 1), head, head2, at, acc)
            at += c.shape[0]
        grad_wk, grad_wv = acc
        return (out_y.reshape(hidden.shape), grad_h.reshape(hidden.shape), grad_mem, grad_ln_gain, grad_ln_bias,
                grad_wq, grad_bq, grad_wk, grad_wv, grad_bv, grad_wo, grad_bo)

    return jax.shard_map(device_step, mesh=mesh, in_specs=in_specs, out_specs=out_specs, check_vma=False)
```
